32 devices in a mesh: groups: 2 (over y), tok: 8 (over z, core), head: 2 (over x), pair: 1.
Axes of the slice: x: 2, y: 2, z: 4, core: 2. Of those that a mesh axis runs over, the one named last changes fastest.
Arguments:
- queries: bfloat16 [2048, 4096], P(('groups', 'tok'), ('head', 'pair')), parts along dimension 0, may hold values from -6 to 6
- keys_values: bfloat16 [2048, 1024], P(('groups', 'tok'), ('head', 'pair')), parts along dimension 0, may hold values from -6 to 6
- sink_logits: float32 [64], P(('head', 'pair')), may hold values from -2 to 3
- residual: bfloat16 [2048, 2880], P(('groups', 'tok')), parts along dimension 0, may hold values from -60 to 60
- out_weight: bfloat16 [4096, 2880], P(('head', 'pair')), may hold values from -0.09375 to 0.09375
- norm_gain: float32 [2880], replicated, may hold values from 0.5 to 1.5
- expert_ids: int32 [2048, 4], P(('groups', 'tok')), parts along dimension 0, may hold values from 0 to 7, all different within a row; in each aligned block of 128 rows (0 to 127, 128 to 255, ...) at most 80 rows name the same one
- route_weights: float32 [2048, 4], P(('groups', 'tok')), parts along dimension 0, may hold values from 0.1 to 1
- gate_up: bfloat16 [8, 2880, 2, 1440], P('tok', None, None, ('head', 'pair')), may hold values from -0.109375 to 0.109375
- down_weight: bfloat16 [8, 1440, 2880], P('tok', ('head', 'pair')), may hold values from -0.21875 to 0.21875
Outputs:
- layer_output: bfloat16 [2048, 2880], P(('groups', 'tok'), ('head', 'pair')), parts along dimension 0
The draws below stay inside these ranges and needn't reach their ends.
There are 2 independent parts, one for each index of `groups`. The reference program is written for one: setup_inputs(seed, part) draws one part's arguments, and reference() takes and returns one part's arrays. A program takes and returns all parts, laid end to end along the dimension named above; an argument that names none is the same for every part. Nothing has to cross between parts.
Inputs may be any that keep to these rules, and one draw needn't show every extreme that they name: `expert_ids`: in each aligned block of 128 rows (the rows of one index of tok), a row names 4 different experts and no expert is named by more than 80 rows.
All inputs are finite; a program needn't handle non-finite values.
Results may differ from the reference program's by a relative error of at most 0.01.
Values may be sent and summed in bfloat16 or wider, within the bound.
A program may use at most 128 MiB of HBM per device.

```python
import math
import jax
import jax.numpy as jnp
import numpy as np
from jax import lax

D = 2880
HEADS = 64
KV_HEADS = 8
HEAD_DIM = 64
FFE = 1440
TOP = 4
TOK_DEV = 128
TOKENS = 1024
EXPERTS = 8
CAP = 80
N_TOK = 8


def attention_inputs(key):
    base = jax.random.fold_in(key, 11)
    key_query, key_keys = jax.random.split(base, 2)
    query_width = HEADS * HEAD_DIM
    key_width = KV_HEADS * 2 * HEAD_DIM
    queries = jnp.clip(jax.random.normal(key_query, (TOKENS, query_width), jnp.float32), -6.0, 6.0)
    keys_values = jnp.clip(jax.random.normal(key_keys, (TOKENS, key_width), jnp.float32), -6.0, 6.0)
    return (queries, keys_values)


def draw_queries(key, part):
    return attention_inputs(key)[0].astype(jnp.bfloat16)


def draw_keys_values(key, part):
    return attention_inputs(key)[1].astype(jnp.bfloat16)


def draw_residual(key, part):
    key_base, key_rows, key_cols = jax.random.split(jax.random.fold_in(key, 5), 3)
    values = jnp.clip(jax.random.normal(key_base, (TOKENS, D), jnp.float32), -4.0, 4.0)
    row_scale = jnp.exp(jax.random.uniform(key_rows, (TOKENS, 1), jnp.float32, -1.2, 1.1))
    rising = 0.6 + 1.2 * jnp.arange(D, dtype=jnp.float32)[None, :] / D
    col_scale = jnp.exp(jax.random.uniform(key_cols, (1, D), jnp.float32, -1.0, 1.0)) * rising
    return (values * row_scale * col_scale).astype(jnp.bfloat16)


def strengthened(values, rng, source, target, shards_of, factor):
    def block_of(dim):
        return (jnp.arange(values.shape[dim]) // (values.shape[dim] // shards_of)).reshape((-1,) + (1,) * (values.ndim - 1 - dim))

    near = jax.random.permutation(rng, shards_of)[block_of(target)]
    other_side = (block_of(target) + shards_of // 2) % shards_of
    return jnp.where((block_of(source) == near) | (block_of(source) == other_side), factor * values, values)


def levels(stream_key, extent, cuts, smallest, high):
    def one(dim, shards_of):
        steps = jax.random.uniform(jax.random.fold_in(jax.random.fold_in(stream_key, 6), dim), (shards_of,), jnp.float32, smallest / len(cuts), high / len(cuts))
        return jnp.repeat(jnp.exp(steps), extent[dim] // shards_of).reshape((-1,) + (1,) * (len(extent) - dim - 1))

    factor_of = one(*cuts[0])
    for cut in cuts[1:]:
        factor_of = factor_of * one(*cut)
    return factor_of


def deal_out(rng, own, number, rows, number_of, top, limit, lean):
    sequence = jax.random.permutation(rng, number_of)
    heavy_load, usual = load_shares(number_of, rows * top, limit, lean, True), load_shares(number_of, rows * top, limit, lean, False)
    places = jnp.arange(number_of)

    def named(sizes, rotation):
        used = int((sizes > 0).sum())
        fixed = max(1, used // 4)
        moved = fixed + (places - fixed + rotation * (used - fixed)) % max(1, number_of - fixed)
        return jnp.zeros((number_of,), jnp.int32).at[sequence[jnp.where(places < fixed, places, moved)]].set(jnp.asarray(sizes, jnp.int32))

    sizes = jnp.where(number % 4 == 0, named(heavy_load, number // 4), named(usual, number - number // 4 - 1))
    mixed = jax.random.permutation(jax.random.fold_in(own, 3), number_of)
    source_of, receiver = mixed[0:number_of // 2 * 2:2], mixed[1:number_of // 2 * 2:2]
    slack = jnp.minimum(sizes[source_of] - 1, limit - sizes[receiver]) // 2
    slack = jnp.where((source_of == sequence[0]) | (receiver == sequence[0]) | (sizes[receiver] == 0), 0, jnp.maximum(slack, 0))
    moved = jax.random.randint(jax.random.fold_in(own, 4), (number_of // 2,), 0, 1 << 20) % (slack + 1)
    sizes = sizes.at[source_of].add(-moved).at[receiver].add(moved)
    items = jnp.searchsorted(jnp.cumsum(sizes), jnp.arange(rows * top), side="right").astype(jnp.int32)
    table = items.reshape(top, rows).T
    table = table[jax.random.permutation(jax.random.fold_in(own, 1), rows)]
    rotation = jax.random.randint(jax.random.fold_in(own, 2), (rows, 1), 0, top)
    return jnp.take_along_axis(table, (jnp.arange(top)[None, :] + rotation) % top, axis=1)


def load_shares(count, total, most, lean, full):
    loads = [(1 << 20) // math.isqrt(rank ** lean) + 1 for rank in range(1, count + 1)]
    largest = most if full else min(most, max(-(-total // count), total * loads[0] // sum(loads)))
    least = 1 if total - largest >= count - 1 else 0
    holding, spare = [largest] + [least] * (count - 1), total - largest - least * (count - 1)
    while spare > 0:
        candidates = [i for i in range(1, count) if holding[i] < largest] or [i for i in range(1, count) if holding[i] < most]
        pool, budget = sum([loads[i] for i in candidates]), spare
        for i in candidates:
            extra = min(most - holding[i], max(1, budget * loads[i] // pool), spare)
            holding[i] = holding[i] + extra
            spare = spare - extra
    return np.array(holding)


def noise(key, dims, deviation, bound, pieces=(), kind=jnp.bfloat16):
    values = jax.random.normal(key, dims, jnp.float32) * deviation
    if len(pieces) > 0:
        values = levels(key, dims, pieces, -0.22, 0.18) * values
    return jnp.clip(values, min=-bound, max=bound).astype(kind)


def gaussian_with(rng, extent, spread, limit, shards, heavy, held_as=jnp.bfloat16):
    values = spread * jax.random.normal(rng, extent, jnp.float32)
    if shards:
        values = values * levels(rng, extent, shards, -0.22, 0.18)
    return jnp.clip(strengthened(values, jax.random.fold_in(rng, 3), *heavy), -limit, limit).astype(held_as)


def setup_inputs(seed: int = 0, part: int = 0) -> dict:
    arg_keys = jax.random.split(jax.random.key(seed), 11)
    part_splits = jax.random.split(jax.random.fold_in(arg_keys[10], part), 11)
    queries = draw_queries(jax.random.fold_in(jax.random.fold_in(arg_keys[10], part), 71), part)
    keys_values = draw_keys_values(jax.random.fold_in(jax.random.fold_in(arg_keys[10], part), 71), part)
    sink_logits = jnp.clip(-2.0 + 5.0 * jax.random.uniform(arg_keys[2], (HEADS,), jnp.float32) ** levels(arg_keys[2], (HEADS,), ((0, 2),), -0.2, 0.2), -2.0, 3.0)
    residual = draw_residual(jax.random.fold_in(jax.random.fold_in(arg_keys[10], part), 71), part)
    out_weight = noise(arg_keys[4], (HEADS * HEAD_DIM, D), (HEADS * HEAD_DIM) ** -0.5, 0.09375, ((0, 2),))
    norm_gain = jnp.clip(1.0 + 0.1 * jax.random.normal(arg_keys[5], (D,), jnp.float32), 0.5, 1.5)
    expert_ids_keys = jax.random.split(jax.random.fold_in(part_splits[6], 1), TOKENS // TOK_DEV)
    expert_ids_turns = jax.random.permutation(jax.random.fold_in(part_splits[6], 3), TOKENS // TOK_DEV)
    expert_ids = jax.vmap(lambda own, number: deal_out(jax.random.fold_in(part_splits[6], 2), own, number, TOK_DEV, EXPERTS, TOP, CAP, 2))(expert_ids_keys, expert_ids_turns).reshape((TOKENS, TOP))
    route_weights = jnp.clip(0.1 + 0.9 * jax.random.uniform(part_splits[7], (TOKENS, TOP), jnp.float32) ** levels(part_splits[7], (TOKENS, TOP), ((0, 8),), -0.2, 0.2), 0.1, 1.0)
    gate_up = noise(arg_keys[8], (EXPERTS, D, 2, FFE), D ** -0.5, 0.109375, ((0, 8), (3, 2)))
    down_weight = gaussian_with(arg_keys[9], (EXPERTS, FFE, D), FFE ** -0.5, 0.21875, ((0, 8), (1, 2)), (1, 2, 2, 2.0))
    return {"queries": queries, "keys_values": keys_values, "sink_logits": sink_logits, "residual": residual, "out_weight": out_weight, "norm_gain": norm_gain, "expert_ids": expert_ids, "route_weights": route_weights, "gate_up": gate_up, "down_weight": down_weight}


def slot_places(expert_ids, experts, capacity):
    tok_rows = expert_ids.shape[0]
    fanout = expert_ids.shape[1]
    flat_ids = expert_ids.reshape(-1).astype(jnp.int32)
    one_hot = (flat_ids[:, None] == jnp.arange(experts, dtype=jnp.int32)[None, :]).astype(jnp.int32)
    earlier = (jnp.cumsum(one_hot, axis=0) - one_hot).astype(jnp.int32)
    ranking = lax.optimization_barrier(jnp.sum(earlier * one_hot, axis=1)).astype(jnp.int32)
    targets = (flat_ids * capacity + ranking).astype(jnp.int32)
    sources = jnp.arange(tok_rows * fanout, dtype=jnp.int32) // fanout
    table = jnp.full((experts * capacity,), tok_rows, jnp.int32).at[targets].set(sources)
    return (targets.reshape(tok_rows, fanout), table)

def reference(queries, keys_values, sink_logits, residual, out_weight, norm_gain, expert_ids, route_weights, gate_up, down_weight):
    length = queries.shape[0]
    repeat = HEADS // KV_HEADS
    position = jnp.arange(length, dtype=jnp.int32)
    allowed = position[None, :] <= position[:, None]

    def one_head(number):
        query_head = lax.dynamic_slice_in_dim(queries, number * HEAD_DIM, HEAD_DIM, 1)
        group = number // repeat
        key_head = lax.dynamic_slice_in_dim(keys_values, group * 2 * HEAD_DIM, HEAD_DIM, 1)
        value_head = lax.dynamic_slice_in_dim(keys_values, group * 2 * HEAD_DIM + HEAD_DIM, HEAD_DIM, 1)
        scores = jnp.dot(query_head, key_head.T, preferred_element_type=jnp.float32) * 0.125
        scores = jnp.where(allowed, scores, jnp.float32(-1e+30))
        sink_value = sink_logits[number]
        top_value = jnp.maximum(lax.optimization_barrier(jnp.max(scores, axis=-1)), sink_value)
        weights = jnp.exp(scores - top_value[:, None])
        totals = jnp.exp(sink_value - top_value) + lax.optimization_barrier(jnp.sum(weights, axis=-1))
        mixed = jnp.dot(weights.astype(jnp.bfloat16), value_head, preferred_element_type=jnp.float32)
        return (mixed / totals[:, None]).astype(jnp.bfloat16)
    heads_out = lax.map(one_head, jnp.arange(HEADS, dtype=jnp.int32))
    attended = jnp.transpose(heads_out, (1, 0, 2)).reshape(length, HEADS * HEAD_DIM)
    projected = jnp.dot(attended, out_weight, preferred_element_type=jnp.float32)
    stream = residual.astype(jnp.float32) + projected
    inverse = lax.rsqrt(lax.optimization_barrier(jnp.mean(stream * stream, axis=-1, keepdims=True)) + 1e-05)
    normed = (stream * inverse * norm_gain).astype(jnp.bfloat16)
    block_ids = expert_ids.reshape(N_TOK, TOK_DEV, TOP)
    targets, tables = jax.vmap(lambda block_rows: slot_places(block_rows, EXPERTS, CAP))(block_ids)
    padded = jnp.concatenate([normed.reshape(N_TOK, TOK_DEV, D), jnp.zeros((N_TOK, 1, D), jnp.bfloat16)], axis=1)

    def pick_rows(block_rows, table_row):
        return block_rows[table_row]
    dispatched = jax.vmap(pick_rows)(padded, tables).reshape(N_TOK, EXPERTS, CAP, D)
    dispatched = jnp.transpose(dispatched, (1, 0, 2, 3))

    def one_expert(number):
        inputs = dispatched[number].reshape(N_TOK * CAP, D)
        weights_in = gate_up[number]
        gate_part = jnp.dot(inputs, weights_in[:, 0, :], preferred_element_type=jnp.float32)
        up_part = jnp.dot(inputs, weights_in[:, 1, :], preferred_element_type=jnp.float32)
        active = (gate_part * jax.nn.sigmoid(1.702 * gate_part) * (up_part + 1.0)).astype(jnp.bfloat16)
        result = jnp.dot(active, down_weight[number], preferred_element_type=jnp.float32).astype(jnp.bfloat16)
        return result.reshape(N_TOK, CAP, D)
    expert_out = lax.map(one_expert, jnp.arange(EXPERTS, dtype=jnp.int32))
    ranks = (targets - block_ids * CAP).astype(jnp.int32)
    block_index = jnp.arange(N_TOK, dtype=jnp.int32)[:, None, None]
    picked = expert_out[block_ids, block_index, ranks].reshape(length, TOP, D)
    mixture = lax.optimization_barrier(jnp.sum(route_weights[:, :, None] * picked.astype(jnp.float32), axis=1))
    return (stream + mixture).astype(jnp.bfloat16)
```

```python
import functools

import jax
import jax.numpy as jnp
from jax import lax
from jax.experimental import pallas as pl
from jax.experimental.pallas import tpu as pltpu
from jax.sharding import PartitionSpec as P

HEAD_DIM = 64

MESH_ID = pl.DeviceIdType.MESH

VMEM_BYTES = 67_043_328


def moe_kernel(
    dims,
    parts_ref,
    residual_ref,
    gain_ref,
    tail_ref,
    gate_hbm,
    down_hbm,
    out_ref,
    gate_w,
    down_w,
    rows,
    part,
    from_core,
    kept,
    from_peer,
    hop,
    from_right,
    from_left,
    peer_parts,
    stream,
    squares,
    peer_squares,
    acc,
    parts_send,
    parts_recv,
    squares_send,
    squares_recv,
    load_sem,
    row_recv,
    row_right,
    row_left,
    row_peer,
    row_core,
    part_send,
    part_recv,
    peer_send,
    peer_recv,
    hop_send,
    right_recv,
    left_recv,
):
    chips, cores, shares, pairs, width = dims
    tok = lax.axis_index("tok")
    z = tok // cores
    c = tok % cores
    mine = lax.axis_index("head") * pairs + lax.axis_index("pair")
    other = cores - 1 - c

    def tok_id(chip, core):
        return {"tok": chip * cores + core}

    def peer_id(share):
        return {"head": share // pairs, "pair": share % pairs}

    def remote(src, dst, send, recv, target):
        return pltpu.make_async_remote_copy(
            src_ref=src, dst_ref=dst, send_sem=send, recv_sem=recv,
            device_id=target, device_id_type=MESH_ID,
        )

    loads = [
        pltpu.make_async_copy(gate_hbm, gate_w.at[:, :, pl.ds(0, width)], load_sem.at[0]),
        pltpu.make_async_copy(down_hbm, down_w, load_sem.at[1]),
    ]
    for load in loads:
        load.start()

    barrier = pltpu.get_barrier_semaphore()

    @pl.when(z > 0)
    def _():
        pl.semaphore_signal(barrier, 1, device_id=tok_id(z - 1, c), device_id_type=MESH_ID)

    @pl.when(z < chips - 1)
    def _():
        pl.semaphore_signal(barrier, 1, device_id=tok_id(z + 1, c), device_id_type=MESH_ID)

    if cores > 1:
        pl.semaphore_signal(barrier, 1, device_id=tok_id(z, other), device_id_type=MESH_ID)
    for d in range(1, shares):
        pl.semaphore_signal(
            barrier, 1, device_id=peer_id((mine + d) % shares), device_id_type=MESH_ID
        )
    sides = jnp.where(z > 0, 1, 0) + jnp.where(z < chips - 1, 1, 0)
    pl.semaphore_wait(barrier, sides + (cores - 1) + (shares - 1))

    def parts_copy(d):
        share = (mine + d) % shares
        return remote(
            parts_ref.at[share], peer_parts.at[mine], parts_send.at[d - 1],
            parts_recv.at[mine], peer_id(share),
        )

    def squares_copy(d):
        return remote(
            squares, peer_squares.at[mine], squares_send.at[d - 1],
            squares_recv.at[mine], peer_id((mine + d) % shares),
        )

    for d in range(1, shares):
        parts_copy(d).start()
    gate_w[:, :, width:, :] = jnp.zeros(
        gate_w.shape[:2] + (gate_w.shape[2] - width, gate_w.shape[3]), jnp.bfloat16
    )
    stream[...] = residual_ref[...].astype(jnp.float32) + parts_ref[mine].astype(jnp.float32)
    for d in range(1, shares):
        share = (mine + d) % shares
        slot = peer_parts.at[share]
        pltpu.make_async_copy(slot, slot, parts_recv.at[share]).wait()
        stream[...] += peer_parts[share].astype(jnp.float32)
    own = stream[...]
    square = jnp.sum(own * own, axis=1, keepdims=True)
    squares[...] = jnp.broadcast_to(square, squares.shape)
    for d in range(1, shares):
        squares_copy(d).start()
    total_square = squares[...]
    for d in range(1, shares):
        share = (mine + d) % shares
        slot = peer_squares.at[share]
        pltpu.make_async_copy(slot, slot, squares_recv.at[share]).wait()
        total_square += peer_squares[share]
    inverse = lax.rsqrt(total_square[:, :1] / (shares * width) + 1e-05)
    normed = stream[...] * inverse * gain_ref[...] + tail_ref[...].astype(jnp.float32)
    rows[z, mine, c] = normed.astype(jnp.bfloat16)

    near = jnp.minimum(z, chips - 1 - z)

    def chip_at(i):
        inner = jnp.where(i % 2 == 1, z - (i + 1) // 2, z + i // 2)
        outer = jnp.where(z < chips - 1 - z, i, chips - 1 - i)
        return jnp.where(i <= 2 * near, inner, outer)

    def row_copy(chip, share, core, send, target):
        slot = rows.at[chip, share, core]
        return remote(slot, slot, send, row_recv.at[chip, core, share], target)

    def go_right(chip):
        return (chip <= z) & (z < chips - 1)

    def go_left(chip):
        return (chip >= z) & (z > 0)

    def right_copy(chip):
        return row_copy(chip, mine, c, row_right.at[chip], tok_id(z + 1, c))

    def left_copy(chip):
        return row_copy(chip, mine, c, row_left.at[chip], tok_id(z - 1, c))

    def peer_copy(chip, d):
        return row_copy(chip, mine, c, row_peer.at[chip, d - 1], peer_id((mine + d) % shares))

    def core_copy(chip, share):
        return row_copy(chip, share, c, row_core.at[chip, share], tok_id(z, other))

    def row_wait(chip, share, core):
        slot = rows.at[chip, share, core]
        pltpu.make_async_copy(slot, slot, row_recv.at[chip, core, share]).wait()

    def forward(i):
        chip = chip_at(i)

        @pl.when(go_right(chip))
        def _():
            right_copy(chip).start()

        @pl.when(go_left(chip))
        def _():
            left_copy(chip).start()

        for d in range(1, shares):
            peer_copy(chip, d).start()
        if cores > 1:
            core_copy(chip, mine).start()

    forward(0)
    loads[0].wait()
    loads[1].wait()

    tail = (width // 128) * 128
    wide = rows.shape[-1]
    depth = rows.shape[-2]
    experts = chips * cores
    tail_lane = tail + lax.broadcasted_iota(jnp.int32, (cores * depth, wide - tail), 1)
    weight_lane = (tail_lane == width + tok) | (tail_lane == width + experts + tok)

    def kept_at(chip, share):
        return kept.at[chip, share] if cores > 1 else part.at[chip, share, 0]

    def part_copy(chip, share):
        return remote(
            part.at[chip, share, other], from_core.at[chip, share],
            part_send.at[chip, share], part_recv.at[chip, share], tok_id(z, other),
        )

    def sum_copy(chip, d):
        share = (mine + d) % shares
        return remote(
            kept_at(chip, share), from_peer.at[chip, mine],
            peer_send.at[chip, d - 1], peer_recv.at[chip, mine], peer_id(share),
        )

    def compute(i, carry):
        @pl.when(i + 1 < chips)
        def _():
            row_wait(chip_at(i + 1), mine, c)
            forward(i + 1)

        chip = chip_at(i)
        for d in range(1, shares):
            share = (mine + d) % shares
            row_wait(chip, share, c)
            if cores > 1:
                core_copy(chip, share).start()
        if cores > 1:
            for share in range(shares):
                row_wait(chip, share, other)
        gate = jnp.zeros((cores * depth, gate_w.shape[-1]), jnp.float32)
        up = gate
        for share in range(shares):
            block = rows[chip, share].reshape(cores * depth, wide)
            gate += jnp.dot(block, gate_w[0, share], preferred_element_type=jnp.float32)
            up += jnp.dot(block, gate_w[1, share], preferred_element_type=jnp.float32)
        active = (gate * jax.nn.sigmoid(1.702 * gate) * (up + 1.0)).astype(jnp.bfloat16)
        ends = rows[chip, 0, :, :, tail:].reshape(cores * depth, wide - tail).astype(jnp.float32)
        weight = jnp.sum(jnp.where(weight_lane, ends, 0.0), axis=1, keepdims=True)
        for share in range(shares):
            out = jnp.dot(active, down_w[share], preferred_element_type=jnp.float32)
            out = (out * weight).astype(jnp.bfloat16)
            part[chip, share] = out.reshape(cores, depth, width)
            if cores > 1:
                part_copy(chip, share).start()
        for share in range(shares):
            if cores > 1:
                part_copy(chip, share).wait_recv()
                total = part[chip, share, c].astype(jnp.float32)
                total += from_core[chip, share].astype(jnp.float32)
                kept[chip, share] = total.astype(jnp.bfloat16)
        for d in range(1, shares):
            sum_copy(chip, d).start()
        return carry

    lax.fori_loop(0, chips, compute, 0)

    def right_hop(chip):
        return remote(
            hop.at[chip], from_left.at[chip], hop_send.at[chip], left_recv.at[chip],
            tok_id(z + 1, c),
        )

    def left_hop(chip):
        return remote(
            hop.at[chip], from_right.at[chip], hop_send.at[chip], right_recv.at[chip],
            tok_id(z - 1, c),
        )

    def hop_wait(buffer, sem, chip):
        pltpu.make_async_copy(buffer.at[chip], buffer.at[chip], sem.at[chip]).wait()

    def give_back(j, carry):
        chip = chip_at(chips - 1 - j)
        total = kept_at(chip, mine)[...].astype(jnp.float32)
        for d in range(1, shares):
            share = (mine + d) % shares
            slot = from_peer.at[chip, share]
            pltpu.make_async_copy(slot, slot, peer_recv.at[chip, share]).wait()
            total += from_peer[chip, share].astype(jnp.float32)
        acc[...] = total

        @pl.when((chip <= z) & (z < chips - 1))
        def _():
            hop_wait(from_right, right_recv, chip)
            acc[...] += from_right[chip].astype(jnp.float32)

        @pl.when((chip >= z) & (z > 0))
        def _():
            hop_wait(from_left, left_recv, chip)
            acc[...] += from_left[chip].astype(jnp.float32)

        @pl.when(chip == z)
        def _():
            out_ref[...] = (stream[:, :width] + acc[...]).astype(jnp.bfloat16)

        @pl.when(chip != z)
        def _():
            hop[chip] = acc[...].astype(jnp.bfloat16)

        @pl.when(chip < z)
        def _():
            left_hop(chip).start()

        @pl.when(chip > z)
        def _():
            right_hop(chip).start()

        return carry

    lax.fori_loop(0, chips, give_back, 0)

    def drain(chip, carry):
        @pl.when(go_right(chip))
        def _():
            right_copy(chip).wait_send()

        @pl.when(go_left(chip))
        def _():
            left_copy(chip).wait_send()

        for d in range(1, shares):
            peer_copy(chip, d).wait_send()
            sum_copy(chip, d).wait_send()
        if cores > 1:
            for share in range(shares):
                core_copy(chip, share).wait_send()
                part_copy(chip, share).wait_send()

        @pl.when(chip < z)
        def _():
            left_hop(chip).wait_send()

        @pl.when(chip > z)
        def _():
            right_hop(chip).wait_send()

        return carry

    lax.fori_loop(0, chips, drain, 0)
    for d in range(1, shares):
        parts_copy(d).wait_send()
        squares_copy(d).wait_send()


def moe(dims, parts, residual, gain, tail, gate_w, down_w):
    chips, cores, shares, pairs, width = dims
    depth, wide = residual.shape
    hidden = down_w.shape[1]
    bf16 = jnp.bfloat16
    dma = pltpu.SemaphoreType.DMA
    return pl.pallas_call(
        functools.partial(moe_kernel, dims),
        out_shape=jax.ShapeDtypeStruct((depth, width), jnp.bfloat16),
        in_specs=[pl.BlockSpec(memory_space=pltpu.VMEM)] * 4
        + [
            pl.BlockSpec(memory_space=pl.ANY),
            pl.BlockSpec(memory_space=pl.ANY),
        ],
        out_specs=pl.BlockSpec(memory_space=pltpu.VMEM),
        scratch_shapes=[
            pltpu.VMEM((2, shares, wide, hidden), bf16),
            pltpu.VMEM(down_w.shape, bf16),
            pltpu.VMEM((chips, shares, cores, depth, wide), bf16),
            pltpu.VMEM((chips, shares, cores, depth, width), bf16),
            pltpu.VMEM((chips, shares, depth, width) if cores > 1 else (8, 128), bf16),
            pltpu.VMEM((chips, shares, depth, width) if cores > 1 else (8, 128), bf16),
            pltpu.VMEM((chips, shares, depth, width), bf16),
            pltpu.VMEM((chips, depth, width), bf16),
            pltpu.VMEM((chips, depth, width), bf16),
            pltpu.VMEM((chips, depth, width), bf16),
            pltpu.VMEM((shares, depth, wide), bf16),
            pltpu.VMEM((depth, wide), jnp.float32),
            pltpu.VMEM((depth, 128), jnp.float32),
            pltpu.VMEM((shares, depth, 128), jnp.float32),
            pltpu.VMEM((depth, width), jnp.float32),
            dma((max(shares - 1, 1),)),
            dma((shares,)),
            dma((max(shares - 1, 1),)),
            dma((shares,)),
            dma((2,)),
            dma((chips, cores, shares)),
            dma((chips,)),
            dma((chips,)),
            dma((chips, max(shares - 1, 1))),
            dma((chips, shares)),
            dma((chips, shares)),
            dma((chips, shares)),
            dma((chips, max(shares - 1, 1))),
            dma((chips, shares)),
            dma((chips,)),
            dma((chips,)),
            dma((chips,)),
        ],
        compiler_params=pltpu.CompilerParams(
            collective_id=0, has_side_effects=True, vmem_limit_bytes=60 * 1024 * 1024
        ),
        cost_estimate=pl.CostEstimate(
            flops=6 * chips * cores * depth * shares * width * hidden,
            bytes_accessed=6 * shares * width * hidden,
            transcendentals=0,
        ),
    )(parts, residual, gain, tail, gate_w, down_w)


def per_device(
    queries,
    keys_values,
    sink_logits,
    residual,
    out_weight,
    norm_gain,
    expert_ids,
    route_weights,
    gate_up,
    down_weight,
):
    tok_rows = queries.shape[0]
    kv_groups = keys_values.shape[1] // (2 * HEAD_DIM)
    local_heads = queries.shape[1] // HEAD_DIM
    repeat = local_heads // kv_groups
    position = lax.axis_index("tok") * tok_rows + jnp.arange(tok_rows, dtype=jnp.int32)
    grouped = queries.reshape(tok_rows, kv_groups, repeat, HEAD_DIM)
    start_max = jnp.broadcast_to(
        sink_logits.reshape(kv_groups, repeat)[:, :, None], (kv_groups, repeat, tok_rows)
    )
    start_totals = jnp.ones((kv_groups, repeat, tok_rows), jnp.float32)
    start_accum = jnp.zeros((kv_groups, repeat, tok_rows, HEAD_DIM), jnp.float32)
    key_piece = lax.all_gather(keys_values, "tok", axis=0, tiled=True)
    hidden = down_weight.shape[1]
    shares = lax.axis_size(("head", "pair"))
    share = out_weight.shape[1] // shares
    gate_w = jnp.transpose(gate_up[0], (1, 0, 2)).reshape(2, shares, share, hidden)
    down_w = jnp.transpose(down_weight[0].reshape(hidden, shares, share), (1, 0, 2))
    key_piece, gate_w, down_w = lax.optimization_barrier((key_piece, gate_w, down_w))
    totals = start_totals
    accum = start_accum
    count = key_piece.shape[0]
    split_piece = key_piece.reshape(count, kv_groups, 2, HEAD_DIM)
    scores = (
        jnp.einsum(
            "tgrd,ngd->grtn", grouped, split_piece[:, :, 0], preferred_element_type=jnp.float32
        )
        * 0.125
    )
    key_position = jnp.arange(count, dtype=jnp.int32)
    allowed = key_position[None, :] <= position[:, None]
    scores = jnp.where(allowed, scores, jnp.float32(-1e30))
    new_max = jnp.maximum(start_max, jnp.max(scores, axis=-1))
    decay = jnp.exp(start_max - new_max)
    weights = jnp.exp(scores - new_max[..., None])
    totals = totals * decay + jnp.sum(weights, axis=-1)
    update = jnp.einsum(
        "grtn,ngd->grtd",
        weights.astype(jnp.bfloat16),
        split_piece[:, :, 1],
        preferred_element_type=jnp.float32,
    )
    accum = accum * decay[..., None] + update
    final_max, totals, accum = (new_max, totals, accum)
    attended = (accum / totals[..., None]).astype(jnp.bfloat16)
    attended = jnp.transpose(attended, (2, 0, 1, 3)).reshape(tok_rows, local_heads * HEAD_DIM)
    width = out_weight.shape[1]
    share = width // lax.axis_size(("head", "pair"))
    column_start = lax.axis_index(("head", "pair")) * share
    partial_value = jnp.dot(attended, out_weight, preferred_element_type=jnp.float32)
    experts = lax.axis_size("tok")
    pairs = lax.axis_size("pair")
    cores = 2 // pairs
    shares = width // share
    wide = -(-(share + 2 * experts) // 128) * 128
    expert = jnp.arange(experts, dtype=jnp.int32)
    routed = expert_ids[:, :, None] == expert
    dense = jnp.sum(jnp.where(routed, route_weights[:, :, None], 0.0), axis=1)
    high = lax.reduce_precision(dense, 8, 7)
    weights = jnp.concatenate([high, dense - high], axis=1).astype(jnp.bfloat16)
    tail = jnp.pad(weights, ((0, 0), (share, wide - share - 2 * experts)))
    spare = (0, wide - share)
    parts = jnp.transpose(
        partial_value.astype(jnp.bfloat16).reshape(tok_rows, shares, share), (1, 0, 2)
    )
    parts = jnp.pad(parts, ((0, 0), (0, 0), spare))
    own_residual = jnp.pad(
        lax.dynamic_slice_in_dim(residual, column_start, share, 1), ((0, 0), spare)
    )
    own_gain = jnp.pad(lax.dynamic_slice_in_dim(norm_gain, column_start, share, 0), spare)
    return moe(
        (experts // cores, cores, shares, pairs, share),
        parts, own_residual, own_gain[None, :], tail, gate_w, down_w,
    )


def layer_kernel(
    dims,
    sink_ref,
    ids_ref,
    route_ref,
    gain_ref,
    query_hbm,
    kv_hbm,
    residual_hbm,
    project_hbm,
    gate_hbm,
    down_hbm,
    out_ref,
    query_v,
    query_t,
    kvs,
    row_max,
    row_total,
    accum,
    attended,
    residual_v,
    project_w,
    gate_w,
    down_v,
    down_t,
    gain_cols,
    stream,
    parts,
    peer_parts,
    rows,
    meta,
    hidden,
    active,
    part,
    kept,
    from_core,
    cross,
    from_peer,
    hop,
    from_left,
    from_right,
    load_sem,
    kv_recv,
    kv_core_send,
    kv_up_send,
    parts_send,
    parts_recv,
    row_recv,
    row_up,
    row_down,
    row_core,
    row_peer,
    meta_recv,
    meta_up,
    meta_down,
    meta_core,
    part_send,
    part_recv,
    peer_send,
    peer_recv,
    hop_send,
    left_recv,
    right_recv,
):
    chips, pairs, chunk, piece = dims
    cores = 2
    width, depth = residual_hbm.shape
    kv_groups = kvs.shape[1]
    repeat = query_t.shape[2] // depth
    half = width // 2
    f32, bf16 = jnp.float32, jnp.bfloat16
    full = width // chunk
    tail = width - full * chunk
    own = full // 2
    shared = full - 2 * own
    pieces = half // piece
    last = chips - 1

    tok = lax.axis_index("tok")
    z = tok // cores
    c = tok % cores
    x = lax.axis_index("head") * pairs + lax.axis_index("pair")
    peer = {"head": (1 - x) // pairs, "pair": (1 - x) % pairs}
    other = {"tok": z * cores + (1 - c)}
    above = {"tok": (z + 1) * cores + c}
    below = {"tok": (z - 1) * cores + c}

    def remote(src, dst, send, recv, target):
        return pltpu.make_async_remote_copy(
            src_ref=src, dst_ref=dst, send_sem=send, recv_sem=recv,
            device_id=target, device_id_type=MESH_ID,
        )

    def landed(slot, sem):
        pltpu.make_async_copy(slot, slot, sem).wait()

    def mult(value, of):
        return pl.multiple_of(value, of)

    loads = [
        pltpu.make_async_copy(
            kv_hbm.at[:, pl.ds(g * 2 * HEAD_DIM, 2 * HEAD_DIM)], kvs.at[tok, g], load_sem.at[g]
        )
        for g in range(kv_groups)
    ]
    bulk = [
        pltpu.make_async_copy(src, dst, load_sem.at[kv_groups + i])
        for i, (src, dst) in enumerate(
            [
                (query_hbm, query_v),
                (residual_hbm, residual_v),
                (project_hbm, project_w),
                (down_hbm, down_v),
                (gate_hbm, gate_w),
            ]
        )
    ]
    for load in loads + bulk:
        load.start()

    barrier = pltpu.get_barrier_semaphore()

    @pl.when(z > 0)
    def _():
        pl.semaphore_signal(barrier, 1, device_id=below, device_id_type=MESH_ID)

    @pl.when(z < last)
    def _():
        pl.semaphore_signal(barrier, 1, device_id=above, device_id_type=MESH_ID)

    pl.semaphore_signal(barrier, 1, device_id=other, device_id_type=MESH_ID)
    pl.semaphore_signal(barrier, 1, device_id=peer, device_id_type=MESH_ID)
    sides = jnp.where(z > 0, 1, 0) + jnp.where(z < last, 1, 0)
    pl.semaphore_wait(barrier, sides + 2)

    def kv_up(chip):
        slot = kvs.at[chip * cores + c]
        return remote(slot, slot, kv_up_send.at[chip], kv_recv.at[chip, c], above)

    def kv_core(chip):
        slot = kvs.at[chip * cores + c]
        return remote(slot, slot, kv_core_send.at[chip], kv_recv.at[chip, c], other)

    def kv_wait(chip, core):
        landed(kvs.at[chip * cores + core], kv_recv.at[chip, core])

    def kv_pass(chip):
        @pl.when(z < last)
        def _():
            kv_up(chip).start()

        kv_core(chip).start()

    for load in loads:
        load.wait()
    kv_pass(z)

    bulk[0].wait()
    for g in range(kv_groups):
        query_t[g, HEAD_DIM:, :] = jnp.zeros((HEAD_DIM, repeat * depth), bf16)
        for m in range(repeat // 2):
            lane = (g * repeat + 2 * m) * HEAD_DIM
            turned = (query_v[:, lane:lane + 2 * HEAD_DIM].astype(f32) * 0.125).T.astype(bf16)
            query_t[g, :HEAD_DIM, 2 * m * depth:(2 * m + 1) * depth] = turned[:HEAD_DIM]
            query_t[g, :HEAD_DIM, (2 * m + 1) * depth:(2 * m + 2) * depth] = turned[HEAD_DIM:]
        for r in range(repeat):
            row_max[g, :, r * depth:(r + 1) * depth] = jnp.full(
                (1, depth), sink_ref[g * repeat + r], f32
            )
    row_total[...] = jnp.ones(row_total.shape, f32)
    accum[...] = jnp.zeros(accum.shape, f32)

    def attend(chip, g, masked):
        keys = kvs[pl.ds(chip * cores, cores), g].reshape(cores * depth, 2 * HEAD_DIM)
        values = keys.astype(f32).T[HEAD_DIM:].astype(bf16)
        for m in range(repeat // 2):
            lanes = slice(2 * m * depth, (2 * m + 2) * depth)
            scores = jnp.dot(keys, query_t[g, :, lanes], preferred_element_type=f32)
            if masked:
                row = lax.broadcasted_iota(jnp.int32, scores.shape, 0)
                column = lax.broadcasted_iota(jnp.int32, scores.shape, 1)
                column = jnp.where(column >= depth, column - depth, column)
                scores = jnp.where(row <= c * depth + column, scores, jnp.float32(-1e30))
            old = row_max[g, :, lanes]
            new = jnp.maximum(old, jnp.max(scores, axis=0, keepdims=True))
            weights = jnp.exp(scores - new)
            decay = jnp.exp(old - new)
            row_max[g, :, lanes] = new
            row_total[g, :, lanes] = row_total[g, :, lanes] * decay + jnp.sum(
                weights, axis=0, keepdims=True
            )
            accum[g, :, lanes] = accum[g, :, lanes] * decay + jnp.dot(
                values, weights.astype(bf16), preferred_element_type=f32
            )

    def attend_chip(chip, masked):
        kv_wait(chip, 1 - c)

        def group(g, carry):
            attend(chip, g, masked)
            return carry

        lax.fori_loop(0, kv_groups // 2, group, 0)

        @pl.when(chip > 0)
        def _():
            kv_wait(chip - 1, c)
            kv_pass(chip - 1)

        lax.fori_loop(kv_groups // 2, kv_groups, group, 0)

    attend_chip(z, True)

    def earlier(i, carry):
        attend_chip(z - i, False)
        return carry

    lax.fori_loop(1, z + 1, earlier, 0)

    for g in range(kv_groups):
        inverse = 1.0 / row_total[g]
        for r in range(repeat):
            lanes = slice(r * depth, (r + 1) * depth)
            head = (g * repeat + r) * HEAD_DIM
            attended[head:head + HEAD_DIM, :] = (accum[g, :, lanes] * inverse[:, lanes]).astype(bf16)

    order = [side * own + k for k in range(own) for side in range(2)]
    order += list(range(2 * own, full + (1 if tail else 0)))
    spans = {k: (k * chunk, tail if k == full else chunk) for k in order}

    def parts_copy(k):
        start, size = spans[k]
        return remote(
            parts.at[pl.ds(start, size)], peer_parts.at[pl.ds(start, size)],
            parts_send.at[k], parts_recv.at[k], peer,
        )

    bulk[1].wait()
    bulk[2].wait()
    for k in order:
        start, size = spans[k]
        block = slice(start, start + size)
        value = jnp.dot(project_w[block, :], attended[...], preferred_element_type=f32)
        parts[block, :] = value.astype(bf16)
        parts_copy(k).start()
        stream[block, :] = value + residual_v[block, :].astype(f32)

    lanes_all = -(-width // 128)
    for b in range(lanes_all):
        size = min(128, width - b * 128)
        gain = gain_ref[:, b * 128:b * 128 + size]
        gain_cols[b * 128:b * 128 + size, :] = jnp.broadcast_to(gain, (128, size)).T

    bulk[3].wait()

    def turn(b, carry):
        at = pl.ds(mult(b * 128, 128), 128)
        down_t[at, :] = down_v[:, at].astype(f32).T.astype(bf16)
        return carry

    lax.fori_loop(0, width // 128, turn, 0)
    if width % 128:
        at = pl.ds(width // 128 * 128, width % 128)
        down_t[at, :] = down_v[:, at].astype(f32).T.astype(bf16)

    def carried(k):
        return k >= 2 * own

    def row_slot(chip, core, start, size):
        return rows.at[chip, core, pl.ds(start, size)]

    def row_copy(chip, k, size, send, target):
        slot = row_slot(chip, c, mult(k * chunk, chunk), size)
        return remote(slot, slot, send.at[chip, k], row_recv.at[chip, c, k], target)

    def row_wait(chip, core, k, size):
        landed(row_slot(chip, core, mult(k * chunk, chunk), size), row_recv.at[chip, core, k])

    def pass_along(chip, k, size):
        @pl.when((chip <= z) & (z < last))
        def _():
            row_copy(chip, k, size, row_up, above).start()

        @pl.when((chip >= z) & (z > 0))
        def _():
            row_copy(chip, k, size, row_down, below).start()

    def meta_copy(chip, send, target):
        slot = meta.at[chip, c]
        return remote(slot, slot, send.at[chip], meta_recv.at[chip, c], target)

    def meta_wait(chip, core):
        landed(meta.at[chip, core], meta_recv.at[chip, core])

    def pass_meta(chip):
        @pl.when((chip <= z) & (z < last))
        def _():
            meta_copy(chip, meta_up, above).start()

        @pl.when((chip >= z) & (z > 0))
        def _():
            meta_copy(chip, meta_down, below).start()

        meta_copy(chip, meta_core, other).start()

    squares = jnp.zeros((8, depth), f32)
    for k in order:
        start, size = spans[k]
        block = slice(start, start + size)
        landed(peer_parts.at[pl.ds(start, size)], parts_recv.at[k])
        value = stream[block, :] + peer_parts[block, :].astype(f32)
        stream[block, :] = value
        rows[z, c, block, :] = (value * gain_cols[block, :]).astype(bf16)
        squares += jnp.sum((value * value).reshape(size // 8, 8, depth), axis=0)
        if carried(k):
            pass_along(z, k, size)
        else:
            @pl.when(x == k // own)
            def _():
                pass_along(z, k, size)

        row_copy(z, k, size, row_core, other).start()
    total = jnp.sum(squares, axis=0, keepdims=True)
    scale = lax.rsqrt(total / width + 1e-05)
    meta[z, c, 0:8, :] = jnp.broadcast_to(scale, (8, depth))
    experts = chips * cores
    expert = lax.broadcasted_iota(jnp.int32, (experts, depth), 0)
    dense = jnp.zeros((experts, depth), f32)
    for k in range(ids_ref.shape[0]):
        dense += jnp.where(ids_ref[k:k + 1, :] == expert, route_ref[k:k + 1, :], 0.0)
    meta[z, c, pl.ds(8, experts), :] = dense
    pass_meta(z)

    bulk[4].wait()

    near = jnp.minimum(z, last - z)

    def chip_at(i):
        inner = jnp.where(i % 2 == 1, z - (i + 1) // 2, z + i // 2)
        outer = jnp.where(z < last - z, i, last - i)
        return jnp.where(i <= 2 * near, inner, outer)

    def each_side(i, act):
        @pl.when(z - 1 - i >= 0)
        def _():
            act(z - 1 - i)

        @pl.when(z + 1 + i <= last)
        def _():
            act(z + 1 + i)

    def pump_line(i, k, size, crosses):
        def act(chip):
            row_wait(chip, c, k, size)
            pass_along(chip, k, size)
            if crosses is not None:
                @pl.when(crosses)
                def _():
                    row_copy(chip, k, size, row_peer, peer).start()

            row_copy(chip, k, size, row_core, other).start()

        each_side(i, act)

    def pump_cross(i, k, size):
        def act(chip):
            row_wait(chip, c, k, size)
            row_copy(chip, k, size, row_core, other).start()

        each_side(i, act)

    def multiply(chip, k, size):
        row_wait(chip, 1 - c, k, size)
        at = pl.ds(mult(k * chunk, chunk), size)
        both = jnp.concatenate([rows[chip, c, at, :], rows[chip, 1 - c, at, :]], axis=1)
        for side in range(2):
            hidden[side] += jnp.dot(gate_w[side, :, at], both, preferred_element_type=f32)

    def part_copy(chip, r):
        return remote(
            part.at[chip, r], from_core.at[chip, r], part_send.at[chip, r],
            part_recv.at[chip, r], other,
        )

    def cross_copy(chip, r):
        return remote(
            cross.at[chip, r], from_peer.at[chip, r], peer_send.at[chip, r],
            peer_recv.at[chip, r], peer,
        )

    def up_hop(chip, r):
        return remote(
            hop.at[chip, r], from_left.at[chip, r], hop_send.at[chip, r],
            left_recv.at[chip, r], above,
        )

    def down_hop(chip, r):
        return remote(
            hop.at[chip, r], from_right.at[chip, r], hop_send.at[chip, r],
            right_recv.at[chip, r], below,
        )


    def send_sum(chip, incoming, buffer, sem, copy):
        def one(r, carry):
            landed(from_peer.at[chip, r], peer_recv.at[chip, r])
            value = kept[chip, x * pieces + r].astype(f32) + from_peer[chip, r].astype(f32)

            @pl.when(incoming)
            def _():
                landed(buffer.at[chip, r], sem.at[chip, r])
                hop[chip, r] = (value + buffer[chip, r].astype(f32)).astype(bf16)

            @pl.when(jnp.logical_not(incoming))
            def _():
                hop[chip, r] = value.astype(bf16)

            copy(chip, r).start()
            return carry

        lax.fori_loop(0, pieces, one, 0)

    def step(i, carry):
        chip = chip_at(i)
        hidden[...] = jnp.zeros(hidden.shape, f32)

        def line(t, carry):
            k = jnp.where(t < own, own * x + t, own + t)
            pump_line(i, k, chunk, t < own)
            multiply(chip, k, chunk)
            return carry

        lax.fori_loop(0, own + shared, line, 0)
        if tail:
            pump_line(i, full, tail, None)
            multiply(chip, full, tail)

        def forward_meta(q):
            meta_wait(q, c)
            pass_meta(q)

        each_side(i, forward_meta)

        def crossed(t, carry):
            k = own * (1 - x) + t
            pump_cross(i, k, chunk)
            multiply(chip, k, chunk)
            return carry

        lax.fori_loop(0, own, crossed, 0)

        meta_wait(chip, 1 - c)
        scale = jnp.concatenate([meta[chip, c, 0:1, :], meta[chip, 1 - c, 0:1, :]], axis=1)
        weight = jnp.concatenate(
            [meta[chip, c, pl.ds(8 + tok, 1), :], meta[chip, 1 - c, pl.ds(8 + tok, 1), :]], axis=1
        )
        gate = hidden[0] * scale
        up = hidden[1] * scale
        active[...] = (gate * jax.nn.sigmoid(1.702 * gate) * (up + 1.0) * weight).astype(bf16)

        def spread(r, carry):
            at = jnp.where(r < pieces, (1 - x) * pieces + r, x * pieces + r - pieces)
            value = jnp.dot(
                down_t[pl.ds(mult(at * piece, piece), piece), :], active[...],
                preferred_element_type=f32,
            )
            part[chip, at] = value[:, depth:].astype(bf16)
            part_copy(chip, at).start()
            kept[chip, at] = value[:, :depth].astype(bf16)
            return carry

        lax.fori_loop(0, 2 * pieces, spread, 0)

        def join(r, carry):
            at = (1 - x) * pieces + r
            landed(from_core.at[chip, at], part_recv.at[chip, at])
            value = kept[chip, at].astype(f32) + from_core[chip, at].astype(f32)
            cross[chip, r] = value.astype(bf16)
            cross_copy(chip, r).start()
            return carry

        lax.fori_loop(0, pieces, join, 0)

        def keep(r, carry):
            at = x * pieces + r
            landed(from_core.at[chip, at], part_recv.at[chip, at])
            value = kept[chip, at].astype(f32) + from_core[chip, at].astype(f32)
            kept[chip, at] = value.astype(bf16)
            return carry

        lax.fori_loop(0, pieces, keep, 0)

        @pl.when(i > z)
        def _():
            send_sum(i, z > 0, from_left, left_recv, up_hop)

        @pl.when((i > 0) & (last - i < z))
        def _():
            send_sum(last - i, z < last, from_right, right_recv, down_hop)

        return carry

    lax.fori_loop(0, chips, step, 0)

    def finish(r, carry):
        at = pl.ds(mult(x * half + r * piece, 16), piece)
        landed(from_peer.at[z, r], peer_recv.at[z, r])
        stream[at, :] += (
            kept[z, x * pieces + r].astype(f32) + from_peer[z, r].astype(f32)
        )

        @pl.when(z > 0)
        def _():
            landed(from_left.at[z, r], left_recv.at[z, r])
            stream[at, :] += from_left[z, r].astype(f32)

        @pl.when(z < last)
        def _():
            landed(from_right.at[z, r], right_recv.at[z, r])
            stream[at, :] += from_right[z, r].astype(f32)

        out_ref[pl.ds(mult(r * piece, piece), piece), :] = stream[at, :].astype(bf16)
        return carry

    lax.fori_loop(0, pieces, finish, 0)

    def drain(chip, carry):
        @pl.when(chip <= z)
        def _():
            kv_core(chip).wait_send()

        @pl.when((chip <= z) & (z < last))
        def _():
            kv_up(chip).wait_send()

        def sent(k, size, on_line, crosses):
            def line():
                @pl.when((chip <= z) & (z < last))
                def _():
                    row_copy(chip, k, size, row_up, above).wait_send()

                @pl.when((chip >= z) & (z > 0))
                def _():
                    row_copy(chip, k, size, row_down, below).wait_send()

            if on_line:
                line()
            if crosses:
                @pl.when(chip != z)
                def _():
                    row_copy(chip, k, size, row_peer, peer).wait_send()

            row_copy(chip, k, size, row_core, other).wait_send()

        for t in range(own):
            sent(own * x + t, chunk, True, True)
            sent(own * (1 - x) + t, chunk, False, False)
        for t in range(shared):
            sent(2 * own + t, chunk, True, False)
        if tail:
            sent(full, tail, True, False)

        @pl.when((chip <= z) & (z < last))
        def _():
            meta_copy(chip, meta_up, above).wait_send()

        @pl.when((chip >= z) & (z > 0))
        def _():
            meta_copy(chip, meta_down, below).wait_send()

        meta_copy(chip, meta_core, other).wait_send()
        for r in range(2 * pieces):
            part_copy(chip, r).wait_send()
        for r in range(pieces):
            cross_copy(chip, r).wait_send()

            @pl.when(chip > z)
            def _():
                up_hop(chip, r).wait_send()

            @pl.when(chip < z)
            def _():
                down_hop(chip, r).wait_send()

        return carry

    lax.fori_loop(0, chips, drain, 0)
    for k in order:
        parts_copy(k).wait_send()


def whole_layer(
    dims, sinks, ids, route, gain, queries, keys_values, residual, project, gate_up, down
):
    chips, pairs, chunk, piece = dims
    cores = 2
    width, depth = residual.shape
    kv_groups = keys_values.shape[1] // (2 * HEAD_DIM)
    heads = queries.shape[1] // HEAD_DIM
    repeat = heads // kv_groups
    hidden = down.shape[0]
    half = width // 2
    pieces = half // piece
    count = -(-width // chunk)
    bf16, f32 = jnp.bfloat16, jnp.float32
    dma = pltpu.SemaphoreType.DMA
    vmem = pltpu.VMEM
    experts = chips * cores
    flops = 2 * width * (
        depth * heads * HEAD_DIM + chips * cores * depth * 3 * hidden
    )
    return pl.pallas_call(
        functools.partial(layer_kernel, dims),
        out_shape=jax.ShapeDtypeStruct((half, depth), bf16),
        in_specs=[pl.BlockSpec(memory_space=pltpu.SMEM)]
        + [pl.BlockSpec(memory_space=pltpu.VMEM)] * 3
        + [pl.BlockSpec(memory_space=pl.ANY)] * 6,
        out_specs=pl.BlockSpec(memory_space=pltpu.VMEM),
        scratch_shapes=[
            vmem(queries.shape, bf16),
            vmem((kv_groups, 2 * HEAD_DIM, repeat * depth), bf16),
            vmem((experts, kv_groups, depth, 2 * HEAD_DIM), bf16),
            vmem((kv_groups, 1, repeat * depth), f32),
            vmem((kv_groups, 1, repeat * depth), f32),
            vmem((kv_groups, HEAD_DIM, repeat * depth), f32),
            vmem((heads * HEAD_DIM, depth), bf16),
            vmem(residual.shape, bf16),
            vmem(project.shape, bf16),
            vmem(gate_up.shape, bf16),
            vmem(down.shape, bf16),
            vmem((width, hidden), bf16),
            vmem((width, depth), f32),
            vmem((width, depth), f32),
            vmem((width, depth), bf16),
            vmem((width, depth), bf16),
            vmem((chips, cores, width, depth), bf16),
            vmem((chips, cores, 8 + experts, depth), f32),
            vmem((2, hidden, cores * depth), f32),
            vmem((hidden, cores * depth), bf16),
            vmem((chips, 2 * pieces, piece, depth), bf16),
            vmem((chips, 2 * pieces, piece, depth), bf16),
            vmem((chips, 2 * pieces, piece, depth), bf16),
            vmem((chips, pieces, piece, depth), bf16),
            vmem((chips, pieces, piece, depth), bf16),
            vmem((chips, pieces, piece, depth), bf16),
            vmem((chips, pieces, piece, depth), bf16),
            vmem((chips, pieces, piece, depth), bf16),
            dma((kv_groups + 5,)),
            dma((chips, cores)),
            dma((chips,)),
            dma((chips,)),
            dma((count,)),
            dma((count,)),
            dma((chips, cores, count)),
            dma((chips, count)),
            dma((chips, count)),
            dma((chips, count)),
            dma((chips, count)),
            dma((chips, cores)),
            dma((chips,)),
            dma((chips,)),
            dma((chips,)),
            dma((chips, 2 * pieces)),
            dma((chips, 2 * pieces)),
            dma((chips, pieces)),
            dma((chips, pieces)),
            dma((chips, pieces)),
            dma((chips, pieces)),
            dma((chips, pieces)),
        ],
        compiler_params=pltpu.CompilerParams(
            collective_id=0, has_side_effects=True, vmem_limit_bytes=VMEM_BYTES
        ),
        cost_estimate=pl.CostEstimate(
            flops=flops,
            bytes_accessed=2 * (project.size + gate_up.size + down.size),
            transcendentals=0,
        ),
    )(sinks, ids, route, gain, queries, keys_values, residual, project, gate_up, down)


def per_device_whole(
    queries,
    keys_values,
    sink_logits,
    residual,
    out_weight,
    norm_gain,
    expert_ids,
    route_weights,
    gate_up,
    down_weight,
):
    width = residual.shape[1]
    pairs = lax.axis_size("pair")
    chips = lax.axis_size("tok") // 2
    half = width // 2
    chunk = min(512, half // 128 * 128)
    piece = next(n for n in (480, 240, 160, 80, 48, 32, 16, half) if half % n == 0)
    out = whole_layer(
        (chips, pairs, chunk, piece),
        sink_logits,
        expert_ids.T,
        route_weights.T,
        norm_gain[None, :],
        queries,
        keys_values,
        residual.T,
        out_weight.T,
        jnp.transpose(gate_up[0], (1, 2, 0)),
        down_weight[0],
    )
    return out.T


def solution(mesh):
    placed = (
        P(("groups", "tok"), ("head", "pair")),
        P(("groups", "tok"), ("head", "pair")),
        P(("head", "pair")),
        P(("groups", "tok"), None),
        P(("head", "pair"), None),
        P(),
        P(("groups", "tok"), None),
        P(("groups", "tok"), None),
        P("tok", None, None, ("head", "pair")),
        P("tok", ("head", "pair"), None),
    )
    sizes = mesh.shape
    chip_pair = sizes["pair"] == 1 and sizes["head"] == 2 and sizes["tok"] % 2 == 0
    return jax.shard_map(
        per_device_whole if chip_pair else per_device,
        mesh=mesh,
        in_specs=placed,
        out_specs=P(("groups", "tok"), ("head", "pair")),
        check_vma=False,
    )
```

```python
import functools

import jax
import jax.numpy as jnp
from jax import lax
from jax.experimental import pallas as pl
from jax.experimental.pallas import tpu as pltpu
from jax.sharding import PartitionSpec as P

HEAD_DIM = 64

MESH_ID = pl.DeviceIdType.MESH

VMEM_BYTES = 67_043_328
OWN_LESS = 0
BOTH = 1


def moe_kernel(
    dims,
    parts_ref,
    residual_ref,
    gain_ref,
    tail_ref,
    gate_hbm,
    down_hbm,
    out_ref,
    gate_w,
    down_w,
    rows,
    part,
    from_core,
    kept,
    from_peer,
    hop,
    from_right,
    from_left,
    peer_parts,
    stream,
    squares,
    peer_squares,
    acc,
    parts_send,
    parts_recv,
    squares_send,
    squares_recv,
    load_sem,
    row_recv,
    row_right,
    row_left,
    row_peer,
    row_core,
    part_send,
    part_recv,
    peer_send,
    peer_recv,
    hop_send,
    right_recv,
    left_recv,
):
    chips, cores, shares, pairs, width = dims
    tok = lax.axis_index("tok")
    z = tok // cores
    c = tok % cores
    mine = lax.axis_index("head") * pairs + lax.axis_index("pair")
    other = cores - 1 - c

    def tok_id(chip, core):
        return {"tok": chip * cores + core}

    def peer_id(share):
        return {"head": share // pairs, "pair": share % pairs}

    def remote(src, dst, send, recv, target):
        return pltpu.make_async_remote_copy(
            src_ref=src, dst_ref=dst, send_sem=send, recv_sem=recv,
            device_id=target, device_id_type=MESH_ID,
        )

    loads = [
        pltpu.make_async_copy(gate_hbm, gate_w.at[:, :, pl.ds(0, width)], load_sem.at[0]),
        pltpu.make_async_copy(down_hbm, down_w, load_sem.at[1]),
    ]
    for load in loads:
        load.start()

    barrier = pltpu.get_barrier_semaphore()

    @pl.when(z > 0)
    def _():
        pl.semaphore_signal(barrier, 1, device_id=tok_id(z - 1, c), device_id_type=MESH_ID)

    @pl.when(z < chips - 1)
    def _():
        pl.semaphore_signal(barrier, 1, device_id=tok_id(z + 1, c), device_id_type=MESH_ID)

    if cores > 1:
        pl.semaphore_signal(barrier, 1, device_id=tok_id(z, other), device_id_type=MESH_ID)
    for d in range(1, shares):
        pl.semaphore_signal(
            barrier, 1, device_id=peer_id((mine + d) % shares), device_id_type=MESH_ID
        )
    sides = jnp.where(z > 0, 1, 0) + jnp.where(z < chips - 1, 1, 0)
    pl.semaphore_wait(barrier, sides + (cores - 1) + (shares - 1))

    def parts_copy(d):
        share = (mine + d) % shares
        return remote(
            parts_ref.at[share], peer_parts.at[mine], parts_send.at[d - 1],
            parts_recv.at[mine], peer_id(share),
        )

    def squares_copy(d):
        return remote(
            squares, peer_squares.at[mine], squares_send.at[d - 1],
            squares_recv.at[mine], peer_id((mine + d) % shares),
        )

    for d in range(1, shares):
        parts_copy(d).start()
    gate_w[:, :, width:, :] = jnp.zeros(
        gate_w.shape[:2] + (gate_w.shape[2] - width, gate_w.shape[3]), jnp.bfloat16
    )
    stream[...] = residual_ref[...].astype(jnp.float32) + parts_ref[mine].astype(jnp.float32)
    for d in range(1, shares):
        share = (mine + d) % shares
        slot = peer_parts.at[share]
        pltpu.make_async_copy(slot, slot, parts_recv.at[share]).wait()
        stream[...] += peer_parts[share].astype(jnp.float32)
    own = stream[...]
    square = jnp.sum(own * own, axis=1, keepdims=True)
    squares[...] = jnp.broadcast_to(square, squares.shape)
    for d in range(1, shares):
        squares_copy(d).start()
    total_square = squares[...]
    for d in range(1, shares):
        share = (mine + d) % shares
        slot = peer_squares.at[share]
        pltpu.make_async_copy(slot, slot, squares_recv.at[share]).wait()
        total_square += peer_squares[share]
    inverse = lax.rsqrt(total_square[:, :1] / (shares * width) + 1e-05)
    normed = stream[...] * inverse * gain_ref[...] + tail_ref[...].astype(jnp.float32)
    rows[z, mine, c] = normed.astype(jnp.bfloat16)

    near = jnp.minimum(z, chips - 1 - z)

    def chip_at(i):
        inner = jnp.where(i % 2 == 1, z - (i + 1) // 2, z + i // 2)
        outer = jnp.where(z < chips - 1 - z, i, chips - 1 - i)
        return jnp.where(i <= 2 * near, inner, outer)

    def row_copy(chip, share, core, send, target):
        slot = rows.at[chip, share, core]
        return remote(slot, slot, send, row_recv.at[chip, core, share], target)

    def go_right(chip):
        return (chip <= z) & (z < chips - 1)

    def go_left(chip):
        return (chip >= z) & (z > 0)

    def right_copy(chip):
        return row_copy(chip, mine, c, row_right.at[chip], tok_id(z + 1, c))

    def left_copy(chip):
        return row_copy(chip, mine, c, row_left.at[chip], tok_id(z - 1, c))

    def peer_copy(chip, d):
        return row_copy(chip, mine, c, row_peer.at[chip, d - 1], peer_id((mine + d) % shares))

    def core_copy(chip, share):
        return row_copy(chip, share, c, row_core.at[chip, share], tok_id(z, other))

    def row_wait(chip, share, core):
        slot = rows.at[chip, share, core]
        pltpu.make_async_copy(slot, slot, row_recv.at[chip, core, share]).wait()

    def forward(i):
        chip = chip_at(i)

        @pl.when(go_right(chip))
        def _():
            right_copy(chip).start()

        @pl.when(go_left(chip))
        def _():
            left_copy(chip).start()

        for d in range(1, shares):
            peer_copy(chip, d).start()
        if cores > 1:
            core_copy(chip, mine).start()

    forward(0)
    loads[0].wait()
    loads[1].wait()

    tail = (width // 128) * 128
    wide = rows.shape[-1]
    depth = rows.shape[-2]
    experts = chips * cores
    tail_lane = tail + lax.broadcasted_iota(jnp.int32, (cores * depth, wide - tail), 1)
    weight_lane = (tail_lane == width + tok) | (tail_lane == width + experts + tok)

    def kept_at(chip, share):
        return kept.at[chip, share] if cores > 1 else part.at[chip, share, 0]

    def part_copy(chip, share):
        return remote(
            part.at[chip, share, other], from_core.at[chip, share],
            part_send.at[chip, share], part_recv.at[chip, share], tok_id(z, other),
        )

    def sum_copy(chip, d):
        share = (mine + d) % shares
        return remote(
            kept_at(chip, share), from_peer.at[chip, mine],
            peer_send.at[chip, d - 1], peer_recv.at[chip, mine], peer_id(share),
        )

    def compute(i, carry):
        @pl.when(i + 1 < chips)
        def _():
            row_wait(chip_at(i + 1), mine, c)
            forward(i + 1)

        chip = chip_at(i)
        for d in range(1, shares):
            share = (mine + d) % shares
            row_wait(chip, share, c)
            if cores > 1:
                core_copy(chip, share).start()
        if cores > 1:
            for share in range(shares):
                row_wait(chip, share, other)
        gate = jnp.zeros((cores * depth, gate_w.shape[-1]), jnp.float32)
        up = gate
        for share in range(shares):
            block = rows[chip, share].reshape(cores * depth, wide)
            gate += jnp.dot(block, gate_w[0, share], preferred_element_type=jnp.float32)
            up += jnp.dot(block, gate_w[1, share], preferred_element_type=jnp.float32)
        active = (gate * jax.nn.sigmoid(1.702 * gate) * (up + 1.0)).astype(jnp.bfloat16)
        ends = rows[chip, 0, :, :, tail:].reshape(cores * depth, wide - tail).astype(jnp.float32)
        weight = jnp.sum(jnp.where(weight_lane, ends, 0.0), axis=1, keepdims=True)
        for share in range(shares):
            out = jnp.dot(active, down_w[share], preferred_element_type=jnp.float32)
            out = (out * weight).astype(jnp.bfloat16)
            part[chip, share] = out.reshape(cores, depth, width)
            if cores > 1:
                part_copy(chip, share).start()
        for share in range(shares):
            if cores > 1:
                part_copy(chip, share).wait_recv()
                total = part[chip, share, c].astype(jnp.float32)
                total += from_core[chip, share].astype(jnp.float32)
                kept[chip, share] = total.astype(jnp.bfloat16)
        for d in range(1, shares):
            sum_copy(chip, d).start()
        return carry

    lax.fori_loop(0, chips, compute, 0)

    def right_hop(chip):
        return remote(
            hop.at[chip], from_left.at[chip], hop_send.at[chip], left_recv.at[chip],
            tok_id(z + 1, c),
        )

    def left_hop(chip):
        return remote(
            hop.at[chip], from_right.at[chip], hop_send.at[chip], right_recv.at[chip],
            tok_id(z - 1, c),
        )

    def hop_wait(buffer, sem, chip):
        pltpu.make_async_copy(buffer.at[chip], buffer.at[chip], sem.at[chip]).wait()

    def give_back(j, carry):
        chip = chip_at(chips - 1 - j)
        total = kept_at(chip, mine)[...].astype(jnp.float32)
        for d in range(1, shares):
            share = (mine + d) % shares
            slot = from_peer.at[chip, share]
            pltpu.make_async_copy(slot, slot, peer_recv.at[chip, share]).wait()
            total += from_peer[chip, share].astype(jnp.float32)
        acc[...] = total

        @pl.when((chip <= z) & (z < chips - 1))
        def _():
            hop_wait(from_right, right_recv, chip)
            acc[...] += from_right[chip].astype(jnp.float32)

        @pl.when((chip >= z) & (z > 0))
        def _():
            hop_wait(from_left, left_recv, chip)
            acc[...] += from_left[chip].astype(jnp.float32)

        @pl.when(chip == z)
        def _():
            out_ref[...] = (stream[:, :width] + acc[...]).astype(jnp.bfloat16)

        @pl.when(chip != z)
        def _():
            hop[chip] = acc[...].astype(jnp.bfloat16)

        @pl.when(chip < z)
        def _():
            left_hop(chip).start()

        @pl.when(chip > z)
        def _():
            right_hop(chip).start()

        return carry

    lax.fori_loop(0, chips, give_back, 0)

    def drain(chip, carry):
        @pl.when(go_right(chip))
        def _():
            right_copy(chip).wait_send()

        @pl.when(go_left(chip))
        def _():
            left_copy(chip).wait_send()

        for d in range(1, shares):
            peer_copy(chip, d).wait_send()
            sum_copy(chip, d).wait_send()
        if cores > 1:
            for share in range(shares):
                core_copy(chip, share).wait_send()
                part_copy(chip, share).wait_send()

        @pl.when(chip < z)
        def _():
            left_hop(chip).wait_send()

        @pl.when(chip > z)
        def _():
            right_hop(chip).wait_send()

        return carry

    lax.fori_loop(0, chips, drain, 0)
    for d in range(1, shares):
        parts_copy(d).wait_send()
        squares_copy(d).wait_send()


def moe(dims, parts, residual, gain, tail, gate_w, down_w):
    chips, cores, shares, pairs, width = dims
    depth, wide = residual.shape
    hidden = down_w.shape[1]
    bf16 = jnp.bfloat16
    dma = pltpu.SemaphoreType.DMA
    return pl.pallas_call(
        functools.partial(moe_kernel, dims),
        out_shape=jax.ShapeDtypeStruct((depth, width), jnp.bfloat16),
        in_specs=[pl.BlockSpec(memory_space=pltpu.VMEM)] * 4
        + [
            pl.BlockSpec(memory_space=pl.ANY),
            pl.BlockSpec(memory_space=pl.ANY),
        ],
        out_specs=pl.BlockSpec(memory_space=pltpu.VMEM),
        scratch_shapes=[
            pltpu.VMEM((2, shares, wide, hidden), bf16),
            pltpu.VMEM(down_w.shape, bf16),
            pltpu.VMEM((chips, shares, cores, depth, wide), bf16),
            pltpu.VMEM((chips, shares, cores, depth, width), bf16),
            pltpu.VMEM((chips, shares, depth, width) if cores > 1 else (8, 128), bf16),
            pltpu.VMEM((chips, shares, depth, width) if cores > 1 else (8, 128), bf16),
            pltpu.VMEM((chips, shares, depth, width), bf16),
            pltpu.VMEM((chips, depth, width), bf16),
            pltpu.VMEM((chips, depth, width), bf16),
            pltpu.VMEM((chips, depth, width), bf16),
            pltpu.VMEM((shares, depth, wide), bf16),
            pltpu.VMEM((depth, wide), jnp.float32),
            pltpu.VMEM((depth, 128), jnp.float32),
            pltpu.VMEM((shares, depth, 128), jnp.float32),
            pltpu.VMEM((depth, width), jnp.float32),
            dma((max(shares - 1, 1),)),
            dma((shares,)),
            dma((max(shares - 1, 1),)),
            dma((shares,)),
            dma((2,)),
            dma((chips, cores, shares)),
            dma((chips,)),
            dma((chips,)),
            dma((chips, max(shares - 1, 1))),
            dma((chips, shares)),
            dma((chips, shares)),
            dma((chips, shares)),
            dma((chips, max(shares - 1, 1))),
            dma((chips, shares)),
            dma((chips,)),
            dma((chips,)),
            dma((chips,)),
        ],
        compiler_params=pltpu.CompilerParams(
            collective_id=0, has_side_effects=True, vmem_limit_bytes=60 * 1024 * 1024
        ),
        cost_estimate=pl.CostEstimate(
            flops=6 * chips * cores * depth * shares * width * hidden,
            bytes_accessed=6 * shares * width * hidden,
            transcendentals=0,
        ),
    )(parts, residual, gain, tail, gate_w, down_w)


def per_device(
    queries,
    keys_values,
    sink_logits,
    residual,
    out_weight,
    norm_gain,
    expert_ids,
    route_weights,
    gate_up,
    down_weight,
):
    tok_rows = queries.shape[0]
    kv_groups = keys_values.shape[1] // (2 * HEAD_DIM)
    local_heads = queries.shape[1] // HEAD_DIM
    repeat = local_heads // kv_groups
    position = lax.axis_index("tok") * tok_rows + jnp.arange(tok_rows, dtype=jnp.int32)
    grouped = queries.reshape(tok_rows, kv_groups, repeat, HEAD_DIM)
    start_max = jnp.broadcast_to(
        sink_logits.reshape(kv_groups, repeat)[:, :, None], (kv_groups, repeat, tok_rows)
    )
    start_totals = jnp.ones((kv_groups, repeat, tok_rows), jnp.float32)
    start_accum = jnp.zeros((kv_groups, repeat, tok_rows, HEAD_DIM), jnp.float32)
    key_piece = lax.all_gather(keys_values, "tok", axis=0, tiled=True)
    hidden = down_weight.shape[1]
    shares = lax.axis_size(("head", "pair"))
    share = out_weight.shape[1] // shares
    gate_w = jnp.transpose(gate_up[0], (1, 0, 2)).reshape(2, shares, share, hidden)
    down_w = jnp.transpose(down_weight[0].reshape(hidden, shares, share), (1, 0, 2))
    key_piece, gate_w, down_w = lax.optimization_barrier((key_piece, gate_w, down_w))
    totals = start_totals
    accum = start_accum
    count = key_piece.shape[0]
    split_piece = key_piece.reshape(count, kv_groups, 2, HEAD_DIM)
    scores = (
        jnp.einsum(
            "tgrd,ngd->grtn", grouped, split_piece[:, :, 0], preferred_element_type=jnp.float32
        )
        * 0.125
    )
    key_position = jnp.arange(count, dtype=jnp.int32)
    allowed = key_position[None, :] <= position[:, None]
    scores = jnp.where(allowed, scores, jnp.float32(-1e30))
    new_max = jnp.maximum(start_max, jnp.max(scores, axis=-1))
    decay = jnp.exp(start_max - new_max)
    weights = jnp.exp(scores - new_max[..., None])
    totals = totals * decay + jnp.sum(weights, axis=-1)
    update = jnp.einsum(
        "grtn,ngd->grtd",
        weights.astype(jnp.bfloat16),
        split_piece[:, :, 1],
        preferred_element_type=jnp.float32,
    )
    accum = accum * decay[..., None] + update
    final_max, totals, accum = (new_max, totals, accum)
    attended = (accum / totals[..., None]).astype(jnp.bfloat16)
    attended = jnp.transpose(attended, (2, 0, 1, 3)).reshape(tok_rows, local_heads * HEAD_DIM)
    width = out_weight.shape[1]
    share = width // lax.axis_size(("head", "pair"))
    column_start = lax.axis_index(("head", "pair")) * share
    partial_value = jnp.dot(attended, out_weight, preferred_element_type=jnp.float32)
    experts = lax.axis_size("tok")
    pairs = lax.axis_size("pair")
    cores = 2 // pairs
    shares = width // share
    wide = -(-(share + 2 * experts) // 128) * 128
    expert = jnp.arange(experts, dtype=jnp.int32)
    routed = expert_ids[:, :, None] == expert
    dense = jnp.sum(jnp.where(routed, route_weights[:, :, None], 0.0), axis=1)
    high = lax.reduce_precision(dense, 8, 7)
    weights = jnp.concatenate([high, dense - high], axis=1).astype(jnp.bfloat16)
    tail = jnp.pad(weights, ((0, 0), (share, wide - share - 2 * experts)))
    spare = (0, wide - share)
    parts = jnp.transpose(
        partial_value.astype(jnp.bfloat16).reshape(tok_rows, shares, share), (1, 0, 2)
    )
    parts = jnp.pad(parts, ((0, 0), (0, 0), spare))
    own_residual = jnp.pad(
        lax.dynamic_slice_in_dim(residual, column_start, share, 1), ((0, 0), spare)
    )
    own_gain = jnp.pad(lax.dynamic_slice_in_dim(norm_gain, column_start, share, 0), spare)
    return moe(
        (experts // cores, cores, shares, pairs, share),
        parts, own_residual, own_gain[None, :], tail, gate_w, down_w,
    )


def layer_kernel(
    dims,
    sink_ref,
    ids_ref,
    route_ref,
    gain_ref,
    query_hbm,
    kv_hbm,
    residual_hbm,
    project_hbm,
    gate_hbm,
    down_hbm,
    out_ref,
    query_v,
    query_t,
    kvs,
    row_max,
    row_total,
    accum,
    attended,
    residual_v,
    project_w,
    gate_w,
    down_v,
    down_t,
    gain_cols,
    stream,
    parts,
    peer_parts,
    rows,
    meta,
    hidden,
    active,
    part,
    kept,
    from_core,
    cross,
    from_peer,
    hop,
    inbox,
    closing,
    from_closing,
    acc,
    squares,
    peer_squares,
    load_sem,
    kv_recv,
    kv_core_send,
    kv_up_send,
    parts_send,
    parts_recv,
    squares_sem,
    row_recv,
    row_up,
    row_down,
    row_core,
    row_peer,
    meta_recv,
    meta_up,
    meta_down,
    meta_core,
    part_send,
    part_recv,
    peer_send,
    peer_recv,
    hop_send,
    inbox_recv,
    closing_send,
    closing_recv,
):
    chips, pairs, chunk, piece, own, both = dims
    cores = 2
    width, depth = residual_hbm.shape
    kv_groups = kvs.shape[1]
    repeat = query_t.shape[2] // depth
    half = width // 2
    f32, bf16 = jnp.float32, jnp.bfloat16
    far = (width - own * chunk) // 128 * 128
    edges = [(at, min(chunk, far - at)) for at in range(own * chunk, far, chunk)]
    if far + own * chunk < width:
        edges.append((far + own * chunk, width - far - own * chunk))
    spread_over = [(2 * own + n, at, size) for n, (at, size) in enumerate(edges)]
    pieces = half // piece
    last = chips - 1

    tok = lax.axis_index("tok")
    z = tok // cores
    c = tok % cores
    x = lax.axis_index("head") * pairs + lax.axis_index("pair")
    peer = {"head": (1 - x) // pairs, "pair": (1 - x) % pairs}
    other = {"tok": z * cores + (1 - c)}
    above = {"tok": (z + 1) * cores + c}
    below = {"tok": (z - 1) * cores + c}

    def remote(src, dst, send, recv, target):
        return pltpu.make_async_remote_copy(
            src_ref=src, dst_ref=dst, send_sem=send, recv_sem=recv,
            device_id=target, device_id_type=MESH_ID,
        )

    def landed(slot, sem):
        pltpu.make_async_copy(slot, slot, sem).wait()

    def mult(value, of):
        return pl.multiple_of(value, of)

    loads = [
        pltpu.make_async_copy(
            kv_hbm.at[:, pl.ds(g * 2 * HEAD_DIM, 2 * HEAD_DIM)], kvs.at[tok, g], load_sem.at[g]
        )
        for g in range(kv_groups)
    ]
    bulk = [
        pltpu.make_async_copy(src, dst, load_sem.at[kv_groups + i])
        for i, (src, dst) in enumerate(
            [
                (query_hbm, query_v),
                (residual_hbm, residual_v),
                (project_hbm, project_w),
                (down_hbm, down_v),
                (gate_hbm, gate_w),
            ]
        )
    ]
    for load in loads + bulk:
        load.start()

    barrier = pltpu.get_barrier_semaphore()

    @pl.when(z > 0)
    def _():
        pl.semaphore_signal(barrier, 1, device_id=below, device_id_type=MESH_ID)

    @pl.when(z < last)
    def _():
        pl.semaphore_signal(barrier, 1, device_id=above, device_id_type=MESH_ID)

    pl.semaphore_signal(barrier, 1, device_id=other, device_id_type=MESH_ID)
    pl.semaphore_signal(barrier, 1, device_id=peer, device_id_type=MESH_ID)
    sides = jnp.where(z > 0, 1, 0) + jnp.where(z < last, 1, 0)
    pl.semaphore_wait(barrier, sides + 2)

    def kv_up(chip):
        slot = kvs.at[chip * cores + c]
        return remote(slot, slot, kv_up_send.at[chip], kv_recv.at[chip, c], above)

    def kv_core(chip):
        slot = kvs.at[chip * cores + c]
        return remote(slot, slot, kv_core_send.at[chip], kv_recv.at[chip, c], other)

    def kv_wait(chip, core):
        landed(kvs.at[chip * cores + core], kv_recv.at[chip, core])

    def kv_pass(chip):
        @pl.when(z < last)
        def _():
            kv_up(chip).start()

        kv_core(chip).start()

    for load in loads:
        load.wait()
    kv_pass(z)

    for b in range(-(-width // 128)):
        size = min(128, width - b * 128)
        gain = gain_ref[:, b * 128:b * 128 + size]
        gain_cols[b * 128:b * 128 + size, :] = jnp.broadcast_to(gain, (128, size)).T

    bulk[0].wait()
    for g in range(kv_groups):
        query_t[g, HEAD_DIM:, :] = jnp.zeros((HEAD_DIM, repeat * depth), bf16)
        for m in range(repeat // 2):
            lane = (g * repeat + 2 * m) * HEAD_DIM
            turned = (query_v[:, lane:lane + 2 * HEAD_DIM].astype(f32) * 0.125).T.astype(bf16)
            query_t[g, :HEAD_DIM, 2 * m * depth:(2 * m + 1) * depth] = turned[:HEAD_DIM]
            query_t[g, :HEAD_DIM, (2 * m + 1) * depth:(2 * m + 2) * depth] = turned[HEAD_DIM:]
        for r in range(repeat):
            row_max[g, :, r * depth:(r + 1) * depth] = jnp.full(
                (1, depth), sink_ref[g * repeat + r], f32
            )
    row_total[...] = jnp.ones(row_total.shape, f32)
    accum[...] = jnp.zeros(accum.shape, f32)

    def attend(chip, g, masked):
        keys = kvs[pl.ds(chip * cores, cores), g].reshape(cores * depth, 2 * HEAD_DIM)
        values = keys.astype(f32).T[HEAD_DIM:].astype(bf16)
        olds, totals, sums = row_max[g], row_total[g], accum[g]
        lanes = [slice(2 * m * depth, (2 * m + 2) * depth) for m in range(repeat // 2)]
        scores = [
            jnp.dot(keys, query_t[g, :, lane], preferred_element_type=f32) for lane in lanes
        ]
        if masked:
            row = lax.broadcasted_iota(jnp.int32, scores[0].shape, 0)
            column = lax.broadcasted_iota(jnp.int32, scores[0].shape, 1)
            column = jnp.where(column >= depth, column - depth, column)
            allowed = row <= c * depth + column
            scores = [jnp.where(allowed, score, jnp.float32(-1e30)) for score in scores]
        news = [
            jnp.maximum(olds[:, lane], jnp.max(score, axis=0, keepdims=True))
            for lane, score in zip(lanes, scores)
        ]
        weights = [jnp.exp(score - new) for score, new in zip(scores, news)]
        added = [
            jnp.dot(values, weight.astype(bf16), preferred_element_type=f32) for weight in weights
        ]
        for lane, new, weight, more in zip(lanes, news, weights, added):
            decay = jnp.exp(olds[:, lane] - new)
            row_max[g, :, lane] = new
            row_total[g, :, lane] = totals[:, lane] * decay + jnp.sum(
                weight, axis=0, keepdims=True
            )
            accum[g, :, lane] = sums[:, lane] * decay + more

    def attend_chip(chip, masked):
        kv_wait(chip, 1 - c)

        def group(g, carry):
            attend(chip, g, masked)
            return carry

        lax.fori_loop(0, kv_groups // 2, group, 0)

        @pl.when(chip > 0)
        def _():
            kv_wait(chip - 1, c)
            kv_pass(chip - 1)

        lax.fori_loop(kv_groups // 2, kv_groups, group, 0)

    attend_chip(z, True)

    def earlier(i, carry):
        attend_chip(z - i, False)
        return carry

    lax.fori_loop(1, z + 1, earlier, 0)

    for g in range(kv_groups):
        inverse = 1.0 / row_total[g]
        for r in range(repeat):
            lanes = slice(r * depth, (r + 1) * depth)
            head = (g * repeat + r) * HEAD_DIM
            attended[head:head + HEAD_DIM, :] = (accum[g, :, lanes] * inverse[:, lanes]).astype(bf16)

    def own_at(side, t):
        return mult(side * far + t * chunk, 128)

    def own_id(side, t):
        return side * own + t

    def parts_copy(n, start, size):
        return remote(
            parts.at[pl.ds(start, size)], peer_parts.at[pl.ds(start, size)],
            parts_send.at[n], parts_recv.at[n], peer,
        )

    def project(start, size):
        return jnp.dot(
            project_w[pl.ds(start, size), :], attended[...], preferred_element_type=f32
        )

    def give(n, start, size):
        value = project(start, size)
        parts[pl.ds(start, size), :] = value.astype(bf16)
        parts_copy(n, start, size).start()
        return value

    def hold(start, size, value):
        at = pl.ds(start, size)
        stream[at, :] = value + residual_v[at, :].astype(f32)

    def row_copy(chip, k, start, size, send, target):
        slot = rows.at[chip, c, pl.ds(start, size)]
        return remote(slot, slot, send.at[chip, k], row_recv.at[chip, c, k], target)

    def row_wait(chip, core, k, start, size):
        landed(rows.at[chip, core, pl.ds(start, size)], row_recv.at[chip, core, k])

    def pass_along(chip, k, start, size):
        @pl.when((chip <= z) & (z < last))
        def _():
            row_copy(chip, k, start, size, row_up, above).start()

        @pl.when((chip >= z) & (z > 0))
        def _():
            row_copy(chip, k, start, size, row_down, below).start()

    def meta_copy(chip, send, target):
        slot = meta.at[chip, c]
        return remote(slot, slot, send.at[chip], meta_recv.at[chip, c], target)

    def meta_wait(chip, core):
        landed(meta.at[chip, core], meta_recv.at[chip, core])

    def pass_meta(chip):
        @pl.when((chip <= z) & (z < last))
        def _():
            meta_copy(chip, meta_up, above).start()

        @pl.when((chip >= z) & (z > 0))
        def _():
            meta_copy(chip, meta_down, below).start()

        meta_copy(chip, meta_core, other).start()

    def settle(n, k, start, size):
        at = pl.ds(start, size)
        landed(peer_parts.at[at], parts_recv.at[n])
        value = stream[at, :] + peer_parts[at, :].astype(f32)
        stream[at, :] = value
        rows[z, c, at, :] = (value * gain_cols[at, :]).astype(bf16)
        pass_along(z, k, start, size)
        row_copy(z, k, start, size, row_core, other).start()
        return jnp.sum((value * value).reshape(size // 8, 8, depth), axis=0)

    bulk[1].wait()
    bulk[2].wait()
    for t in range(own):
        give(t, own_at(1 - x, t), chunk)
    squares_own = jnp.zeros((8, depth), f32)
    squares_all = jnp.zeros((8, depth), f32)
    for t in range(own):
        hold(own_at(x, t), chunk, project(own_at(x, t), chunk))
        for n, (k, start, size) in enumerate(spread_over):
            if t == 0:
                hold(start, size, give(own + n, start, size))
        squares_own += settle(t, own_id(x, t), own_at(x, t), chunk)
    squares[...] = squares_own
    squares_copy = remote(squares, peer_squares, squares_sem.at[0], squares_sem.at[1], peer)
    squares_copy.start()

    experts = chips * cores
    expert = lax.broadcasted_iota(jnp.int32, (experts, depth), 0)
    dense = jnp.zeros((experts, depth), f32)
    for k in range(ids_ref.shape[0]):
        dense += jnp.where(ids_ref[k:k + 1, :] == expert, route_ref[k:k + 1, :], 0.0)
    meta[z, c, pl.ds(8, experts), :] = dense
    bulk[3].wait()

    def turn(b, carry):
        at = pl.ds(mult(b * 128, 128), 128)
        down_t[at, :] = down_v[:, at].astype(f32).T.astype(bf16)
        return carry

    turns = width // 128
    if width % 128:
        at = pl.ds(turns * 128, width % 128)
        down_t[at, :] = down_v[:, at].astype(f32).T.astype(bf16)
    for n, (k, start, size) in enumerate(spread_over):
        if n < 2:
            lax.fori_loop(n * turns // 2, (n + 1) * turns // 2, turn, 0)
        squares_all += settle(own + n, k, start, size)
    if len(spread_over) < 2:
        lax.fori_loop(len(spread_over) * turns // 2, turns, turn, 0)
    landed(peer_squares, squares_sem.at[1])
    squares_all += squares[...] + peer_squares[...]
    total = jnp.sum(squares_all, axis=0, keepdims=True)
    scale = lax.rsqrt(total / width + 1e-05)
    meta[z, c, 0:8, :] = jnp.broadcast_to(scale, (8, depth))
    pass_meta(z)

    near = jnp.minimum(z, last - z)

    def chip_at(i):
        inner = jnp.where(i % 2 == 1, z - (i + 1) // 2, z + i // 2)
        outer = jnp.where(z < last - z, i, last - i)
        return jnp.where(i <= 2 * near, inner, outer)

    def each_side(i, act):
        @pl.when(z - 1 - i >= 0)
        def _():
            act(z - 1 - i)

        @pl.when(z + 1 + i <= last)
        def _():
            act(z + 1 + i)

    def pump(i, k, start, size, crosses):
        def act(chip):
            row_wait(chip, c, k, start, size)
            pass_along(chip, k, start, size)
            if crosses:
                row_copy(chip, k, start, size, row_peer, peer).start()
            row_copy(chip, k, start, size, row_core, other).start()

        each_side(i, act)

    def pump_all(i):
        def one(t, carry):
            pump(i, own_id(x, t), own_at(x, t), chunk, True)
            return carry

        lax.fori_loop(0, own, one, 0)
        for k, start, size in spread_over:
            pump(i, k, start, size, False)

        def act(chip):
            meta_wait(chip, c)
            pass_meta(chip)

        each_side(i, act)

    def cross_in(chip):
        def one(t, carry):
            k, start = own_id(1 - x, t), own_at(1 - x, t)
            row_wait(chip, c, k, start, chunk)
            row_copy(chip, k, start, chunk, row_core, other).start()
            return carry

        lax.fori_loop(0, own, one, 0)

    def multiply(chip, k, start, size):
        row_wait(chip, 1 - c, k, start, size)
        at = pl.ds(start, size)
        pair = jnp.concatenate([rows[chip, c, at, :], rows[chip, 1 - c, at, :]], axis=1)
        for side in range(2):
            hidden[side] += jnp.dot(gate_w[side, :, at], pair, preferred_element_type=f32)

    def multiply_line(chip):
        hidden[...] = jnp.zeros(hidden.shape, f32)

        def one(t, carry):
            multiply(chip, own_id(x, t), own_at(x, t), chunk)
            return carry

        lax.fori_loop(0, own, one, 0)
        for k, start, size in spread_over:
            multiply(chip, k, start, size)

    def multiply_crossed(chip):
        def one(t, carry):
            multiply(chip, own_id(1 - x, t), own_at(1 - x, t), chunk)
            return carry

        lax.fori_loop(0, own, one, 0)

    def part_copy(chip, r):
        return remote(
            part.at[chip, r], from_core.at[chip, r], part_send.at[chip, r],
            part_recv.at[chip, r], other,
        )

    def cross_copy(chip, r):
        return remote(
            cross.at[chip, r], from_peer.at[chip, r], peer_send.at[chip, r],
            peer_recv.at[chip, r], peer,
        )

    def hop_copy(way, chip, u):
        return remote(
            hop.at[chip, u], inbox.at[way, chip, u], hop_send.at[chip, u],
            inbox_recv.at[way, chip, u], {"tok": tok + cores * (1 - 2 * way)},
        )

    def last_copy(u):
        return remote(
            closing.at[u], from_closing.at[u], closing_send.at[u], closing_recv.at[u], peer
        )

    def piece_of(u):
        return jnp.where(u < both, (1 - x) * pieces + u, x * pieces + u - both)

    slots = pieces + both
    nearer = jnp.where(z < last - z, 0, 1)

    def hops(i, ends):
        def toward(turn_of, carry):
            way = jnp.where(nearer == 0, turn_of, 1 - turn_of)
            chip = jnp.where(way == 0, i, last - i)
            incoming = jnp.where(way == 0, z, last - z) > 0
            sends = jnp.where(way == 0, chip - z, z - chip) > 0
            if ends is not None:
                sends = sends & (incoming != ends)

            def one(u, carry):
                at = piece_of(u)
                @pl.when(u >= 2 * both)
                def _():
                    r = jnp.maximum(u - 2 * both, 0)
                    landed(from_peer.at[chip, r], peer_recv.at[chip, r])
                    acc[...] = kept[chip, at].astype(f32) + from_peer[chip, r].astype(f32)

                @pl.when(u < 2 * both)
                def _():
                    acc[...] = kept[chip, at].astype(f32)

                @pl.when(incoming)
                def _():
                    landed(inbox.at[way, chip, u], inbox_recv.at[way, chip, u])
                    acc[...] += inbox[way, chip, u].astype(f32)

                hop[chip, u] = acc[...].astype(bf16)
                hop_copy(way, chip, u).start()
                return carry

            @pl.when(sends)
            def _():
                lax.fori_loop(0, slots, one, 0)

            return carry

        lax.fori_loop(0, 2, toward, 0)

    def finish_rows(chip, between=None):
        meta_wait(chip, 1 - c)
        scale = jnp.concatenate([meta[chip, c, 0:1, :], meta[chip, 1 - c, 0:1, :]], axis=1)
        weight = jnp.concatenate(
            [meta[chip, c, pl.ds(8 + tok, 1), :], meta[chip, 1 - c, pl.ds(8 + tok, 1), :]], axis=1
        )
        gate = hidden[0] * scale
        up = hidden[1] * scale
        active[...] = (gate * jax.nn.sigmoid(1.702 * gate) * (up + 1.0) * weight).astype(bf16)

        def spread(r, carry):
            at = jnp.where(r < pieces, (1 - x) * pieces + r, x * pieces + r - pieces)
            value = jnp.dot(
                down_t[pl.ds(mult(at * piece, piece), piece), :], active[...],
                preferred_element_type=f32,
            )
            part[chip, at] = value[:, depth:].astype(bf16)
            part_copy(chip, at).start()
            kept[chip, at] = value[:, :depth].astype(bf16)
            return carry

        lax.fori_loop(0, 2 * pieces, spread, 0)
        if between is not None:
            between()

        def join(r, carry):
            at = (1 - x) * pieces + r
            landed(from_core.at[chip, at], part_recv.at[chip, at])
            value = kept[chip, at].astype(f32) + from_core[chip, at].astype(f32)

            @pl.when(r >= both)
            def _():
                cross[chip, jnp.maximum(r - both, 0)] = value.astype(bf16)
                cross_copy(chip, jnp.maximum(r - both, 0)).start()

            @pl.when(r < both)
            def _():
                kept[chip, at] = value.astype(bf16)

            return carry

        lax.fori_loop(0, pieces, join, 0)

        def keep(r, carry):
            at = x * pieces + r
            landed(from_core.at[chip, at], part_recv.at[chip, at])
            value = kept[chip, at].astype(f32) + from_core[chip, at].astype(f32)
            kept[chip, at] = value.astype(bf16)
            return carry

        lax.fori_loop(0, pieces, keep, 0)

    is_end = (z == 0) | (z == last)

    def own_block():
        multiply_line(z)
        cross_in(z)
        multiply_crossed(z)
        finish_rows(z)

    bulk[4].wait()
    pump_all(0)

    def step(i, carry):
        chip = chip_at(i)
        multiply_line(chip)
        each_side(i - 1, cross_in)
        multiply_crossed(chip)

        @pl.when(jnp.logical_not(is_end))
        def _():
            pump_all(i)

        @pl.when(i > 1)
        def _():
            hops(i - 1, True)

        def between():
            @pl.when(is_end)
            def _():
                pump_all(i)

            @pl.when(i == jnp.where(is_end, last, 1))
            def _():
                for t in range(own):
                    row_copy(z, own_id(x, t), own_at(x, t), chunk, row_peer, peer).start()

        finish_rows(chip, between)
        return carry

    lax.fori_loop(1, chips, step, 0)

    @pl.when(jnp.logical_not(is_end))
    def _():
        own_block()

    for i in range(1, last):
        hops(i, False)
    hops(last, None)

    @pl.when(is_end)
    def _():
        own_block()

    def from_line(u):
        acc[...] = kept[z, piece_of(u)].astype(f32)

        @pl.when(z > 0)
        def _():
            landed(inbox.at[0, z, u], inbox_recv.at[0, z, u])
            acc[...] += inbox[0, z, u].astype(f32)

        @pl.when(z < last)
        def _():
            landed(inbox.at[1, z, u], inbox_recv.at[1, z, u])
            acc[...] += inbox[1, z, u].astype(f32)

    def closes(u, carry):
        from_line(u)
        closing[u] = acc[...].astype(bf16)
        last_copy(u).start()
        return carry

    lax.fori_loop(0, both, closes, 0)

    def finish(r, carry):
        p = jnp.where(r < pieces - both, r + both, r - (pieces - both))
        at = pl.ds(mult(x * half + p * piece, 16), piece)
        from_line(p + both)

        @pl.when(p >= both)
        def _():
            q = jnp.maximum(p - both, 0)
            landed(from_peer.at[z, q], peer_recv.at[z, q])
            acc[...] += from_peer[z, q].astype(f32)

        if both:
            @pl.when(p < both)
            def _():
                q = jnp.minimum(p, both - 1)
                landed(from_closing.at[q], closing_recv.at[q])
                acc[...] += from_closing[q].astype(f32)

        out_ref[pl.ds(mult(p * piece, piece), piece), :] = (stream[at, :] + acc[...]).astype(bf16)
        return carry

    lax.fori_loop(0, pieces, finish, 0)

    def drain(chip, carry):
        @pl.when(chip <= z)
        def _():
            kv_core(chip).wait_send()

        @pl.when((chip <= z) & (z < last))
        def _():
            kv_up(chip).wait_send()

        def sent(k, start, size, on_line, crosses):
            if on_line:
                @pl.when((chip <= z) & (z < last))
                def _():
                    row_copy(chip, k, start, size, row_up, above).wait_send()

                @pl.when((chip >= z) & (z > 0))
                def _():
                    row_copy(chip, k, start, size, row_down, below).wait_send()

            if crosses:
                row_copy(chip, k, start, size, row_peer, peer).wait_send()

            row_copy(chip, k, start, size, row_core, other).wait_send()

        for t in range(own):
            sent(own_id(x, t), own_at(x, t), chunk, True, True)
            sent(own_id(1 - x, t), own_at(1 - x, t), chunk, False, False)
        for k, start, size in spread_over:
            sent(k, start, size, True, False)

        @pl.when((chip <= z) & (z < last))
        def _():
            meta_copy(chip, meta_up, above).wait_send()

        @pl.when((chip >= z) & (z > 0))
        def _():
            meta_copy(chip, meta_down, below).wait_send()

        meta_copy(chip, meta_core, other).wait_send()
        for r in range(2 * pieces):
            part_copy(chip, r).wait_send()
        for r in range(pieces - both):
            cross_copy(chip, r).wait_send()
        for u in range(slots):
            @pl.when(chip > z)
            def _():
                hop_copy(0, chip, u).wait_send()

            @pl.when(chip < z)
            def _():
                hop_copy(1, chip, u).wait_send()

        return carry

    lax.fori_loop(0, chips, drain, 0)
    for t in range(own):
        parts_copy(t, own_at(1 - x, t), chunk).wait_send()
    for n, (k, start, size) in enumerate(spread_over):
        parts_copy(own + n, start, size).wait_send()
    squares_copy.wait_send()
    for u in range(both):
        last_copy(u).wait_send()


def whole_layer(
    dims, sinks, ids, route, gain, queries, keys_values, residual, project, gate_up, down
):
    chips, pairs, chunk, piece, own, both = dims
    cores = 2
    width, depth = residual.shape
    kv_groups = keys_values.shape[1] // (2 * HEAD_DIM)
    heads = queries.shape[1] // HEAD_DIM
    repeat = heads // kv_groups
    hidden = down.shape[0]
    half = width // 2
    pieces = half // piece
    count = -(-width // chunk) + 2
    bf16, f32 = jnp.bfloat16, jnp.float32
    dma = pltpu.SemaphoreType.DMA
    vmem = pltpu.VMEM
    experts = chips * cores
    flops = 2 * width * (
        depth * heads * HEAD_DIM + chips * cores * depth * 3 * hidden
    )
    return pl.pallas_call(
        functools.partial(layer_kernel, dims),
        out_shape=jax.ShapeDtypeStruct((half, depth), bf16),
        in_specs=[pl.BlockSpec(memory_space=pltpu.SMEM)]
        + [pl.BlockSpec(memory_space=pltpu.VMEM)] * 3
        + [pl.BlockSpec(memory_space=pl.ANY)] * 6,
        out_specs=pl.BlockSpec(memory_space=pltpu.VMEM),
        scratch_shapes=[
            vmem(queries.shape, bf16),
            vmem((kv_groups, 2 * HEAD_DIM, repeat * depth), bf16),
            vmem((experts, kv_groups, depth, 2 * HEAD_DIM), bf16),
            vmem((kv_groups, 1, repeat * depth), f32),
            vmem((kv_groups, 1, repeat * depth), f32),
            vmem((kv_groups, HEAD_DIM, repeat * depth), f32),
            vmem((heads * HEAD_DIM, depth), bf16),
            vmem(residual.shape, bf16),
            vmem(project.shape, bf16),
            vmem(gate_up.shape, bf16),
            vmem(down.shape, bf16),
            vmem((width, hidden), bf16),
            vmem((width, depth), f32),
            vmem((width, depth), f32),
            vmem((width, depth), bf16),
            vmem((width, depth), bf16),
            vmem((chips, cores, width, depth), bf16),
            vmem((chips, cores, 8 + experts, depth), f32),
            vmem((2, hidden, cores * depth), f32),
            vmem((hidden, cores * depth), bf16),
            vmem((chips, 2 * pieces, piece, depth), bf16),
            vmem((chips, 2 * pieces, piece, depth), bf16),
            vmem((chips, 2 * pieces, piece, depth), bf16),
            vmem((chips, max(pieces - both, 1), piece, depth), bf16),
            vmem((chips, max(pieces - both, 1), piece, depth), bf16),
            vmem((chips, pieces + both, piece, depth), bf16),
            vmem((2, chips, pieces + both, piece, depth), bf16),
            vmem((max(both, 1), piece, depth), bf16),
            vmem((max(both, 1), piece, depth), bf16),
            vmem((piece, depth), f32),
            vmem((8, depth), f32),
            vmem((8, depth), f32),
            dma((kv_groups + 5,)),
            dma((chips, cores)),
            dma((chips,)),
            dma((chips,)),
            dma((count,)),
            dma((count,)),
            dma((2,)),
            dma((chips, cores, count)),
            dma((chips, count)),
            dma((chips, count)),
            dma((chips, count)),
            dma((chips, count)),
            dma((chips, cores)),
            dma((chips,)),
            dma((chips,)),
            dma((chips,)),
            dma((chips, 2 * pieces)),
            dma((chips, 2 * pieces)),
            dma((chips, max(pieces - both, 1))),
            dma((chips, max(pieces - both, 1))),
            dma((chips, pieces + both)),
            dma((2, chips, pieces + both)),
            dma((max(both, 1),)),
            dma((max(both, 1),)),
        ],
        compiler_params=pltpu.CompilerParams(
            collective_id=0, has_side_effects=True, vmem_limit_bytes=VMEM_BYTES
        ),
        cost_estimate=pl.CostEstimate(
            flops=flops,
            bytes_accessed=2 * (project.size + gate_up.size + down.size),
            transcendentals=0,
        ),
    )(sinks, ids, route, gain, queries, keys_values, residual, project, gate_up, down)


def per_device_whole(
    queries,
    keys_values,
    sink_logits,
    residual,
    out_weight,
    norm_gain,
    expert_ids,
    route_weights,
    gate_up,
    down_weight,
):
    width = residual.shape[1]
    pairs = lax.axis_size("pair")
    chips = lax.axis_size("tok") // 2
    half = width // 2
    chunk = min(512, half // 128 * 128)
    piece = next(n for n in (480, 240, 160, 80, 48, 32, 16, half) if half % n == 0)
    own = max(width // chunk // 2 - OWN_LESS, 1)
    both = min(BOTH, half // piece - 1)
    out = whole_layer(
        (chips, pairs, chunk, piece, own, both),
        sink_logits,
        expert_ids.T,
        route_weights.T,
        norm_gain[None, :],
        queries,
        keys_values,
        residual.T,
        out_weight.T,
        jnp.transpose(gate_up[0], (1, 2, 0)),
        down_weight[0],
    )
    return out.T


def solution(mesh):
    placed = (
        P(("groups", "tok"), ("head", "pair")),
        P(("groups", "tok"), ("head", "pair")),
        P(("head", "pair")),
        P(("groups", "tok"), None),
        P(("head", "pair"), None),
        P(),
        P(("groups", "tok"), None),
        P(("groups", "tok"), None),
        P("tok", None, None, ("head", "pair")),
        P("tok", ("head", "pair"), None),
    )
    sizes = mesh.shape
    chip_pair = sizes["pair"] == 1 and sizes["head"] == 2 and sizes["tok"] % 2 == 0
    return jax.shard_map(
        per_device_whole if chip_pair else per_device,
        mesh=mesh,
        in_specs=placed,
        out_specs=P(("groups", "tok"), ("head", "pair")),
        check_vma=False,
    )
```

```python
import functools

import jax
import jax.numpy as jnp
from jax import lax
from jax.experimental import pallas as pl
from jax.experimental.pallas import tpu as pltpu
from jax.sharding import PartitionSpec as P

HEAD_DIM = 64

MESH_ID = pl.DeviceIdType.MESH

VMEM_BYTES = 67_043_328
OWN_LESS = 0
BOTH = 0


def moe_kernel(
    dims,
    parts_ref,
    residual_ref,
    gain_ref,
    tail_ref,
    gate_hbm,
    down_hbm,
    out_ref,
    gate_w,
    down_w,
    rows,
    part,
    from_core,
    kept,
    from_peer,
    hop,
    from_right,
    from_left,
    peer_parts,
    stream,
    squares,
    peer_squares,
    acc,
    parts_send,
    parts_recv,
    squares_send,
    squares_recv,
    load_sem,
    row_recv,
    row_right,
    row_left,
    row_peer,
    row_core,
    part_send,
    part_recv,
    peer_send,
    peer_recv,
    hop_send,
    right_recv,
    left_recv,
):
    chips, cores, shares, pairs, width = dims
    tok = lax.axis_index("tok")
    z = tok // cores
    c = tok % cores
    mine = lax.axis_index("head") * pairs + lax.axis_index("pair")
    other = cores - 1 - c

    def tok_id(chip, core):
        return {"tok": chip * cores + core}

    def peer_id(share):
        return {"head": share // pairs, "pair": share % pairs}

    def remote(src, dst, send, recv, target):
        return pltpu.make_async_remote_copy(
            src_ref=src, dst_ref=dst, send_sem=send, recv_sem=recv,
            device_id=target, device_id_type=MESH_ID,
        )

    loads = [
        pltpu.make_async_copy(gate_hbm, gate_w.at[:, :, pl.ds(0, width)], load_sem.at[0]),
        pltpu.make_async_copy(down_hbm, down_w, load_sem.at[1]),
    ]
    for load in loads:
        load.start()

    barrier = pltpu.get_barrier_semaphore()

    @pl.when(z > 0)
    def _():
        pl.semaphore_signal(barrier, 1, device_id=tok_id(z - 1, c), device_id_type=MESH_ID)

    @pl.when(z < chips - 1)
    def _():
        pl.semaphore_signal(barrier, 1, device_id=tok_id(z + 1, c), device_id_type=MESH_ID)

    if cores > 1:
        pl.semaphore_signal(barrier, 1, device_id=tok_id(z, other), device_id_type=MESH_ID)
    for d in range(1, shares):
        pl.semaphore_signal(
            barrier, 1, device_id=peer_id((mine + d) % shares), device_id_type=MESH_ID
        )
    sides = jnp.where(z > 0, 1, 0) + jnp.where(z < chips - 1, 1, 0)
    pl.semaphore_wait(barrier, sides + (cores - 1) + (shares - 1))

    def parts_copy(d):
        share = (mine + d) % shares
        return remote(
            parts_ref.at[share], peer_parts.at[mine], parts_send.at[d - 1],
            parts_recv.at[mine], peer_id(share),
        )

    def squares_copy(d):
        return remote(
            squares, peer_squares.at[mine], squares_send.at[d - 1],
            squares_recv.at[mine], peer_id((mine + d) % shares),
        )

    for d in range(1, shares):
        parts_copy(d).start()
    gate_w[:, :, width:, :] = jnp.zeros(
        gate_w.shape[:2] + (gate_w.shape[2] - width, gate_w.shape[3]), jnp.bfloat16
    )
    stream[...] = residual_ref[...].astype(jnp.float32) + parts_ref[mine].astype(jnp.float32)
    for d in range(1, shares):
        share = (mine + d) % shares
        slot = peer_parts.at[share]
        pltpu.make_async_copy(slot, slot, parts_recv.at[share]).wait()
        stream[...] += peer_parts[share].astype(jnp.float32)
    own = stream[...]
    square = jnp.sum(own * own, axis=1, keepdims=True)
    squares[...] = jnp.broadcast_to(square, squares.shape)
    for d in range(1, shares):
        squares_copy(d).start()
    total_square = squares[...]
    for d in range(1, shares):
        share = (mine + d) % shares
        slot = peer_squares.at[share]
        pltpu.make_async_copy(slot, slot, squares_recv.at[share]).wait()
        total_square += peer_squares[share]
    inverse = lax.rsqrt(total_square[:, :1] / (shares * width) + 1e-05)
    normed = stream[...] * inverse * gain_ref[...] + tail_ref[...].astype(jnp.float32)
    rows[z, mine, c] = normed.astype(jnp.bfloat16)

    near = jnp.minimum(z, chips - 1 - z)

    def chip_at(i):
        inner = jnp.where(i % 2 == 1, z - (i + 1) // 2, z + i // 2)
        outer = jnp.where(z < chips - 1 - z, i, chips - 1 - i)
        return jnp.where(i <= 2 * near, inner, outer)

    def row_copy(chip, share, core, send, target):
        slot = rows.at[chip, share, core]
        return remote(slot, slot, send, row_recv.at[chip, core, share], target)

    def go_right(chip):
        return (chip <= z) & (z < chips - 1)

    def go_left(chip):
        return (chip >= z) & (z > 0)

    def right_copy(chip):
        return row_copy(chip, mine, c, row_right.at[chip], tok_id(z + 1, c))

    def left_copy(chip):
        return row_copy(chip, mine, c, row_left.at[chip], tok_id(z - 1, c))

    def peer_copy(chip, d):
        return row_copy(chip, mine, c, row_peer.at[chip, d - 1], peer_id((mine + d) % shares))

    def core_copy(chip, share):
        return row_copy(chip, share, c, row_core.at[chip, share], tok_id(z, other))

    def row_wait(chip, share, core):
        slot = rows.at[chip, share, core]
        pltpu.make_async_copy(slot, slot, row_recv.at[chip, core, share]).wait()

    def forward(i):
        chip = chip_at(i)

        @pl.when(go_right(chip))
        def _():
            right_copy(chip).start()

        @pl.when(go_left(chip))
        def _():
            left_copy(chip).start()

        for d in range(1, shares):
            peer_copy(chip, d).start()
        if cores > 1:
            core_copy(chip, mine).start()

    forward(0)
    loads[0].wait()
    loads[1].wait()

    tail = (width // 128) * 128
    wide = rows.shape[-1]
    depth = rows.shape[-2]
    experts = chips * cores
    tail_lane = tail + lax.broadcasted_iota(jnp.int32, (cores * depth, wide - tail), 1)
    weight_lane = (tail_lane == width + tok) | (tail_lane == width + experts + tok)

    def kept_at(chip, share):
        return kept.at[chip, share] if cores > 1 else part.at[chip, share, 0]

    def part_copy(chip, share):
        return remote(
            part.at[chip, share, other], from_core.at[chip, share],
            part_send.at[chip, share], part_recv.at[chip, share], tok_id(z, other),
        )

    def sum_copy(chip, d):
        share = (mine + d) % shares
        return remote(
            kept_at(chip, share), from_peer.at[chip, mine],
            peer_send.at[chip, d - 1], peer_recv.at[chip, mine], peer_id(share),
        )

    def compute(i, carry):
        @pl.when(i + 1 < chips)
        def _():
            row_wait(chip_at(i + 1), mine, c)
            forward(i + 1)

        chip = chip_at(i)
        for d in range(1, shares):
            share = (mine + d) % shares
            row_wait(chip, share, c)
            if cores > 1:
                core_copy(chip, share).start()
        if cores > 1:
            for share in range(shares):
                row_wait(chip, share, other)
        gate = jnp.zeros((cores * depth, gate_w.shape[-1]), jnp.float32)
        up = gate
        for share in range(shares):
            block = rows[chip, share].reshape(cores * depth, wide)
            gate += jnp.dot(block, gate_w[0, share], preferred_element_type=jnp.float32)
            up += jnp.dot(block, gate_w[1, share], preferred_element_type=jnp.float32)
        active = (gate * jax.nn.sigmoid(1.702 * gate) * (up + 1.0)).astype(jnp.bfloat16)
        ends = rows[chip, 0, :, :, tail:].reshape(cores * depth, wide - tail).astype(jnp.float32)
        weight = jnp.sum(jnp.where(weight_lane, ends, 0.0), axis=1, keepdims=True)
        for share in range(shares):
            out = jnp.dot(active, down_w[share], preferred_element_type=jnp.float32)
            out = (out * weight).astype(jnp.bfloat16)
            part[chip, share] = out.reshape(cores, depth, width)
            if cores > 1:
                part_copy(chip, share).start()
        for share in range(shares):
            if cores > 1:
                part_copy(chip, share).wait_recv()
                total = part[chip, share, c].astype(jnp.float32)
                total += from_core[chip, share].astype(jnp.float32)
                kept[chip, share] = total.astype(jnp.bfloat16)
        for d in range(1, shares):
            sum_copy(chip, d).start()
        return carry

    lax.fori_loop(0, chips, compute, 0)

    def right_hop(chip):
        return remote(
            hop.at[chip], from_left.at[chip], hop_send.at[chip], left_recv.at[chip],
            tok_id(z + 1, c),
        )

    def left_hop(chip):
        return remote(
            hop.at[chip], from_right.at[chip], hop_send.at[chip], right_recv.at[chip],
            tok_id(z - 1, c),
        )

    def hop_wait(buffer, sem, chip):
        pltpu.make_async_copy(buffer.at[chip], buffer.at[chip], sem.at[chip]).wait()

    def give_back(j, carry):
        chip = chip_at(chips - 1 - j)
        total = kept_at(chip, mine)[...].astype(jnp.float32)
        for d in range(1, shares):
            share = (mine + d) % shares
            slot = from_peer.at[chip, share]
            pltpu.make_async_copy(slot, slot, peer_recv.at[chip, share]).wait()
            total += from_peer[chip, share].astype(jnp.float32)
        acc[...] = total

        @pl.when((chip <= z) & (z < chips - 1))
        def _():
            hop_wait(from_right, right_recv, chip)
            acc[...] += from_right[chip].astype(jnp.float32)

        @pl.when((chip >= z) & (z > 0))
        def _():
            hop_wait(from_left, left_recv, chip)
            acc[...] += from_left[chip].astype(jnp.float32)

        @pl.when(chip == z)
        def _():
            out_ref[...] = (stream[:, :width] + acc[...]).astype(jnp.bfloat16)

        @pl.when(chip != z)
        def _():
            hop[chip] = acc[...].astype(jnp.bfloat16)

        @pl.when(chip < z)
        def _():
            left_hop(chip).start()

        @pl.when(chip > z)
        def _():
            right_hop(chip).start()

        return carry

    lax.fori_loop(0, chips, give_back, 0)

    def drain(chip, carry):
        @pl.when(go_right(chip))
        def _():
            right_copy(chip).wait_send()

        @pl.when(go_left(chip))
        def _():
            left_copy(chip).wait_send()

        for d in range(1, shares):
            peer_copy(chip, d).wait_send()
            sum_copy(chip, d).wait_send()
        if cores > 1:
            for share in range(shares):
                core_copy(chip, share).wait_send()
                part_copy(chip, share).wait_send()

        @pl.when(chip < z)
        def _():
            left_hop(chip).wait_send()

        @pl.when(chip > z)
        def _():
            right_hop(chip).wait_send()

        return carry

    lax.fori_loop(0, chips, drain, 0)
    for d in range(1, shares):
        parts_copy(d).wait_send()
        squares_copy(d).wait_send()


def moe(dims, parts, residual, gain, tail, gate_w, down_w):
    chips, cores, shares, pairs, width = dims
    depth, wide = residual.shape
    hidden = down_w.shape[1]
    bf16 = jnp.bfloat16
    dma = pltpu.SemaphoreType.DMA
    return pl.pallas_call(
        functools.partial(moe_kernel, dims),
        out_shape=jax.ShapeDtypeStruct((depth, width), jnp.bfloat16),
        in_specs=[pl.BlockSpec(memory_space=pltpu.VMEM)] * 4
        + [
            pl.BlockSpec(memory_space=pl.ANY),
            pl.BlockSpec(memory_space=pl.ANY),
        ],
        out_specs=pl.BlockSpec(memory_space=pltpu.VMEM),
        scratch_shapes=[
            pltpu.VMEM((2, shares, wide, hidden), bf16),
            pltpu.VMEM(down_w.shape, bf16),
            pltpu.VMEM((chips, shares, cores, depth, wide), bf16),
            pltpu.VMEM((chips, shares, cores, depth, width), bf16),
            pltpu.VMEM((chips, shares, depth, width) if cores > 1 else (8, 128), bf16),
            pltpu.VMEM((chips, shares, depth, width) if cores > 1 else (8, 128), bf16),
            pltpu.VMEM((chips, shares, depth, width), bf16),
            pltpu.VMEM((chips, depth, width), bf16),
            pltpu.VMEM((chips, depth, width), bf16),
            pltpu.VMEM((chips, depth, width), bf16),
            pltpu.VMEM((shares, depth, wide), bf16),
            pltpu.VMEM((depth, wide), jnp.float32),
            pltpu.VMEM((depth, 128), jnp.float32),
            pltpu.VMEM((shares, depth, 128), jnp.float32),
            pltpu.VMEM((depth, width), jnp.float32),
            dma((max(shares - 1, 1),)),
            dma((shares,)),
            dma((max(shares - 1, 1),)),
            dma((shares,)),
            dma((2,)),
            dma((chips, cores, shares)),
            dma((chips,)),
            dma((chips,)),
            dma((chips, max(shares - 1, 1))),
            dma((chips, shares)),
            dma((chips, shares)),
            dma((chips, shares)),
            dma((chips, max(shares - 1, 1))),
            dma((chips, shares)),
            dma((chips,)),
            dma((chips,)),
            dma((chips,)),
        ],
        compiler_params=pltpu.CompilerParams(
            collective_id=0, has_side_effects=True, vmem_limit_bytes=60 * 1024 * 1024
        ),
        cost_estimate=pl.CostEstimate(
            flops=6 * chips * cores * depth * shares * width * hidden,
            bytes_accessed=6 * shares * width * hidden,
            transcendentals=0,
        ),
    )(parts, residual, gain, tail, gate_w, down_w)


def per_device(
    queries,
    keys_values,
    sink_logits,
    residual,
    out_weight,
    norm_gain,
    expert_ids,
    route_weights,
    gate_up,
    down_weight,
):
    tok_rows = queries.shape[0]
    kv_groups = keys_values.shape[1] // (2 * HEAD_DIM)
    local_heads = queries.shape[1] // HEAD_DIM
    repeat = local_heads // kv_groups
    position = lax.axis_index("tok") * tok_rows + jnp.arange(tok_rows, dtype=jnp.int32)
    grouped = queries.reshape(tok_rows, kv_groups, repeat, HEAD_DIM)
    start_max = jnp.broadcast_to(
        sink_logits.reshape(kv_groups, repeat)[:, :, None], (kv_groups, repeat, tok_rows)
    )
    start_totals = jnp.ones((kv_groups, repeat, tok_rows), jnp.float32)
    start_accum = jnp.zeros((kv_groups, repeat, tok_rows, HEAD_DIM), jnp.float32)
    key_piece = lax.all_gather(keys_values, "tok", axis=0, tiled=True)
    hidden = down_weight.shape[1]
    shares = lax.axis_size(("head", "pair"))
    share = out_weight.shape[1] // shares
    gate_w = jnp.transpose(gate_up[0], (1, 0, 2)).reshape(2, shares, share, hidden)
    down_w = jnp.transpose(down_weight[0].reshape(hidden, shares, share), (1, 0, 2))
    key_piece, gate_w, down_w = lax.optimization_barrier((key_piece, gate_w, down_w))
    totals = start_totals
    accum = start_accum
    count = key_piece.shape[0]
    split_piece = key_piece.reshape(count, kv_groups, 2, HEAD_DIM)
    scores = (
        jnp.einsum(
            "tgrd,ngd->grtn", grouped, split_piece[:, :, 0], preferred_element_type=jnp.float32
        )
        * 0.125
    )
    key_position = jnp.arange(count, dtype=jnp.int32)
    allowed = key_position[None, :] <= position[:, None]
    scores = jnp.where(allowed, scores, jnp.float32(-1e30))
    new_max = jnp.maximum(start_max, jnp.max(scores, axis=-1))
    decay = jnp.exp(start_max - new_max)
    weights = jnp.exp(scores - new_max[..., None])
    totals = totals * decay + jnp.sum(weights, axis=-1)
    update = jnp.einsum(
        "grtn,ngd->grtd",
        weights.astype(jnp.bfloat16),
        split_piece[:, :, 1],
        preferred_element_type=jnp.float32,
    )
    accum = accum * decay[..., None] + update
    final_max, totals, accum = (new_max, totals, accum)
    attended = (accum / totals[..., None]).astype(jnp.bfloat16)
    attended = jnp.transpose(attended, (2, 0, 1, 3)).reshape(tok_rows, local_heads * HEAD_DIM)
    width = out_weight.shape[1]
    share = width // lax.axis_size(("head", "pair"))
    column_start = lax.axis_index(("head", "pair")) * share
    partial_value = jnp.dot(attended, out_weight, preferred_element_type=jnp.float32)
    experts = lax.axis_size("tok")
    pairs = lax.axis_size("pair")
    cores = 2 // pairs
    shares = width // share
    wide = -(-(share + 2 * experts) // 128) * 128
    expert = jnp.arange(experts, dtype=jnp.int32)
    routed = expert_ids[:, :, None] == expert
    dense = jnp.sum(jnp.where(routed, route_weights[:, :, None], 0.0), axis=1)
    high = lax.reduce_precision(dense, 8, 7)
    weights = jnp.concatenate([high, dense - high], axis=1).astype(jnp.bfloat16)
    tail = jnp.pad(weights, ((0, 0), (share, wide - share - 2 * experts)))
    spare = (0, wide - share)
    parts = jnp.transpose(
        partial_value.astype(jnp.bfloat16).reshape(tok_rows, shares, share), (1, 0, 2)
    )
    parts = jnp.pad(parts, ((0, 0), (0, 0), spare))
    own_residual = jnp.pad(
        lax.dynamic_slice_in_dim(residual, column_start, share, 1), ((0, 0), spare)
    )
    own_gain = jnp.pad(lax.dynamic_slice_in_dim(norm_gain, column_start, share, 0), spare)
    return moe(
        (experts // cores, cores, shares, pairs, share),
        parts, own_residual, own_gain[None, :], tail, gate_w, down_w,
    )


def layer_kernel(
    dims,
    sink_ref,
    ids_ref,
    route_ref,
    gain_ref,
    query_hbm,
    kv_hbm,
    residual_hbm,
    project_hbm,
    gate_hbm,
    down_hbm,
    out_ref,
    query_v,
    query_t,
    kvs,
    row_max,
    row_total,
    accum,
    attended,
    residual_v,
    project_w,
    gate_w,
    down_v,
    down_t,
    gain_cols,
    stream,
    parts,
    peer_parts,
    rows,
    meta,
    hidden,
    active,
    part,
    kept,
    from_core,
    cross,
    from_peer,
    hop,
    inbox,
    closing,
    from_closing,
    acc,
    squares,
    peer_squares,
    load_sem,
    kv_recv,
    kv_core_send,
    kv_up_send,
    parts_send,
    parts_recv,
    squares_sem,
    row_recv,
    row_up,
    row_down,
    row_core,
    row_peer,
    meta_recv,
    meta_up,
    meta_down,
    meta_core,
    part_send,
    part_recv,
    peer_send,
    peer_recv,
    hop_send,
    inbox_recv,
    closing_send,
    closing_recv,
):
    chips, pairs, chunk, piece, own, both = dims
    cores = 2
    width, depth = residual_hbm.shape
    kv_groups = kvs.shape[1]
    repeat = query_t.shape[2] // depth
    half = width // 2
    f32, bf16 = jnp.float32, jnp.bfloat16
    far = (width - own * chunk) // 128 * 128
    edges = [(at, min(chunk, far - at)) for at in range(own * chunk, far, chunk)]
    if far + own * chunk < width:
        edges.append((far + own * chunk, width - far - own * chunk))
    spread_over = [(2 * own + n, at, size) for n, (at, size) in enumerate(edges)]
    pieces = half // piece
    last = chips - 1

    tok = lax.axis_index("tok")
    z = tok // cores
    c = tok % cores
    x = lax.axis_index("head") * pairs + lax.axis_index("pair")
    peer = {"head": (1 - x) // pairs, "pair": (1 - x) % pairs}
    other = {"tok": z * cores + (1 - c)}
    above = {"tok": (z + 1) * cores + c}
    below = {"tok": (z - 1) * cores + c}

    def remote(src, dst, send, recv, target):
        return pltpu.make_async_remote_copy(
            src_ref=src, dst_ref=dst, send_sem=send, recv_sem=recv,
            device_id=target, device_id_type=MESH_ID,
        )

    def landed(slot, sem):
        pltpu.make_async_copy(slot, slot, sem).wait()

    def mult(value, of):
        return pl.multiple_of(value, of)

    loads = [
        pltpu.make_async_copy(
            kv_hbm.at[:, pl.ds(g * 2 * HEAD_DIM, 2 * HEAD_DIM)], kvs.at[tok, g], load_sem.at[g]
        )
        for g in range(kv_groups)
    ]
    bulk = [
        pltpu.make_async_copy(src, dst, load_sem.at[kv_groups + i])
        for i, (src, dst) in enumerate(
            [
                (query_hbm, query_v),
                (residual_hbm, residual_v),
                (project_hbm, project_w),
                (down_hbm, down_v),
                (gate_hbm, gate_w),
            ]
        )
    ]
    for load in loads + bulk:
        load.start()

    barrier = pltpu.get_barrier_semaphore()

    @pl.when(z > 0)
    def _():
        pl.semaphore_signal(barrier, 1, device_id=below, device_id_type=MESH_ID)

    @pl.when(z < last)
    def _():
        pl.semaphore_signal(barrier, 1, device_id=above, device_id_type=MESH_ID)

    pl.semaphore_signal(barrier, 1, device_id=other, device_id_type=MESH_ID)
    pl.semaphore_signal(barrier, 1, device_id=peer, device_id_type=MESH_ID)
    sides = jnp.where(z > 0, 1, 0) + jnp.where(z < last, 1, 0)
    pl.semaphore_wait(barrier, sides + 2)

    def kv_up(chip, g):
        slot = kvs.at[chip * cores + c, g]
        return remote(slot, slot, kv_up_send.at[chip, g], kv_recv.at[chip, c, g], above)

    def kv_core(chip, g):
        slot = kvs.at[chip * cores + c, g]
        return remote(slot, slot, kv_core_send.at[chip, g], kv_recv.at[chip, c, g], other)

    def kv_wait(chip, core, g):
        landed(kvs.at[chip * cores + core, g], kv_recv.at[chip, core, g])

    def kv_pass(chip, g):
        @pl.when(z < last)
        def _():
            kv_up(chip, g).start()

        kv_core(chip, g).start()

    for g, load in enumerate(loads):
        load.wait()
        kv_pass(z, g)

    for b in range(-(-width // 128)):
        size = min(128, width - b * 128)
        gain = gain_ref[b * 128:b * 128 + size]
        gain_cols[b * 128:b * 128 + size, :] = jnp.broadcast_to(gain[None, :], (128, size)).T

    bulk[0].wait()
    for g in range(kv_groups):
        query_t[g, HEAD_DIM:, :] = jnp.zeros((HEAD_DIM, repeat * depth), bf16)
        for m in range(repeat // 2):
            lane = (g * repeat + 2 * m) * HEAD_DIM
            turned = (query_v[:, lane:lane + 2 * HEAD_DIM].astype(f32) * 0.125).T.astype(bf16)
            query_t[g, :HEAD_DIM, 2 * m * depth:(2 * m + 1) * depth] = turned[:HEAD_DIM]
            query_t[g, :HEAD_DIM, (2 * m + 1) * depth:(2 * m + 2) * depth] = turned[HEAD_DIM:]
        for r in range(repeat):
            row_max[g, :, r * depth:(r + 1) * depth] = jnp.full(
                (1, depth), sink_ref[g * repeat + r], f32
            )
    row_total[...] = jnp.ones(row_total.shape, f32)
    accum[...] = jnp.zeros(accum.shape, f32)

    def attend(chip, g, masked):
        keys = kvs[pl.ds(chip * cores, cores), g].reshape(cores * depth, 2 * HEAD_DIM)
        values = keys.astype(f32).T[HEAD_DIM:].astype(bf16)
        olds, totals, sums = row_max[g], row_total[g], accum[g]
        lanes = [slice(2 * m * depth, (2 * m + 2) * depth) for m in range(repeat // 2)]
        scores = [
            jnp.dot(keys, query_t[g, :, lane], preferred_element_type=f32) for lane in lanes
        ]
        if masked:
            row = lax.broadcasted_iota(jnp.int32, scores[0].shape, 0)
            column = lax.broadcasted_iota(jnp.int32, scores[0].shape, 1)
            column = jnp.where(column >= depth, column - depth, column)
            allowed = row <= c * depth + column
            scores = [jnp.where(allowed, score, jnp.float32(-1e30)) for score in scores]
        news = [
            jnp.maximum(olds[:, lane], jnp.max(score, axis=0, keepdims=True))
            for lane, score in zip(lanes, scores)
        ]
        weights = [jnp.exp(score - new) for score, new in zip(scores, news)]
        added = [
            jnp.dot(values, weight.astype(bf16), preferred_element_type=f32) for weight in weights
        ]
        for lane, new, weight, more in zip(lanes, news, weights, added):
            decay = jnp.exp(olds[:, lane] - new)
            row_max[g, :, lane] = new
            row_total[g, :, lane] = totals[:, lane] * decay + jnp.sum(
                weight, axis=0, keepdims=True
            )
            accum[g, :, lane] = sums[:, lane] * decay + more

    def attend_chip(chip, masked):
        def group(g, carry):
            kv_wait(chip, 1 - c, g)
            attend(chip, g, masked)

            @pl.when(chip > 0)
            def _():
                kv_wait(chip - 1, c, g)
                kv_pass(chip - 1, g)

            return carry

        lax.fori_loop(0, kv_groups, group, 0)

    attend_chip(z, True)

    def earlier(i, carry):
        attend_chip(z - i, False)
        return carry

    lax.fori_loop(1, z + 1, earlier, 0)

    for g in range(kv_groups):
        inverse = 1.0 / row_total[g]
        for r in range(repeat):
            lanes = slice(r * depth, (r + 1) * depth)
            head = (g * repeat + r) * HEAD_DIM
            attended[head:head + HEAD_DIM, :] = (accum[g, :, lanes] * inverse[:, lanes]).astype(bf16)

    def own_at(side, t):
        return mult(side * far + t * chunk, 128)

    def own_id(side, t):
        return side * own + t

    def parts_copy(n, start, size):
        return remote(
            parts.at[pl.ds(start, size)], peer_parts.at[pl.ds(start, size)],
            parts_send.at[n], parts_recv.at[n], peer,
        )

    def project(start, size):
        return jnp.dot(
            project_w[pl.ds(start, size), :], attended[...], preferred_element_type=f32
        )

    def give(n, start, size):
        value = project(start, size)
        parts[pl.ds(start, size), :] = value.astype(bf16)
        parts_copy(n, start, size).start()
        return value

    def hold(start, size, value):
        at = pl.ds(start, size)
        stream[at, :] = value + residual_v[at, :].astype(f32)

    def row_copy(chip, k, start, size, send, target):
        slot = rows.at[chip, c, pl.ds(start, size)]
        return remote(slot, slot, send.at[chip, k], row_recv.at[chip, c, k], target)

    def row_wait(chip, core, k, start, size):
        landed(rows.at[chip, core, pl.ds(start, size)], row_recv.at[chip, core, k])

    def pass_along(chip, k, start, size):
        @pl.when((chip <= z) & (z < last))
        def _():
            row_copy(chip, k, start, size, row_up, above).start()

        @pl.when((chip >= z) & (z > 0))
        def _():
            row_copy(chip, k, start, size, row_down, below).start()

    def meta_copy(chip, send, target):
        slot = meta.at[chip, c]
        return remote(slot, slot, send.at[chip], meta_recv.at[chip, c], target)

    def meta_wait(chip, core):
        landed(meta.at[chip, core], meta_recv.at[chip, core])

    def pass_meta(chip):
        @pl.when((chip <= z) & (z < last))
        def _():
            meta_copy(chip, meta_up, above).start()

        @pl.when((chip >= z) & (z > 0))
        def _():
            meta_copy(chip, meta_down, below).start()

        meta_copy(chip, meta_core, other).start()

    def settle(n, k, start, size):
        at = pl.ds(start, size)
        landed(peer_parts.at[at], parts_recv.at[n])
        value = stream[at, :] + peer_parts[at, :].astype(f32)
        stream[at, :] = value
        rows[z, c, at, :] = (value * gain_cols[at, :]).astype(bf16)
        pass_along(z, k, start, size)
        row_copy(z, k, start, size, row_core, other).start()
        return jnp.sum((value * value).reshape(size // 8, 8, depth), axis=0)

    bulk[1].wait()
    bulk[2].wait()

    def give_own(t, carry):
        give(t, own_at(1 - x, t), chunk)
        return carry

    lax.fori_loop(0, own, give_own, 0)
    squares_own = jnp.zeros((8, depth), f32)
    squares_all = jnp.zeros((8, depth), f32)
    for t in range(own):
        hold(own_at(x, t), chunk, project(own_at(x, t), chunk))
        for n, (k, start, size) in enumerate(spread_over):
            if t == 0:
                hold(start, size, give(own + n, start, size))
        squares_own += settle(t, own_id(x, t), own_at(x, t), chunk)
    squares[...] = squares_own
    squares_copy = remote(squares, peer_squares, squares_sem.at[0], squares_sem.at[1], peer)
    squares_copy.start()

    experts = chips * cores
    expert = lax.broadcasted_iota(jnp.int32, (experts, depth), 0)
    dense = jnp.zeros((experts, depth), f32)
    for k in range(ids_ref.shape[0]):
        dense += jnp.where(ids_ref[k:k + 1, :] == expert, route_ref[k:k + 1, :], 0.0)
    meta[z, c, pl.ds(8, experts), :] = dense
    bulk[3].wait()

    def turn(b, carry):
        at = pl.ds(mult(b * 128, 128), 128)
        down_t[at, :] = down_v[:, at].astype(f32).T.astype(bf16)
        return carry

    turns = width // 128
    if width % 128:
        at = pl.ds(turns * 128, width % 128)
        down_t[at, :] = down_v[:, at].astype(f32).T.astype(bf16)
    for n, (k, start, size) in enumerate(spread_over):
        if n < 2:
            lax.fori_loop(n * turns // 2, (n + 1) * turns // 2, turn, 0)
        squares_all += settle(own + n, k, start, size)
    if len(spread_over) < 2:
        lax.fori_loop(len(spread_over) * turns // 2, turns, turn, 0)
    landed(peer_squares, squares_sem.at[1])
    squares_all += squares[...] + peer_squares[...]
    total = jnp.sum(squares_all, axis=0, keepdims=True)
    scale = lax.rsqrt(total / width + 1e-05)
    meta[z, c, 0:8, :] = jnp.broadcast_to(scale, (8, depth))
    pass_meta(z)

    near = jnp.minimum(z, last - z)

    def chip_at(i):
        inner = jnp.where(i % 2 == 1, z - (i + 1) // 2, z + i // 2)
        outer = jnp.where(z < last - z, i, last - i)
        return jnp.where(i <= 2 * near, inner, outer)

    def each_side(i, act):
        @pl.when(z - 1 - i >= 0)
        def _():
            act(z - 1 - i)

        @pl.when(z + 1 + i <= last)
        def _():
            act(z + 1 + i)

    def pump(i, k, start, size, crosses):
        def act(chip):
            row_wait(chip, c, k, start, size)
            pass_along(chip, k, start, size)
            if crosses:
                row_copy(chip, k, start, size, row_peer, peer).start()
            row_copy(chip, k, start, size, row_core, other).start()

        each_side(i, act)

    def pump_own(i):
        def one(t, carry):
            pump(i, own_id(x, t), own_at(x, t), chunk, True)
            return carry

        lax.fori_loop(0, own, one, 0)

    def pump_shared(i):
        for k, start, size in spread_over:
            pump(i, k, start, size, False)

        def act(chip):
            meta_wait(chip, c)
            pass_meta(chip)

        each_side(i, act)

    def cross_in(chip):
        def one(t, carry):
            k, start = own_id(1 - x, t), own_at(1 - x, t)
            row_wait(chip, c, k, start, chunk)
            row_copy(chip, k, start, chunk, row_core, other).start()
            return carry

        lax.fori_loop(0, own, one, 0)

    def multiply(chip, k, start, size):
        row_wait(chip, 1 - c, k, start, size)
        at = pl.ds(start, size)
        pair = jnp.concatenate([rows[chip, c, at, :], rows[chip, 1 - c, at, :]], axis=1)
        for side in range(2):
            hidden[side] += jnp.dot(gate_w[side, :, at], pair, preferred_element_type=f32)

    def multiply_line(chip):
        hidden[...] = jnp.zeros(hidden.shape, f32)

        def one(t, carry):
            multiply(chip, own_id(x, t), own_at(x, t), chunk)
            return carry

        lax.fori_loop(0, own, one, 0)
        for k, start, size in spread_over:
            multiply(chip, k, start, size)

    def multiply_crossed(chip):
        def one(t, carry):
            multiply(chip, own_id(1 - x, t), own_at(1 - x, t), chunk)
            return carry

        lax.fori_loop(0, own, one, 0)

    def part_copy(chip, r):
        return remote(
            part.at[chip, r], from_core.at[chip, r], part_send.at[chip, r],
            part_recv.at[chip, r], other,
        )

    def cross_copy(chip, r):
        return remote(
            cross.at[chip, r], from_peer.at[chip, r], peer_send.at[chip, r],
            peer_recv.at[chip, r], peer,
        )

    def hop_copy(way, chip, u):
        return remote(
            hop.at[chip, u], inbox.at[way, chip, u], hop_send.at[chip, u],
            inbox_recv.at[way, chip, u], {"tok": tok + cores * (1 - 2 * way)},
        )

    def last_copy(u):
        return remote(
            closing.at[u], from_closing.at[u], closing_send.at[u], closing_recv.at[u], peer
        )

    def piece_of(u):
        return jnp.where(u < both, (1 - x) * pieces + u, x * pieces + u - both)

    slots = pieces + both
    nearer = jnp.where(z < last - z, 0, 1)

    def hops(i, ends):
        def toward(turn_of, carry):
            way = jnp.where(nearer == 0, turn_of, 1 - turn_of)
            chip = jnp.where(way == 0, i, last - i)
            incoming = jnp.where(way == 0, z, last - z) > 0
            sends = jnp.where(way == 0, chip - z, z - chip) > 0
            if ends is not None:
                sends = sends & (incoming != ends)

            def one(u, carry):
                at = piece_of(u)
                @pl.when(u >= 2 * both)
                def _():
                    r = jnp.maximum(u - 2 * both, 0)
                    landed(from_peer.at[chip, r], peer_recv.at[chip, r])
                    acc[...] = kept[chip, at].astype(f32) + from_peer[chip, r].astype(f32)

                @pl.when(u < 2 * both)
                def _():
                    acc[...] = kept[chip, at].astype(f32)

                @pl.when(incoming)
                def _():
                    landed(inbox.at[way, chip, u], inbox_recv.at[way, chip, u])
                    acc[...] += inbox[way, chip, u].astype(f32)

                hop[chip, u] = acc[...].astype(bf16)
                hop_copy(way, chip, u).start()
                return carry

            @pl.when(sends)
            def _():
                lax.fori_loop(0, slots, one, 0)

            return carry

        lax.fori_loop(0, 2, toward, 0)

    def finish_rows(chip, between=None):
        meta_wait(chip, 1 - c)
        scale = jnp.concatenate([meta[chip, c, 0:1, :], meta[chip, 1 - c, 0:1, :]], axis=1)
        weight = jnp.concatenate(
            [meta[chip, c, pl.ds(8 + tok, 1), :], meta[chip, 1 - c, pl.ds(8 + tok, 1), :]], axis=1
        )
        gate = hidden[0] * scale
        up = hidden[1] * scale
        active[...] = (gate * jax.nn.sigmoid(1.702 * gate) * (up + 1.0) * weight).astype(bf16)

        def spread(r, carry):
            at = jnp.where(r < pieces, (1 - x) * pieces + r, x * pieces + r - pieces)
            value = jnp.dot(
                down_t[pl.ds(mult(at * piece, piece), piece), :], active[...],
                preferred_element_type=f32,
            )
            part[chip, at] = value[:, depth:].astype(bf16)
            part_copy(chip, at).start()
            kept[chip, at] = value[:, :depth].astype(bf16)
            return carry

        lax.fori_loop(0, 2 * pieces, spread, 0)
        if between is not None:
            between()

        def join(r, carry):
            at = (1 - x) * pieces + r
            landed(from_core.at[chip, at], part_recv.at[chip, at])
            value = kept[chip, at].astype(f32) + from_core[chip, at].astype(f32)

            @pl.when(r >= both)
            def _():
                cross[chip, jnp.maximum(r - both, 0)] = value.astype(bf16)
                cross_copy(chip, jnp.maximum(r - both, 0)).start()

            @pl.when(r < both)
            def _():
                kept[chip, at] = value.astype(bf16)

            return carry

        lax.fori_loop(0, pieces, join, 0)

        def keep(r, carry):
            at = x * pieces + r
            landed(from_core.at[chip, at], part_recv.at[chip, at])
            value = kept[chip, at].astype(f32) + from_core[chip, at].astype(f32)
            kept[chip, at] = value.astype(bf16)
            return carry

        lax.fori_loop(0, pieces, keep, 0)

    is_end = (z == 0) | (z == last)

    def own_block():
        multiply_line(z)
        cross_in(z)
        multiply_crossed(z)
        finish_rows(z)

    bulk[4].wait()
    pump_own(0)
    pump_shared(0)

    def step(i, carry):
        chip = chip_at(i)
        multiply_line(chip)
        pump_own(i)
        each_side(i - 1, cross_in)
        multiply_crossed(chip)

        @pl.when(jnp.logical_not(is_end))
        def _():
            pump_shared(i)

        def between():
            @pl.when(is_end)
            def _():
                pump_shared(i)

        finish_rows(chip, between)

        @pl.when(i == jnp.where(is_end, last, 1))
        def _():
            for t in range(own):
                row_copy(z, own_id(x, t), own_at(x, t), chunk, row_peer, peer).start()

        @pl.when(i > 1)
        def _():
            hops(i - 1, True)

        return carry

    lax.fori_loop(1, chips, step, 0)

    @pl.when(jnp.logical_not(is_end))
    def _():
        own_block()

    for i in range(1, last):
        hops(i, False)
    hops(last, None)

    @pl.when(is_end)
    def _():
        own_block()

    def from_line(u):
        acc[...] = kept[z, piece_of(u)].astype(f32)

        @pl.when(z > 0)
        def _():
            landed(inbox.at[0, z, u], inbox_recv.at[0, z, u])
            acc[...] += inbox[0, z, u].astype(f32)

        @pl.when(z < last)
        def _():
            landed(inbox.at[1, z, u], inbox_recv.at[1, z, u])
            acc[...] += inbox[1, z, u].astype(f32)

    def closes(u, carry):
        from_line(u)
        closing[u] = acc[...].astype(bf16)
        last_copy(u).start()
        return carry

    lax.fori_loop(0, both, closes, 0)

    def finish(r, carry):
        p = jnp.where(r < pieces - both, r + both, r - (pieces - both))
        at = pl.ds(mult(x * half + p * piece, 16), piece)
        from_line(p + both)

        @pl.when(p >= both)
        def _():
            q = jnp.maximum(p - both, 0)
            landed(from_peer.at[z, q], peer_recv.at[z, q])
            acc[...] += from_peer[z, q].astype(f32)

        if both:
            @pl.when(p < both)
            def _():
                q = jnp.minimum(p, both - 1)
                landed(from_closing.at[q], closing_recv.at[q])
                acc[...] += from_closing[q].astype(f32)

        out_ref[pl.ds(mult(p * piece, piece), piece), :] = (stream[at, :] + acc[...]).astype(bf16)
        return carry

    lax.fori_loop(0, pieces, finish, 0)

    def drain(chip, carry):
        for g in range(kv_groups):
            @pl.when(chip <= z)
            def _():
                kv_core(chip, g).wait_send()

            @pl.when((chip <= z) & (z < last))
            def _():
                kv_up(chip, g).wait_send()

        def sent(k, start, size, on_line, crosses):
            if on_line:
                @pl.when((chip <= z) & (z < last))
                def _():
                    row_copy(chip, k, start, size, row_up, above).wait_send()

                @pl.when((chip >= z) & (z > 0))
                def _():
                    row_copy(chip, k, start, size, row_down, below).wait_send()

            if crosses:
                row_copy(chip, k, start, size, row_peer, peer).wait_send()

            row_copy(chip, k, start, size, row_core, other).wait_send()

        for t in range(own):
            sent(own_id(x, t), own_at(x, t), chunk, True, True)
            sent(own_id(1 - x, t), own_at(1 - x, t), chunk, False, False)
        for k, start, size in spread_over:
            sent(k, start, size, True, False)

        @pl.when((chip <= z) & (z < last))
        def _():
            meta_copy(chip, meta_up, above).wait_send()

        @pl.when((chip >= z) & (z > 0))
        def _():
            meta_copy(chip, meta_down, below).wait_send()

        meta_copy(chip, meta_core, other).wait_send()
        for r in range(2 * pieces):
            part_copy(chip, r).wait_send()
        for r in range(pieces - both):
            cross_copy(chip, r).wait_send()
        for u in range(slots):
            @pl.when(chip > z)
            def _():
                hop_copy(0, chip, u).wait_send()

            @pl.when(chip < z)
            def _():
                hop_copy(1, chip, u).wait_send()

        return carry

    lax.fori_loop(0, chips, drain, 0)
    for t in range(own):
        parts_copy(t, own_at(1 - x, t), chunk).wait_send()
    for n, (k, start, size) in enumerate(spread_over):
        parts_copy(own + n, start, size).wait_send()
    squares_copy.wait_send()
    for u in range(both):
        last_copy(u).wait_send()


def whole_layer(
    dims, sinks, ids, route, gain, queries, keys_values, residual, project, gate_up, down
):
    chips, pairs, chunk, piece, own, both = dims
    cores = 2
    width, depth = residual.shape
    kv_groups = keys_values.shape[1] // (2 * HEAD_DIM)
    heads = queries.shape[1] // HEAD_DIM
    repeat = heads // kv_groups
    hidden = down.shape[0]
    half = width // 2
    pieces = half // piece
    count = -(-width // chunk) + 2
    bf16, f32 = jnp.bfloat16, jnp.float32
    dma = pltpu.SemaphoreType.DMA
    vmem = pltpu.VMEM
    experts = chips * cores
    flops = 2 * width * (
        depth * heads * HEAD_DIM + chips * cores * depth * 3 * hidden
    )
    return pl.pallas_call(
        functools.partial(layer_kernel, dims),
        out_shape=jax.ShapeDtypeStruct((half, depth), bf16),
        in_specs=[pl.BlockSpec(memory_space=pltpu.SMEM)]
        + [pl.BlockSpec(memory_space=pltpu.VMEM)] * 3
        + [pl.BlockSpec(memory_space=pl.ANY)] * 6,
        out_specs=pl.BlockSpec(memory_space=pltpu.VMEM),
        scratch_shapes=[
            vmem(queries.shape, bf16),
            vmem((kv_groups, 2 * HEAD_DIM, repeat * depth), bf16),
            vmem((experts, kv_groups, depth, 2 * HEAD_DIM), bf16),
            vmem((kv_groups, 1, repeat * depth), f32),
            vmem((kv_groups, 1, repeat * depth), f32),
            vmem((kv_groups, HEAD_DIM, repeat * depth), f32),
            vmem((heads * HEAD_DIM, depth), bf16),
            vmem(residual.shape, bf16),
            vmem(project.shape, bf16),
            vmem(gate_up.shape, bf16),
            vmem(down.shape, bf16),
            vmem((width, hidden), bf16),
            vmem((width, depth), f32),
            vmem((width, depth), f32),
            vmem((width, depth), bf16),
            vmem((width, depth), bf16),
            vmem((chips, cores, width, depth), bf16),
            vmem((chips, cores, 8 + experts, depth), f32),
            vmem((2, hidden, cores * depth), f32),
            vmem((hidden, cores * depth), bf16),
            vmem((chips, 2 * pieces, piece, depth), bf16),
            vmem((chips, 2 * pieces, piece, depth), bf16),
            vmem((chips, 2 * pieces, piece, depth), bf16),
            vmem((chips, max(pieces - both, 1), piece, depth), bf16),
            vmem((chips, max(pieces - both, 1), piece, depth), bf16),
            vmem((chips, pieces + both, piece, depth), bf16),
            vmem((2, chips, pieces + both, piece, depth), bf16),
            vmem((max(both, 1), piece, depth), bf16),
            vmem((max(both, 1), piece, depth), bf16),
            vmem((piece, depth), f32),
            vmem((8, depth), f32),
            vmem((8, depth), f32),
            dma((kv_groups + 5,)),
            dma((chips, cores, kv_groups)),
            dma((chips, kv_groups)),
            dma((chips, kv_groups)),
            dma((count,)),
            dma((count,)),
            dma((2,)),
            dma((chips, cores, count)),
            dma((chips, count)),
            dma((chips, count)),
            dma((chips, count)),
            dma((chips, count)),
            dma((chips, cores)),
            dma((chips,)),
            dma((chips,)),
            dma((chips,)),
            dma((chips, 2 * pieces)),
            dma((chips, 2 * pieces)),
            dma((chips, max(pieces - both, 1))),
            dma((chips, max(pieces - both, 1))),
            dma((chips, pieces + both)),
            dma((2, chips, pieces + both)),
            dma((max(both, 1),)),
            dma((max(both, 1),)),
        ],
        compiler_params=pltpu.CompilerParams(
            collective_id=0, has_side_effects=True, vmem_limit_bytes=VMEM_BYTES
        ),
        cost_estimate=pl.CostEstimate(
            flops=flops,
            bytes_accessed=2 * (project.size + gate_up.size + down.size),
            transcendentals=0,
        ),
    )(sinks, ids, route, gain, queries, keys_values, residual, project, gate_up, down)


def per_device_whole(
    queries,
    keys_values,
    sink_logits,
    residual,
    out_weight,
    norm_gain,
    expert_ids,
    route_weights,
    gate_up,
    down_weight,
):
    width = residual.shape[1]
    pairs = lax.axis_size("pair")
    chips = lax.axis_size("tok") // 2
    half = width // 2
    chunk = min(512, half // 128 * 128)
    piece = next(n for n in (480, 240, 160, 80, 48, 32, 16, half) if half % n == 0)
    own = max(width // chunk // 2 - OWN_LESS, 1)
    both = min(BOTH, half // piece - 1)
    out = whole_layer(
        (chips, pairs, chunk, piece, own, both),
        sink_logits,
        expert_ids.T,
        route_weights.T,
        norm_gain,
        queries,
        keys_values,
        residual.T,
        out_weight.T,
        jnp.transpose(gate_up[0], (1, 2, 0)),
        down_weight[0],
    )
    return out.T


def solution(mesh):
    placed = (
        P(("groups", "tok"), ("head", "pair")),
        P(("groups", "tok"), ("head", "pair")),
        P(("head", "pair")),
        P(("groups", "tok"), None),
        P(("head", "pair"), None),
        P(),
        P(("groups", "tok"), None),
        P(("groups", "tok"), None),
        P("tok", None, None, ("head", "pair")),
        P("tok", ("head", "pair"), None),
    )
    sizes = mesh.shape
    chip_pair = sizes["pair"] == 1 and sizes["head"] == 2 and sizes["tok"] % 2 == 0
    return jax.shard_map(
        per_device_whole if chip_pair else per_device,
        mesh=mesh,
        in_specs=placed,
        out_specs=P(("groups", "tok"), ("head", "pair")),
        check_vma=False,
    )
```

```python
import functools

import jax
import jax.numpy as jnp
from jax import lax
from jax.experimental import pallas as pl
from jax.experimental.pallas import tpu as pltpu
from jax.sharding import PartitionSpec as P

HEAD_DIM = 64

MESH_ID = pl.DeviceIdType.MESH

VMEM_BYTES = 67_043_328
CHUNK = 512
PIECE = 240
JOINT = 2
OWN = 2


def moe_kernel(
    dims,
    parts_ref,
    residual_ref,
    gain_ref,
    tail_ref,
    gate_hbm,
    down_hbm,
    out_ref,
    gate_w,
    down_w,
    rows,
    part,
    from_core,
    kept,
    from_peer,
    hop,
    from_right,
    from_left,
    peer_parts,
    stream,
    squares,
    peer_squares,
    acc,
    parts_send,
    parts_recv,
    squares_send,
    squares_recv,
    load_sem,
    row_recv,
    row_right,
    row_left,
    row_peer,
    row_core,
    part_send,
    part_recv,
    peer_send,
    peer_recv,
    hop_send,
    right_recv,
    left_recv,
):
    chips, cores, shares, pairs, width = dims
    tok = lax.axis_index("tok")
    z = tok // cores
    c = tok % cores
    mine = lax.axis_index("head") * pairs + lax.axis_index("pair")
    other = cores - 1 - c

    def tok_id(chip, core):
        return {"tok": chip * cores + core}

    def peer_id(share):
        return {"head": share // pairs, "pair": share % pairs}

    def remote(src, dst, send, recv, target):
        return pltpu.make_async_remote_copy(
            src_ref=src, dst_ref=dst, send_sem=send, recv_sem=recv,
            device_id=target, device_id_type=MESH_ID,
        )

    loads = [
        pltpu.make_async_copy(gate_hbm, gate_w.at[:, :, pl.ds(0, width)], load_sem.at[0]),
        pltpu.make_async_copy(down_hbm, down_w, load_sem.at[1]),
    ]
    for load in loads:
        load.start()

    barrier = pltpu.get_barrier_semaphore()

    @pl.when(z > 0)
    def _():
        pl.semaphore_signal(barrier, 1, device_id=tok_id(z - 1, c), device_id_type=MESH_ID)

    @pl.when(z < chips - 1)
    def _():
        pl.semaphore_signal(barrier, 1, device_id=tok_id(z + 1, c), device_id_type=MESH_ID)

    if cores > 1:
        pl.semaphore_signal(barrier, 1, device_id=tok_id(z, other), device_id_type=MESH_ID)
    for d in range(1, shares):
        pl.semaphore_signal(
            barrier, 1, device_id=peer_id((mine + d) % shares), device_id_type=MESH_ID
        )
    sides = jnp.where(z > 0, 1, 0) + jnp.where(z < chips - 1, 1, 0)
    pl.semaphore_wait(barrier, sides + (cores - 1) + (shares - 1))

    def parts_copy(d):
        share = (mine + d) % shares
        return remote(
            parts_ref.at[share], peer_parts.at[mine], parts_send.at[d - 1],
            parts_recv.at[mine], peer_id(share),
        )

    def squares_copy(d):
        return remote(
            squares, peer_squares.at[mine], squares_send.at[d - 1],
            squares_recv.at[mine], peer_id((mine + d) % shares),
        )

    for d in range(1, shares):
        parts_copy(d).start()
    gate_w[:, :, width:, :] = jnp.zeros(
        gate_w.shape[:2] + (gate_w.shape[2] - width, gate_w.shape[3]), jnp.bfloat16
    )
    stream[...] = residual_ref[...].astype(jnp.float32) + parts_ref[mine].astype(jnp.float32)
    for d in range(1, shares):
        share = (mine + d) % shares
        slot = peer_parts.at[share]
        pltpu.make_async_copy(slot, slot, parts_recv.at[share]).wait()
        stream[...] += peer_parts[share].astype(jnp.float32)
    own = stream[...]
    square = jnp.sum(own * own, axis=1, keepdims=True)
    squares[...] = jnp.broadcast_to(square, squares.shape)
    for d in range(1, shares):
        squares_copy(d).start()
    total_square = squares[...]
    for d in range(1, shares):
        share = (mine + d) % shares
        slot = peer_squares.at[share]
        pltpu.make_async_copy(slot, slot, squares_recv.at[share]).wait()
        total_square += peer_squares[share]
    inverse = lax.rsqrt(total_square[:, :1] / (shares * width) + 1e-05)
    normed = stream[...] * inverse * gain_ref[...] + tail_ref[...].astype(jnp.float32)
    rows[z, mine, c] = normed.astype(jnp.bfloat16)

    near = jnp.minimum(z, chips - 1 - z)

    def chip_at(i):
        inner = jnp.where(i % 2 == 1, z - (i + 1) // 2, z + i // 2)
        outer = jnp.where(z < chips - 1 - z, i, chips - 1 - i)
        return jnp.where(i <= 2 * near, inner, outer)

    def row_copy(chip, share, core, send, target):
        slot = rows.at[chip, share, core]
        return remote(slot, slot, send, row_recv.at[chip, core, share], target)

    def go_right(chip):
        return (chip <= z) & (z < chips - 1)

    def go_left(chip):
        return (chip >= z) & (z > 0)

    def right_copy(chip):
        return row_copy(chip, mine, c, row_right.at[chip], tok_id(z + 1, c))

    def left_copy(chip):
        return row_copy(chip, mine, c, row_left.at[chip], tok_id(z - 1, c))

    def peer_copy(chip, d):
        return row_copy(chip, mine, c, row_peer.at[chip, d - 1], peer_id((mine + d) % shares))

    def core_copy(chip, share):
        return row_copy(chip, share, c, row_core.at[chip, share], tok_id(z, other))

    def row_wait(chip, share, core):
        slot = rows.at[chip, share, core]
        pltpu.make_async_copy(slot, slot, row_recv.at[chip, core, share]).wait()

    def forward(i):
        chip = chip_at(i)

        @pl.when(go_right(chip))
        def _():
            right_copy(chip).start()

        @pl.when(go_left(chip))
        def _():
            left_copy(chip).start()

        for d in range(1, shares):
            peer_copy(chip, d).start()
        if cores > 1:
            core_copy(chip, mine).start()

    forward(0)
    loads[0].wait()
    loads[1].wait()

    tail = (width // 128) * 128
    wide = rows.shape[-1]
    depth = rows.shape[-2]
    experts = chips * cores
    tail_lane = tail + lax.broadcasted_iota(jnp.int32, (cores * depth, wide - tail), 1)
    weight_lane = (tail_lane == width + tok) | (tail_lane == width + experts + tok)

    def kept_at(chip, share):
        return kept.at[chip, share] if cores > 1 else part.at[chip, share, 0]

    def part_copy(chip, share):
        return remote(
            part.at[chip, share, other], from_core.at[chip, share],
            part_send.at[chip, share], part_recv.at[chip, share], tok_id(z, other),
        )

    def sum_copy(chip, d):
        share = (mine + d) % shares
        return remote(
            kept_at(chip, share), from_peer.at[chip, mine],
            peer_send.at[chip, d - 1], peer_recv.at[chip, mine], peer_id(share),
        )

    def compute(i, carry):
        @pl.when(i + 1 < chips)
        def _():
            row_wait(chip_at(i + 1), mine, c)
            forward(i + 1)

        chip = chip_at(i)
        for d in range(1, shares):
            share = (mine + d) % shares
            row_wait(chip, share, c)
            if cores > 1:
                core_copy(chip, share).start()
        if cores > 1:
            for share in range(shares):
                row_wait(chip, share, other)
        gate = jnp.zeros((cores * depth, gate_w.shape[-1]), jnp.float32)
        up = gate
        for share in range(shares):
            block = rows[chip, share].reshape(cores * depth, wide)
            gate += jnp.dot(block, gate_w[0, share], preferred_element_type=jnp.float32)
            up += jnp.dot(block, gate_w[1, share], preferred_element_type=jnp.float32)
        active = (gate * jax.nn.sigmoid(1.702 * gate) * (up + 1.0)).astype(jnp.bfloat16)
        ends = rows[chip, 0, :, :, tail:].reshape(cores * depth, wide - tail).astype(jnp.float32)
        weight = jnp.sum(jnp.where(weight_lane, ends, 0.0), axis=1, keepdims=True)
        for share in range(shares):
            out = jnp.dot(active, down_w[share], preferred_element_type=jnp.float32)
            out = (out * weight).astype(jnp.bfloat16)
            part[chip, share] = out.reshape(cores, depth, width)
            if cores > 1:
                part_copy(chip, share).start()
        for share in range(shares):
            if cores > 1:
                part_copy(chip, share).wait_recv()
                total = part[chip, share, c].astype(jnp.float32)
                total += from_core[chip, share].astype(jnp.float32)
                kept[chip, share] = total.astype(jnp.bfloat16)
        for d in range(1, shares):
            sum_copy(chip, d).start()
        return carry

    lax.fori_loop(0, chips, compute, 0)

    def right_hop(chip):
        return remote(
            hop.at[chip], from_left.at[chip], hop_send.at[chip], left_recv.at[chip],
            tok_id(z + 1, c),
        )

    def left_hop(chip):
        return remote(
            hop.at[chip], from_right.at[chip], hop_send.at[chip], right_recv.at[chip],
            tok_id(z - 1, c),
        )

    def hop_wait(buffer, sem, chip):
        pltpu.make_async_copy(buffer.at[chip], buffer.at[chip], sem.at[chip]).wait()

    def give_back(j, carry):
        chip = chip_at(chips - 1 - j)
        total = kept_at(chip, mine)[...].astype(jnp.float32)
        for d in range(1, shares):
            share = (mine + d) % shares
            slot = from_peer.at[chip, share]
            pltpu.make_async_copy(slot, slot, peer_recv.at[chip, share]).wait()
            total += from_peer[chip, share].astype(jnp.float32)
        acc[...] = total

        @pl.when((chip <= z) & (z < chips - 1))
        def _():
            hop_wait(from_right, right_recv, chip)
            acc[...] += from_right[chip].astype(jnp.float32)

        @pl.when((chip >= z) & (z > 0))
        def _():
            hop_wait(from_left, left_recv, chip)
            acc[...] += from_left[chip].astype(jnp.float32)

        @pl.when(chip == z)
        def _():
            out_ref[...] = (stream[:, :width] + acc[...]).astype(jnp.bfloat16)

        @pl.when(chip != z)
        def _():
            hop[chip] = acc[...].astype(jnp.bfloat16)

        @pl.when(chip < z)
        def _():
            left_hop(chip).start()

        @pl.when(chip > z)
        def _():
            right_hop(chip).start()

        return carry

    lax.fori_loop(0, chips, give_back, 0)

    def drain(chip, carry):
        @pl.when(go_right(chip))
        def _():
            right_copy(chip).wait_send()

        @pl.when(go_left(chip))
        def _():
            left_copy(chip).wait_send()

        for d in range(1, shares):
            peer_copy(chip, d).wait_send()
            sum_copy(chip, d).wait_send()
        if cores > 1:
            for share in range(shares):
                core_copy(chip, share).wait_send()
                part_copy(chip, share).wait_send()

        @pl.when(chip < z)
        def _():
            left_hop(chip).wait_send()

        @pl.when(chip > z)
        def _():
            right_hop(chip).wait_send()

        return carry

    lax.fori_loop(0, chips, drain, 0)
    for d in range(1, shares):
        parts_copy(d).wait_send()
        squares_copy(d).wait_send()


def moe(dims, parts, residual, gain, tail, gate_w, down_w):
    chips, cores, shares, pairs, width = dims
    depth, wide = residual.shape
    hidden = down_w.shape[1]
    bf16 = jnp.bfloat16
    dma = pltpu.SemaphoreType.DMA
    return pl.pallas_call(
        functools.partial(moe_kernel, dims),
        out_shape=jax.ShapeDtypeStruct((depth, width), jnp.bfloat16),
        in_specs=[pl.BlockSpec(memory_space=pltpu.VMEM)] * 4
        + [
            pl.BlockSpec(memory_space=pl.ANY),
            pl.BlockSpec(memory_space=pl.ANY),
        ],
        out_specs=pl.BlockSpec(memory_space=pltpu.VMEM),
        scratch_shapes=[
            pltpu.VMEM((2, shares, wide, hidden), bf16),
            pltpu.VMEM(down_w.shape, bf16),
            pltpu.VMEM((chips, shares, cores, depth, wide), bf16),
            pltpu.VMEM((chips, shares, cores, depth, width), bf16),
            pltpu.VMEM((chips, shares, depth, width) if cores > 1 else (8, 128), bf16),
            pltpu.VMEM((chips, shares, depth, width) if cores > 1 else (8, 128), bf16),
            pltpu.VMEM((chips, shares, depth, width), bf16),
            pltpu.VMEM((chips, depth, width), bf16),
            pltpu.VMEM((chips, depth, width), bf16),
            pltpu.VMEM((chips, depth, width), bf16),
            pltpu.VMEM((shares, depth, wide), bf16),
            pltpu.VMEM((depth, wide), jnp.float32),
            pltpu.VMEM((depth, 128), jnp.float32),
            pltpu.VMEM((shares, depth, 128), jnp.float32),
            pltpu.VMEM((depth, width), jnp.float32),
            dma((max(shares - 1, 1),)),
            dma((shares,)),
            dma((max(shares - 1, 1),)),
            dma((shares,)),
            dma((2,)),
            dma((chips, cores, shares)),
            dma((chips,)),
            dma((chips,)),
            dma((chips, max(shares - 1, 1))),
            dma((chips, shares)),
            dma((chips, shares)),
            dma((chips, shares)),
            dma((chips, max(shares - 1, 1))),
            dma((chips, shares)),
            dma((chips,)),
            dma((chips,)),
            dma((chips,)),
        ],
        compiler_params=pltpu.CompilerParams(
            collective_id=0, has_side_effects=True, vmem_limit_bytes=60 * 1024 * 1024
        ),
        cost_estimate=pl.CostEstimate(
            flops=6 * chips * cores * depth * shares * width * hidden,
            bytes_accessed=6 * shares * width * hidden,
            transcendentals=0,
        ),
    )(parts, residual, gain, tail, gate_w, down_w)


def per_device(
    queries,
    keys_values,
    sink_logits,
    residual,
    out_weight,
    norm_gain,
    expert_ids,
    route_weights,
    gate_up,
    down_weight,
):
    tok_rows = queries.shape[0]
    kv_groups = keys_values.shape[1] // (2 * HEAD_DIM)
    local_heads = queries.shape[1] // HEAD_DIM
    repeat = local_heads // kv_groups
    position = lax.axis_index("tok") * tok_rows + jnp.arange(tok_rows, dtype=jnp.int32)
    grouped = queries.reshape(tok_rows, kv_groups, repeat, HEAD_DIM)
    start_max = jnp.broadcast_to(
        sink_logits.reshape(kv_groups, repeat)[:, :, None], (kv_groups, repeat, tok_rows)
    )
    start_totals = jnp.ones((kv_groups, repeat, tok_rows), jnp.float32)
    start_accum = jnp.zeros((kv_groups, repeat, tok_rows, HEAD_DIM), jnp.float32)
    key_piece = lax.all_gather(keys_values, "tok", axis=0, tiled=True)
    hidden = down_weight.shape[1]
    shares = lax.axis_size(("head", "pair"))
    share = out_weight.shape[1] // shares
    gate_w = jnp.transpose(gate_up[0], (1, 0, 2)).reshape(2, shares, share, hidden)
    down_w = jnp.transpose(down_weight[0].reshape(hidden, shares, share), (1, 0, 2))
    key_piece, gate_w, down_w = lax.optimization_barrier((key_piece, gate_w, down_w))
    totals = start_totals
    accum = start_accum
    count = key_piece.shape[0]
    split_piece = key_piece.reshape(count, kv_groups, 2, HEAD_DIM)
    scores = (
        jnp.einsum(
            "tgrd,ngd->grtn", grouped, split_piece[:, :, 0], preferred_element_type=jnp.float32
        )
        * 0.125
    )
    key_position = jnp.arange(count, dtype=jnp.int32)
    allowed = key_position[None, :] <= position[:, None]
    scores = jnp.where(allowed, scores, jnp.float32(-1e30))
    new_max = jnp.maximum(start_max, jnp.max(scores, axis=-1))
    decay = jnp.exp(start_max - new_max)
    weights = jnp.exp(scores - new_max[..., None])
    totals = totals * decay + jnp.sum(weights, axis=-1)
    update = jnp.einsum(
        "grtn,ngd->grtd",
        weights.astype(jnp.bfloat16),
        split_piece[:, :, 1],
        preferred_element_type=jnp.float32,
    )
    accum = accum * decay[..., None] + update
    final_max, totals, accum = (new_max, totals, accum)
    attended = (accum / totals[..., None]).astype(jnp.bfloat16)
    attended = jnp.transpose(attended, (2, 0, 1, 3)).reshape(tok_rows, local_heads * HEAD_DIM)
    width = out_weight.shape[1]
    share = width // lax.axis_size(("head", "pair"))
    column_start = lax.axis_index(("head", "pair")) * share
    partial_value = jnp.dot(attended, out_weight, preferred_element_type=jnp.float32)
    experts = lax.axis_size("tok")
    pairs = lax.axis_size("pair")
    cores = 2 // pairs
    shares = width // share
    wide = -(-(share + 2 * experts) // 128) * 128
    expert = jnp.arange(experts, dtype=jnp.int32)
    routed = expert_ids[:, :, None] == expert
    dense = jnp.sum(jnp.where(routed, route_weights[:, :, None], 0.0), axis=1)
    high = lax.reduce_precision(dense, 8, 7)
    weights = jnp.concatenate([high, dense - high], axis=1).astype(jnp.bfloat16)
    tail = jnp.pad(weights, ((0, 0), (share, wide - share - 2 * experts)))
    spare = (0, wide - share)
    parts = jnp.transpose(
        partial_value.astype(jnp.bfloat16).reshape(tok_rows, shares, share), (1, 0, 2)
    )
    parts = jnp.pad(parts, ((0, 0), (0, 0), spare))
    own_residual = jnp.pad(
        lax.dynamic_slice_in_dim(residual, column_start, share, 1), ((0, 0), spare)
    )
    own_gain = jnp.pad(lax.dynamic_slice_in_dim(norm_gain, column_start, share, 0), spare)
    return moe(
        (experts // cores, cores, shares, pairs, share),
        parts, own_residual, own_gain[None, :], tail, gate_w, down_w,
    )


def layer_kernel(
    dims,
    sink_ref,
    ids_ref,
    route_ref,
    gain_ref,
    query_hbm,
    kv_hbm,
    residual_hbm,
    project_hbm,
    gate_hbm,
    down_hbm,
    out_ref,
    query_v,
    query_t,
    kvs,
    row_max,
    row_total,
    accum,
    attended,
    residual_v,
    project_w,
    gate_w,
    down_v,
    down_t,
    gain_cols,
    stream,
    parts,
    peer_parts,
    rows,
    meta,
    hidden,
    active,
    part,
    kept,
    from_core,
    cross,
    from_peer,
    hop,
    relay,
    inbox,
    wide,
    acc,
    squares,
    peer_squares,
    load_sem,
    kv_recv,
    kv_core_send,
    kv_up_send,
    parts_send,
    parts_recv,
    squares_sem,
    row_recv,
    row_up,
    row_down,
    row_core,
    row_peer,
    meta_recv,
    meta_up,
    meta_down,
    meta_core,
    part_send,
    part_recv,
    peer_send,
    peer_recv,
    hop_send,
    relay_recv,
    inbox_recv,
    wide_send,
    wide_recv,
):
    chips, pairs, chunk, piece, own = dims
    cores = 2
    width, depth = residual_hbm.shape
    kv_groups = kvs.shape[1]
    repeat = query_t.shape[2] // depth
    half = width // 2
    f32, bf16 = jnp.float32, jnp.bfloat16
    far = (width - own * chunk) // 128 * 128
    edges = [(at, min(chunk, far - at)) for at in range(own * chunk, far, chunk)]
    if far + own * chunk < width:
        edges.append((far + own * chunk, width - far - own * chunk))
    spread_over = [(2 * own + n, at, size) for n, (at, size) in enumerate(edges)]
    pieces = half // piece
    joint = next(n for n in range(JOINT, 0, -1) if pieces % n == 0)
    last = chips - 1

    tok = lax.axis_index("tok")
    z = tok // cores
    c = tok % cores
    x = lax.axis_index("head") * pairs + lax.axis_index("pair")
    peer = {"head": (1 - x) // pairs, "pair": (1 - x) % pairs}
    other = {"tok": z * cores + (1 - c)}
    above = {"tok": (z + 1) * cores + c}
    below = {"tok": (z - 1) * cores + c}

    def remote(src, dst, send, recv, target):
        return pltpu.make_async_remote_copy(
            src_ref=src, dst_ref=dst, send_sem=send, recv_sem=recv,
            device_id=target, device_id_type=MESH_ID,
        )

    def landed(slot, sem):
        pltpu.make_async_copy(slot, slot, sem).wait()

    def mult(value, of):
        return pl.multiple_of(value, of)

    loads = [
        pltpu.make_async_copy(
            kv_hbm.at[:, pl.ds(g * 2 * HEAD_DIM, 2 * HEAD_DIM)], kvs.at[tok, g], load_sem.at[g]
        )
        for g in range(kv_groups)
    ]
    bulk = [
        pltpu.make_async_copy(src, dst, load_sem.at[kv_groups + i])
        for i, (src, dst) in enumerate(
            [
                (query_hbm, query_v),
                (residual_hbm, residual_v),
                (project_hbm, project_w),
                (down_hbm, down_v),
                (gate_hbm, gate_w),
            ]
        )
    ]
    for load in loads + bulk:
        load.start()

    barrier = pltpu.get_barrier_semaphore()

    @pl.when(z > 0)
    def _():
        pl.semaphore_signal(barrier, 1, device_id=below, device_id_type=MESH_ID)

    @pl.when(z < last)
    def _():
        pl.semaphore_signal(barrier, 1, device_id=above, device_id_type=MESH_ID)

    pl.semaphore_signal(barrier, 1, device_id=other, device_id_type=MESH_ID)
    pl.semaphore_signal(barrier, 1, device_id=peer, device_id_type=MESH_ID)
    sides = jnp.where(z > 0, 1, 0) + jnp.where(z < last, 1, 0)
    pl.semaphore_wait(barrier, sides + 2)

    def kv_up(chip, g):
        slot = kvs.at[chip * cores + c, g]
        return remote(slot, slot, kv_up_send.at[chip, g], kv_recv.at[chip, c, g], above)

    def kv_core(chip, g):
        slot = kvs.at[chip * cores + c, g]
        return remote(slot, slot, kv_core_send.at[chip, g], kv_recv.at[chip, c, g], other)

    def kv_wait(chip, core, g):
        landed(kvs.at[chip * cores + core, g], kv_recv.at[chip, core, g])

    def kv_pass(chip, g):
        @pl.when(z < last)
        def _():
            kv_up(chip, g).start()

        kv_core(chip, g).start()

    for g, load in enumerate(loads):
        load.wait()
        kv_pass(z, g)

    for b in range(-(-width // 128)):
        size = min(128, width - b * 128)
        gain = gain_ref[b * 128:b * 128 + size]
        gain_cols[b * 128:b * 128 + size, :] = jnp.broadcast_to(gain[None, :], (128, size)).T

    bulk[0].wait()
    for g in range(kv_groups):
        query_t[g, HEAD_DIM:, :] = jnp.zeros((HEAD_DIM, repeat * depth), bf16)
        for m in range(repeat // 2):
            lane = (g * repeat + 2 * m) * HEAD_DIM
            turned = (query_v[:, lane:lane + 2 * HEAD_DIM].astype(f32) * 0.125).T.astype(bf16)
            query_t[g, :HEAD_DIM, 2 * m * depth:(2 * m + 1) * depth] = turned[:HEAD_DIM]
            query_t[g, :HEAD_DIM, (2 * m + 1) * depth:(2 * m + 2) * depth] = turned[HEAD_DIM:]
        for r in range(repeat):
            row_max[g, :, r * depth:(r + 1) * depth] = jnp.full(
                (1, depth), sink_ref[g * repeat + r], f32
            )
    row_total[...] = jnp.ones(row_total.shape, f32)
    accum[...] = jnp.zeros(accum.shape, f32)

    def attend(chip, g, masked):
        keys = kvs[pl.ds(chip * cores, cores), g].reshape(cores * depth, 2 * HEAD_DIM)
        values = keys.astype(f32).T[HEAD_DIM:].astype(bf16)
        olds, totals, sums = row_max[g], row_total[g], accum[g]
        lanes = [slice(2 * m * depth, (2 * m + 2) * depth) for m in range(repeat // 2)]
        scores = [
            jnp.dot(keys, query_t[g, :, lane], preferred_element_type=f32) for lane in lanes
        ]
        if masked:
            row = lax.broadcasted_iota(jnp.int32, scores[0].shape, 0)
            column = lax.broadcasted_iota(jnp.int32, scores[0].shape, 1)
            column = jnp.where(column >= depth, column - depth, column)
            allowed = row <= c * depth + column
            scores = [jnp.where(allowed, score, jnp.float32(-1e30)) for score in scores]
        news = [
            jnp.maximum(olds[:, lane], jnp.max(score, axis=0, keepdims=True))
            for lane, score in zip(lanes, scores)
        ]
        weights = [jnp.exp(score - new) for score, new in zip(scores, news)]
        added = [
            jnp.dot(values, weight.astype(bf16), preferred_element_type=f32) for weight in weights
        ]
        for lane, new, weight, more in zip(lanes, news, weights, added):
            decay = jnp.exp(olds[:, lane] - new)
            row_max[g, :, lane] = new
            row_total[g, :, lane] = totals[:, lane] * decay + jnp.sum(
                weight, axis=0, keepdims=True
            )
            accum[g, :, lane] = sums[:, lane] * decay + more

    def attend_chip(chip, masked):
        def group(g, carry):
            kv_wait(chip, 1 - c, g)
            attend(chip, g, masked)

            @pl.when(chip > 0)
            def _():
                kv_wait(chip - 1, c, g)
                kv_pass(chip - 1, g)

            return carry

        lax.fori_loop(0, kv_groups, group, 0)

    attend_chip(z, True)

    def earlier(i, carry):
        attend_chip(z - i, False)
        return carry

    lax.fori_loop(1, z + 1, earlier, 0)

    for g in range(kv_groups):
        inverse = 1.0 / row_total[g]
        for r in range(repeat):
            lanes = slice(r * depth, (r + 1) * depth)
            head = (g * repeat + r) * HEAD_DIM
            attended[head:head + HEAD_DIM, :] = (accum[g, :, lanes] * inverse[:, lanes]).astype(bf16)

    def own_at(side, t):
        return mult(side * far + t * chunk, 128)

    def own_id(side, t):
        return side * own + t

    def parts_copy(n, start, size):
        return remote(
            parts.at[pl.ds(start, size)], peer_parts.at[pl.ds(start, size)],
            parts_send.at[n], parts_recv.at[n], peer,
        )

    def project(start, size):
        return jnp.dot(
            project_w[pl.ds(start, size), :], attended[...], preferred_element_type=f32
        )

    def give(n, start, size):
        value = project(start, size)
        parts[pl.ds(start, size), :] = value.astype(bf16)
        parts_copy(n, start, size).start()
        return value

    def hold(start, size, value):
        at = pl.ds(start, size)
        stream[at, :] = value + residual_v[at, :].astype(f32)

    def row_copy(chip, k, start, size, send, target):
        slot = rows.at[chip, c, pl.ds(start, size)]
        return remote(slot, slot, send.at[chip, k], row_recv.at[chip, c, k], target)

    def row_wait(chip, core, k, start, size):
        landed(rows.at[chip, core, pl.ds(start, size)], row_recv.at[chip, core, k])

    def pass_along(chip, k, start, size):
        @pl.when((chip <= z) & (z < last))
        def _():
            row_copy(chip, k, start, size, row_up, above).start()

        @pl.when((chip >= z) & (z > 0))
        def _():
            row_copy(chip, k, start, size, row_down, below).start()

    def meta_copy(chip, send, target):
        slot = meta.at[chip, c]
        return remote(slot, slot, send.at[chip], meta_recv.at[chip, c], target)

    def meta_wait(chip, core):
        landed(meta.at[chip, core], meta_recv.at[chip, core])

    def pass_meta(chip):
        @pl.when((chip <= z) & (z < last))
        def _():
            meta_copy(chip, meta_up, above).start()

        @pl.when((chip >= z) & (z > 0))
        def _():
            meta_copy(chip, meta_down, below).start()

        meta_copy(chip, meta_core, other).start()

    def settle(n, k, start, size):
        at = pl.ds(start, size)
        landed(peer_parts.at[at], parts_recv.at[n])
        value = stream[at, :] + peer_parts[at, :].astype(f32)
        stream[at, :] = value
        rows[z, c, at, :] = (value * gain_cols[at, :]).astype(bf16)
        pass_along(z, k, start, size)
        row_copy(z, k, start, size, row_core, other).start()
        return jnp.sum((value * value).reshape(size // 8, 8, depth), axis=0)

    bulk[1].wait()
    bulk[2].wait()

    def give_own(t, carry):
        give(t, own_at(1 - x, t), chunk)
        return carry

    lax.fori_loop(0, own, give_own, 0)
    squares_own = jnp.zeros((8, depth), f32)
    squares_all = jnp.zeros((8, depth), f32)
    for t in range(own):
        hold(own_at(x, t), chunk, project(own_at(x, t), chunk))
        for n, (k, start, size) in enumerate(spread_over):
            if t == 0:
                hold(start, size, give(own + n, start, size))
        squares_own += settle(t, own_id(x, t), own_at(x, t), chunk)
    squares[...] = squares_own
    squares_copy = remote(squares, peer_squares, squares_sem.at[0], squares_sem.at[1], peer)
    squares_copy.start()

    experts = chips * cores
    expert = lax.broadcasted_iota(jnp.int32, (experts, depth), 0)
    dense = jnp.zeros((experts, depth), f32)
    for k in range(ids_ref.shape[0]):
        dense += jnp.where(ids_ref[k:k + 1, :] == expert, route_ref[k:k + 1, :], 0.0)
    meta[z, c, pl.ds(8, experts), :] = dense
    bulk[3].wait()

    def turn(b, carry):
        at = pl.ds(mult(b * 128, 128), 128)
        down_t[at, :] = down_v[:, at].astype(f32).T.astype(bf16)
        return carry

    turns = width // 128
    if width % 128:
        at = pl.ds(turns * 128, width % 128)
        down_t[at, :] = down_v[:, at].astype(f32).T.astype(bf16)
    for n, (k, start, size) in enumerate(spread_over):
        if n < 2:
            lax.fori_loop(n * turns // 2, (n + 1) * turns // 2, turn, 0)
        squares_all += settle(own + n, k, start, size)
    if len(spread_over) < 2:
        lax.fori_loop(len(spread_over) * turns // 2, turns, turn, 0)
    landed(peer_squares, squares_sem.at[1])
    squares_all += squares[...] + peer_squares[...]
    total = jnp.sum(squares_all, axis=0, keepdims=True)
    scale = lax.rsqrt(total / width + 1e-05)
    meta[z, c, 0:8, :] = jnp.broadcast_to(scale, (8, depth))
    pass_meta(z)

    near = jnp.minimum(z, last - z)

    def chip_at(i):
        inner = jnp.where(i % 2 == 1, z - (i + 1) // 2, z + i // 2)
        outer = jnp.where(z < last - z, i, last - i)
        return jnp.where(i <= 2 * near, inner, outer)

    def each_side(i, act):
        @pl.when(z - 1 - i >= 0)
        def _():
            act(z - 1 - i)

        @pl.when(z + 1 + i <= last)
        def _():
            act(z + 1 + i)

    def pump(i, k, start, size, crosses):
        def act(chip):
            row_wait(chip, c, k, start, size)
            pass_along(chip, k, start, size)
            if crosses:
                row_copy(chip, k, start, size, row_peer, peer).start()
            row_copy(chip, k, start, size, row_core, other).start()

        each_side(i, act)

    def pump_own(i):
        def one(t, carry):
            pump(i, own_id(x, t), own_at(x, t), chunk, True)
            return carry

        lax.fori_loop(0, own, one, 0)

    def pump_shared(i):
        for k, start, size in spread_over:
            pump(i, k, start, size, False)

        def act(chip):
            meta_wait(chip, c)
            pass_meta(chip)

        each_side(i, act)

    def cross_in(chip):
        def one(t, carry):
            k, start = own_id(1 - x, t), own_at(1 - x, t)
            row_wait(chip, c, k, start, chunk)
            row_copy(chip, k, start, chunk, row_core, other).start()
            return carry

        lax.fori_loop(0, own, one, 0)

    def multiply(chip, k, start, size):
        row_wait(chip, 1 - c, k, start, size)
        at = pl.ds(start, size)
        pair = jnp.concatenate([rows[chip, c, at, :], rows[chip, 1 - c, at, :]], axis=1)
        units = hidden.shape[0] // 2
        for side in range(2):
            lot = slice(side * units, (side + 1) * units)
            hidden[lot] += jnp.dot(gate_w[lot, at], pair, preferred_element_type=f32)

    def multiply_line(chip):
        hidden[...] = jnp.zeros(hidden.shape, f32)

        def one(t, carry):
            multiply(chip, own_id(x, t), own_at(x, t), chunk)
            return carry

        lax.fori_loop(0, own, one, 0)
        for k, start, size in spread_over:
            multiply(chip, k, start, size)

    def multiply_crossed(chip):
        def one(t, carry):
            multiply(chip, own_id(1 - x, t), own_at(1 - x, t), chunk)
            return carry

        lax.fori_loop(0, own, one, 0)

    def part_copy(chip, r):
        return remote(
            part.at[chip, r], from_core.at[chip, r], part_send.at[chip, r],
            part_recv.at[chip, r], other,
        )

    def cross_copy(chip, r):
        return remote(
            cross.at[chip, r], from_peer.at[chip, r], peer_send.at[chip, r],
            peer_recv.at[chip, r], peer,
        )

    def far_end(chip):
        return chip == jnp.where(chip > z, last, 0)

    def adds(chip):
        return far_end(chip) & (jnp.where(chip > z, z, last - z) % 2 == 1) & (chip != partner)

    def relay_copy(chip, u):
        return remote(
            hop.at[chip, u], relay.at[chip, u], hop_send.at[chip, u],
            relay_recv.at[chip, u], {"tok": tok + jnp.where(chip > z, cores, -cores)},
        )

    def final_copy(chip, u):
        return remote(
            hop.at[chip, u], inbox.at[z, u], hop_send.at[chip, u],
            inbox_recv.at[z, u], {"tok": chip * cores + c},
        )

    partner = z + 1 - 2 * (z % 2)

    def wide_copy(at):
        return remote(
            kept.at[partner, at], wide.at[at], wide_send.at[at], wide_recv.at[at],
            {"tok": partner * cores + c},
        )

    def send_sum(chip):
        direct = adds(chip) | jnp.logical_not(far_end(chip))

        def one(u, carry):
            landed(from_peer.at[chip, u], peer_recv.at[chip, u])
            acc[...] = kept[chip, x * pieces + u].astype(f32) + from_peer[chip, u].astype(f32)

            @pl.when(adds(chip))
            def _():
                landed(relay.at[chip, u], relay_recv.at[chip, u])
                acc[...] += relay[chip, u].astype(f32)

            hop[chip, u] = acc[...].astype(bf16)

            @pl.when(direct)
            def _():
                final_copy(chip, u).start()

            @pl.when(jnp.logical_not(direct))
            def _():
                relay_copy(chip, u).start()

            return carry

        lax.fori_loop(0, pieces, one, 0)

    def send_own_sum(chip):
        @pl.when((chip != partner) & jnp.logical_not(adds(chip)))
        def _():
            send_sum(chip)

    def activate(chip):
        meta_wait(chip, 1 - c)
        scale = jnp.concatenate([meta[chip, c, 0:1, :], meta[chip, 1 - c, 0:1, :]], axis=1)
        weight = jnp.concatenate(
            [meta[chip, c, pl.ds(8 + tok, 1), :], meta[chip, 1 - c, pl.ds(8 + tok, 1), :]], axis=1
        )
        units = hidden.shape[0] // 2
        gate = hidden[:units] * scale
        up = hidden[units:] * scale
        active[...] = (gate * jax.nn.sigmoid(1.702 * gate) * (up + 1.0) * weight).astype(bf16)

    def spread_out(chip, between=None):
        def spread(n, carry):
            first = joint * n
            first = jnp.where(first < pieces, (1 - x) * pieces + first, x * pieces + first - pieces)
            value = jnp.dot(
                down_t[pl.ds(mult(first * piece, 16), joint * piece), :], active[...],
                preferred_element_type=f32,
            )
            for m in range(joint):
                at = first + m
                block = value[m * piece:(m + 1) * piece]
                part[chip, at] = block[:, depth:].astype(bf16)
                part_copy(chip, at).start()
                kept[chip, at] = block[:, :depth].astype(bf16)
            return carry

        lax.fori_loop(0, 2 * pieces // joint, spread, 0)
        if between is not None:
            between()

        def summed(at):
            landed(from_core.at[chip, at], part_recv.at[chip, at])
            acc[...] = kept[chip, at].astype(f32) + from_core[chip, at].astype(f32)

            @pl.when(chip == z)
            def _():
                landed(wide.at[at], wide_recv.at[at])
                acc[...] += wide[at].astype(f32)

        def keep(at):
            kept[chip, at] = acc[...].astype(bf16)

            @pl.when(chip == partner)
            def _():
                wide_copy(at).start()

        def give_half(r, carry):
            at = (1 - x) * pieces + r
            summed(at)

            @pl.when(chip == partner)
            def _():
                keep(at)

            @pl.when(chip != partner)
            def _():
                cross[chip, r] = acc[...].astype(bf16)
                cross_copy(chip, r).start()

            return carry

        lax.fori_loop(0, pieces, give_half, 0)

        def keep_half(r, carry):
            summed(x * pieces + r)
            keep(x * pieces + r)
            return carry

        lax.fori_loop(0, pieces, keep_half, 0)

    is_end = (z == 0) | (z == last)
    early = z < chips // 2

    def own_across():
        for t in range(own):
            row_copy(z, own_id(x, t), own_at(x, t), chunk, row_peer, peer).start()

    @pl.when(early)
    def _():
        own_across()

    bulk[4].wait()
    pump_own(0)
    pump_shared(0)

    @pl.when(jnp.logical_not(early))
    def _():
        own_across()


    def step(i, carry):
        chip = chip_at(i)
        multiply_line(chip)

        pump_own(i)

        each_side(i - 1, cross_in)
        multiply_crossed(chip)

        @pl.when(jnp.logical_not(is_end))
        def _():
            pump_shared(i)

        def between():
            @pl.when(is_end)
            def _():
                pump_shared(i)

        activate(chip)
        spread_out(chip, between)

        @pl.when(i > 1)
        def _():
            send_own_sum(chip_at(i - 1))

        return carry

    lax.fori_loop(1, chips, step, 0)
    multiply_line(z)
    cross_in(z)
    multiply_crossed(z)
    activate(z)
    spread_out(z)
    send_own_sum(chip_at(last))

    def send_added(i, carry):
        @pl.when(adds(chip_at(i)))
        def _():
            send_sum(chip_at(i))

        return carry

    lax.fori_loop(1, chips, send_added, 0)

    def finish(r, carry):
        at = pl.ds(mult(x * half + r * piece, 16), piece)
        landed(from_peer.at[z, r], peer_recv.at[z, r])
        acc[...] = kept[z, x * pieces + r].astype(f32) + from_peer[z, r].astype(f32)
        for src in range(chips):
            below_it = (src < z) & ((z < last) | (src % 2 == 1))
            above_it = (src > z) & ((z > 0) | ((last - src) % 2 == 1))

            @pl.when((below_it | above_it) & (src != partner))
            def _():
                landed(inbox.at[src, r], inbox_recv.at[src, r])
                acc[...] += inbox[src, r].astype(f32)

        out_ref[pl.ds(mult(r * piece, piece), piece), :] = (stream[at, :] + acc[...]).astype(bf16)
        return carry

    lax.fori_loop(0, pieces, finish, 0)

    def drain(chip, carry):
        for g in range(kv_groups):
            @pl.when(chip <= z)
            def _():
                kv_core(chip, g).wait_send()

            @pl.when((chip <= z) & (z < last))
            def _():
                kv_up(chip, g).wait_send()

        def sent(k, start, size, on_line, crosses):
            if on_line:
                @pl.when((chip <= z) & (z < last))
                def _():
                    row_copy(chip, k, start, size, row_up, above).wait_send()

                @pl.when((chip >= z) & (z > 0))
                def _():
                    row_copy(chip, k, start, size, row_down, below).wait_send()

            if crosses:
                row_copy(chip, k, start, size, row_peer, peer).wait_send()

            row_copy(chip, k, start, size, row_core, other).wait_send()

        for t in range(own):
            sent(own_id(x, t), own_at(x, t), chunk, True, True)
            sent(own_id(1 - x, t), own_at(1 - x, t), chunk, False, False)
        for k, start, size in spread_over:
            sent(k, start, size, True, False)

        @pl.when((chip <= z) & (z < last))
        def _():
            meta_copy(chip, meta_up, above).wait_send()

        @pl.when((chip >= z) & (z > 0))
        def _():
            meta_copy(chip, meta_down, below).wait_send()

        meta_copy(chip, meta_core, other).wait_send()
        for r in range(2 * pieces):
            part_copy(chip, r).wait_send()
        @pl.when(chip != partner)
        def _():
            for r in range(pieces):
                cross_copy(chip, r).wait_send()

        @pl.when(chip == partner)
        def _():
            for r in range(2 * pieces):
                wide_copy(r).wait_send()

        @pl.when((chip != z) & (chip != partner))
        def _():
            for u in range(pieces):
                final_copy(chip, u).wait_send()

        return carry

    lax.fori_loop(0, chips, drain, 0)
    for t in range(own):
        parts_copy(t, own_at(1 - x, t), chunk).wait_send()
    for n, (k, start, size) in enumerate(spread_over):
        parts_copy(own + n, start, size).wait_send()
    squares_copy.wait_send()


def whole_layer(
    dims, sinks, ids, route, gain, queries, keys_values, residual, project, gate_up, down
):
    chips, pairs, chunk, piece, own = dims
    cores = 2
    width, depth = residual.shape
    kv_groups = keys_values.shape[1] // (2 * HEAD_DIM)
    heads = queries.shape[1] // HEAD_DIM
    repeat = heads // kv_groups
    hidden = down.shape[0]
    half = width // 2
    pieces = half // piece
    count = -(-width // chunk) + 2
    bf16, f32 = jnp.bfloat16, jnp.float32
    dma = pltpu.SemaphoreType.DMA
    vmem = pltpu.VMEM
    experts = chips * cores
    flops = 2 * width * (
        depth * heads * HEAD_DIM + chips * cores * depth * 3 * hidden
    )
    return pl.pallas_call(
        functools.partial(layer_kernel, dims),
        out_shape=jax.ShapeDtypeStruct((half, depth), bf16),
        in_specs=[pl.BlockSpec(memory_space=pltpu.SMEM)]
        + [pl.BlockSpec(memory_space=pltpu.VMEM)] * 3
        + [pl.BlockSpec(memory_space=pl.ANY)] * 6,
        out_specs=pl.BlockSpec(memory_space=pltpu.VMEM),
        scratch_shapes=[
            vmem(queries.shape, bf16),
            vmem((kv_groups, 2 * HEAD_DIM, repeat * depth), bf16),
            vmem((experts, kv_groups, depth, 2 * HEAD_DIM), bf16),
            vmem((kv_groups, 1, repeat * depth), f32),
            vmem((kv_groups, 1, repeat * depth), f32),
            vmem((kv_groups, HEAD_DIM, repeat * depth), f32),
            vmem((heads * HEAD_DIM, depth), bf16),
            vmem(residual.shape, bf16),
            vmem(project.shape, bf16),
            vmem(gate_up.shape, bf16),
            vmem(down.shape, bf16),
            vmem((width, hidden), bf16),
            vmem((width, depth), f32),
            vmem((width, depth), f32),
            vmem((width, depth), bf16),
            vmem((width, depth), bf16),
            vmem((chips, cores, width, depth), bf16),
            vmem((chips, cores, 8 + experts, depth), f32),
            vmem((2 * hidden, cores * depth), f32),
            vmem((hidden, cores * depth), bf16),
            vmem((chips, 2 * pieces, piece, depth), bf16),
            vmem((chips, 2 * pieces, piece, depth), bf16),
            vmem((chips, 2 * pieces, piece, depth), bf16),
            vmem((chips, pieces, piece, depth), bf16),
            vmem((chips, pieces, piece, depth), bf16),
            vmem((chips, pieces, piece, depth), bf16),
            vmem((chips, pieces, piece, depth), bf16),
            vmem((chips, pieces, piece, depth), bf16),
            vmem((2 * pieces, piece, depth), bf16),
            vmem((piece, depth), f32),
            vmem((8, depth), f32),
            vmem((8, depth), f32),
            dma((kv_groups + 5,)),
            dma((chips, cores, kv_groups)),
            dma((chips, kv_groups)),
            dma((chips, kv_groups)),
            dma((count,)),
            dma((count,)),
            dma((2,)),
            dma((chips, cores, count)),
            dma((chips, count)),
            dma((chips, count)),
            dma((chips, count)),
            dma((chips, count)),
            dma((chips, cores)),
            dma((chips,)),
            dma((chips,)),
            dma((chips,)),
            dma((chips, 2 * pieces)),
            dma((chips, 2 * pieces)),
            dma((chips, pieces)),
            dma((chips, pieces)),
            dma((chips, pieces)),
            dma((chips, pieces)),
            dma((chips, pieces)),
            dma((2 * pieces,)),
            dma((2 * pieces,)),
        ],
        compiler_params=pltpu.CompilerParams(
            collective_id=0, has_side_effects=True, vmem_limit_bytes=VMEM_BYTES
        ),
        cost_estimate=pl.CostEstimate(
            flops=flops,
            bytes_accessed=2 * (project.size + gate_up.size + down.size),
            transcendentals=0,
        ),
    )(sinks, ids, route, gain, queries, keys_values, residual, project, gate_up, down)


def per_device_whole(
    queries,
    keys_values,
    sink_logits,
    residual,
    out_weight,
    norm_gain,
    expert_ids,
    route_weights,
    gate_up,
    down_weight,
):
    width = residual.shape[1]
    pairs = lax.axis_size("pair")
    chips = lax.axis_size("tok") // 2
    half = width // 2
    chunk = min(CHUNK, half // 128 * 128)
    piece = next(n for n in (PIECE, 160, 80, 48, 32, 16, half) if half % n == 0)
    own = min(OWN, half // chunk)
    out = whole_layer(
        (chips, pairs, chunk, piece, own),
        sink_logits,
        expert_ids.T,
        route_weights.T,
        norm_gain,
        queries,
        keys_values,
        residual.T,
        out_weight.T,
        jnp.transpose(gate_up[0], (1, 2, 0)).reshape(2 * down_weight.shape[1], width),
        down_weight[0],
    )
    return out.T


def solution(mesh):
    placed = (
        P(("groups", "tok"), ("head", "pair")),
        P(("groups", "tok"), ("head", "pair")),
        P(("head", "pair")),
        P(("groups", "tok"), None),
        P(("head", "pair"), None),
        P(),
        P(("groups", "tok"), None),
        P(("groups", "tok"), None),
        P("tok", None, None, ("head", "pair")),
        P("tok", ("head", "pair"), None),
    )
    sizes = mesh.shape
    chip_pair = sizes["pair"] == 1 and sizes["head"] == 2 and sizes["tok"] % 4 == 0
    return jax.shard_map(
        per_device_whole if chip_pair else per_device,
        mesh=mesh,
        in_specs=placed,
        out_specs=P(("groups", "tok"), ("head", "pair")),
        check_vma=False,
    )
```

```python
import functools

import jax
import jax.numpy as jnp
from jax import lax
from jax.experimental import pallas as pl
from jax.experimental.pallas import tpu as pltpu
from jax.sharding import PartitionSpec as P

HEAD_DIM = 64

MESH_ID = pl.DeviceIdType.MESH

VMEM_BYTES = 67_043_328
CHUNK = 512
PIECE = 480
JOINT = 1
OWN = 2


def moe_kernel(
    dims,
    parts_ref,
    residual_ref,
    gain_ref,
    tail_ref,
    gate_hbm,
    down_hbm,
    out_ref,
    gate_w,
    down_w,
    rows,
    part,
    from_core,
    kept,
    from_peer,
    hop,
    from_right,
    from_left,
    peer_parts,
    stream,
    squares,
    peer_squares,
    acc,
    parts_send,
    parts_recv,
    squares_send,
    squares_recv,
    load_sem,
    row_recv,
    row_right,
    row_left,
    row_peer,
    row_core,
    part_send,
    part_recv,
    peer_send,
    peer_recv,
    hop_send,
    right_recv,
    left_recv,
):
    chips, cores, shares, pairs, width = dims
    tok = lax.axis_index("tok")
    z = tok // cores
    c = tok % cores
    mine = lax.axis_index("head") * pairs + lax.axis_index("pair")
    other = cores - 1 - c

    def tok_id(chip, core):
        return {"tok": chip * cores + core}

    def peer_id(share):
        return {"head": share // pairs, "pair": share % pairs}

    def remote(src, dst, send, recv, target):
        return pltpu.make_async_remote_copy(
            src_ref=src, dst_ref=dst, send_sem=send, recv_sem=recv,
            device_id=target, device_id_type=MESH_ID,
        )

    loads = [
        pltpu.make_async_copy(gate_hbm, gate_w.at[:, :, pl.ds(0, width)], load_sem.at[0]),
        pltpu.make_async_copy(down_hbm, down_w, load_sem.at[1]),
    ]
    for load in loads:
        load.start()

    barrier = pltpu.get_barrier_semaphore()

    @pl.when(z > 0)
    def _():
        pl.semaphore_signal(barrier, 1, device_id=tok_id(z - 1, c), device_id_type=MESH_ID)

    @pl.when(z < chips - 1)
    def _():
        pl.semaphore_signal(barrier, 1, device_id=tok_id(z + 1, c), device_id_type=MESH_ID)

    if cores > 1:
        pl.semaphore_signal(barrier, 1, device_id=tok_id(z, other), device_id_type=MESH_ID)
    for d in range(1, shares):
        pl.semaphore_signal(
            barrier, 1, device_id=peer_id((mine + d) % shares), device_id_type=MESH_ID
        )
    sides = jnp.where(z > 0, 1, 0) + jnp.where(z < chips - 1, 1, 0)
    pl.semaphore_wait(barrier, sides + (cores - 1) + (shares - 1))

    def parts_copy(d):
        share = (mine + d) % shares
        return remote(
            parts_ref.at[share], peer_parts.at[mine], parts_send.at[d - 1],
            parts_recv.at[mine], peer_id(share),
        )

    def squares_copy(d):
        return remote(
            squares, peer_squares.at[mine], squares_send.at[d - 1],
            squares_recv.at[mine], peer_id((mine + d) % shares),
        )

    for d in range(1, shares):
        parts_copy(d).start()
    gate_w[:, :, width:, :] = jnp.zeros(
        gate_w.shape[:2] + (gate_w.shape[2] - width, gate_w.shape[3]), jnp.bfloat16
    )
    stream[...] = residual_ref[...].astype(jnp.float32) + parts_ref[mine].astype(jnp.float32)
    for d in range(1, shares):
        share = (mine + d) % shares
        slot = peer_parts.at[share]
        pltpu.make_async_copy(slot, slot, parts_recv.at[share]).wait()
        stream[...] += peer_parts[share].astype(jnp.float32)
    own = stream[...]
    square = jnp.sum(own * own, axis=1, keepdims=True)
    squares[...] = jnp.broadcast_to(square, squares.shape)
    for d in range(1, shares):
        squares_copy(d).start()
    total_square = squares[...]
    for d in range(1, shares):
        share = (mine + d) % shares
        slot = peer_squares.at[share]
        pltpu.make_async_copy(slot, slot, squares_recv.at[share]).wait()
        total_square += peer_squares[share]
    inverse = lax.rsqrt(total_square[:, :1] / (shares * width) + 1e-05)
    normed = stream[...] * inverse * gain_ref[...] + tail_ref[...].astype(jnp.float32)
    rows[z, mine, c] = normed.astype(jnp.bfloat16)

    near = jnp.minimum(z, chips - 1 - z)

    def chip_at(i):
        inner = jnp.where(i % 2 == 1, z - (i + 1) // 2, z + i // 2)
        outer = jnp.where(z < chips - 1 - z, i, chips - 1 - i)
        return jnp.where(i <= 2 * near, inner, outer)

    def row_copy(chip, share, core, send, target):
        slot = rows.at[chip, share, core]
        return remote(slot, slot, send, row_recv.at[chip, core, share], target)

    def go_right(chip):
        return (chip <= z) & (z < chips - 1)

    def go_left(chip):
        return (chip >= z) & (z > 0)

    def right_copy(chip):
        return row_copy(chip, mine, c, row_right.at[chip], tok_id(z + 1, c))

    def left_copy(chip):
        return row_copy(chip, mine, c, row_left.at[chip], tok_id(z - 1, c))

    def peer_copy(chip, d):
        return row_copy(chip, mine, c, row_peer.at[chip, d - 1], peer_id((mine + d) % shares))

    def core_copy(chip, share):
        return row_copy(chip, share, c, row_core.at[chip, share], tok_id(z, other))

    def row_wait(chip, share, core):
        slot = rows.at[chip, share, core]
        pltpu.make_async_copy(slot, slot, row_recv.at[chip, core, share]).wait()

    def forward(i):
        chip = chip_at(i)

        @pl.when(go_right(chip))
        def _():
            right_copy(chip).start()

        @pl.when(go_left(chip))
        def _():
            left_copy(chip).start()

        for d in range(1, shares):
            peer_copy(chip, d).start()
        if cores > 1:
            core_copy(chip, mine).start()

    forward(0)
    loads[0].wait()
    loads[1].wait()

    tail = (width // 128) * 128
    wide = rows.shape[-1]
    depth = rows.shape[-2]
    experts = chips * cores
    tail_lane = tail + lax.broadcasted_iota(jnp.int32, (cores * depth, wide - tail), 1)
    weight_lane = (tail_lane == width + tok) | (tail_lane == width + experts + tok)

    def kept_at(chip, share):
        return kept.at[chip, share] if cores > 1 else part.at[chip, share, 0]

    def part_copy(chip, share):
        return remote(
            part.at[chip, share, other], from_core.at[chip, share],
            part_send.at[chip, share], part_recv.at[chip, share], tok_id(z, other),
        )

    def sum_copy(chip, d):
        share = (mine + d) % shares
        return remote(
            kept_at(chip, share), from_peer.at[chip, mine],
            peer_send.at[chip, d - 1], peer_recv.at[chip, mine], peer_id(share),
        )

    def compute(i, carry):
        @pl.when(i + 1 < chips)
        def _():
            row_wait(chip_at(i + 1), mine, c)
            forward(i + 1)

        chip = chip_at(i)
        for d in range(1, shares):
            share = (mine + d) % shares
            row_wait(chip, share, c)
            if cores > 1:
                core_copy(chip, share).start()
        if cores > 1:
            for share in range(shares):
                row_wait(chip, share, other)
        gate = jnp.zeros((cores * depth, gate_w.shape[-1]), jnp.float32)
        up = gate
        for share in range(shares):
            block = rows[chip, share].reshape(cores * depth, wide)
            gate += jnp.dot(block, gate_w[0, share], preferred_element_type=jnp.float32)
            up += jnp.dot(block, gate_w[1, share], preferred_element_type=jnp.float32)
        active = (gate * jax.nn.sigmoid(1.702 * gate) * (up + 1.0)).astype(jnp.bfloat16)
        ends = rows[chip, 0, :, :, tail:].reshape(cores * depth, wide - tail).astype(jnp.float32)
        weight = jnp.sum(jnp.where(weight_lane, ends, 0.0), axis=1, keepdims=True)
        for share in range(shares):
            out = jnp.dot(active, down_w[share], preferred_element_type=jnp.float32)
            out = (out * weight).astype(jnp.bfloat16)
            part[chip, share] = out.reshape(cores, depth, width)
            if cores > 1:
                part_copy(chip, share).start()
        for share in range(shares):
            if cores > 1:
                part_copy(chip, share).wait_recv()
                total = part[chip, share, c].astype(jnp.float32)
                total += from_core[chip, share].astype(jnp.float32)
                kept[chip, share] = total.astype(jnp.bfloat16)
        for d in range(1, shares):
            sum_copy(chip, d).start()
        return carry

    lax.fori_loop(0, chips, compute, 0)

    def right_hop(chip):
        return remote(
            hop.at[chip], from_left.at[chip], hop_send.at[chip], left_recv.at[chip],
            tok_id(z + 1, c),
        )

    def left_hop(chip):
        return remote(
            hop.at[chip], from_right.at[chip], hop_send.at[chip], right_recv.at[chip],
            tok_id(z - 1, c),
        )

    def hop_wait(buffer, sem, chip):
        pltpu.make_async_copy(buffer.at[chip], buffer.at[chip], sem.at[chip]).wait()

    def give_back(j, carry):
        chip = chip_at(chips - 1 - j)
        total = kept_at(chip, mine)[...].astype(jnp.float32)
        for d in range(1, shares):
            share = (mine + d) % shares
            slot = from_peer.at[chip, share]
            pltpu.make_async_copy(slot, slot, peer_recv.at[chip, share]).wait()
            total += from_peer[chip, share].astype(jnp.float32)
        acc[...] = total

        @pl.when((chip <= z) & (z < chips - 1))
        def _():
            hop_wait(from_right, right_recv, chip)
            acc[...] += from_right[chip].astype(jnp.float32)

        @pl.when((chip >= z) & (z > 0))
        def _():
            hop_wait(from_left, left_recv, chip)
            acc[...] += from_left[chip].astype(jnp.float32)

        @pl.when(chip == z)
        def _():
            out_ref[...] = (stream[:, :width] + acc[...]).astype(jnp.bfloat16)

        @pl.when(chip != z)
        def _():
            hop[chip] = acc[...].astype(jnp.bfloat16)

        @pl.when(chip < z)
        def _():
            left_hop(chip).start()

        @pl.when(chip > z)
        def _():
            right_hop(chip).start()

        return carry

    lax.fori_loop(0, chips, give_back, 0)

    def drain(chip, carry):
        @pl.when(go_right(chip))
        def _():
            right_copy(chip).wait_send()

        @pl.when(go_left(chip))
        def _():
            left_copy(chip).wait_send()

        for d in range(1, shares):
            peer_copy(chip, d).wait_send()
            sum_copy(chip, d).wait_send()
        if cores > 1:
            for share in range(shares):
                core_copy(chip, share).wait_send()
                part_copy(chip, share).wait_send()

        @pl.when(chip < z)
        def _():
            left_hop(chip).wait_send()

        @pl.when(chip > z)
        def _():
            right_hop(chip).wait_send()

        return carry

    lax.fori_loop(0, chips, drain, 0)
    for d in range(1, shares):
        parts_copy(d).wait_send()
        squares_copy(d).wait_send()


def moe(dims, parts, residual, gain, tail, gate_w, down_w):
    chips, cores, shares, pairs, width = dims
    depth, wide = residual.shape
    hidden = down_w.shape[1]
    bf16 = jnp.bfloat16
    dma = pltpu.SemaphoreType.DMA
    return pl.pallas_call(
        functools.partial(moe_kernel, dims),
        out_shape=jax.ShapeDtypeStruct((depth, width), jnp.bfloat16),
        in_specs=[pl.BlockSpec(memory_space=pltpu.VMEM)] * 4
        + [
            pl.BlockSpec(memory_space=pl.ANY),
            pl.BlockSpec(memory_space=pl.ANY),
        ],
        out_specs=pl.BlockSpec(memory_space=pltpu.VMEM),
        scratch_shapes=[
            pltpu.VMEM((2, shares, wide, hidden), bf16),
            pltpu.VMEM(down_w.shape, bf16),
            pltpu.VMEM((chips, shares, cores, depth, wide), bf16),
            pltpu.VMEM((chips, shares, cores, depth, width), bf16),
            pltpu.VMEM((chips, shares, depth, width) if cores > 1 else (8, 128), bf16),
            pltpu.VMEM((chips, shares, depth, width) if cores > 1 else (8, 128), bf16),
            pltpu.VMEM((chips, shares, depth, width), bf16),
            pltpu.VMEM((chips, depth, width), bf16),
            pltpu.VMEM((chips, depth, width), bf16),
            pltpu.VMEM((chips, depth, width), bf16),
            pltpu.VMEM((shares, depth, wide), bf16),
            pltpu.VMEM((depth, wide), jnp.float32),
            pltpu.VMEM((depth, 128), jnp.float32),
            pltpu.VMEM((shares, depth, 128), jnp.float32),
            pltpu.VMEM((depth, width), jnp.float32),
            dma((max(shares - 1, 1),)),
            dma((shares,)),
            dma((max(shares - 1, 1),)),
            dma((shares,)),
            dma((2,)),
            dma((chips, cores, shares)),
            dma((chips,)),
            dma((chips,)),
            dma((chips, max(shares - 1, 1))),
            dma((chips, shares)),
            dma((chips, shares)),
            dma((chips, shares)),
            dma((chips, max(shares - 1, 1))),
            dma((chips, shares)),
            dma((chips,)),
            dma((chips,)),
            dma((chips,)),
        ],
        compiler_params=pltpu.CompilerParams(
            collective_id=0, has_side_effects=True, vmem_limit_bytes=60 * 1024 * 1024
        ),
        cost_estimate=pl.CostEstimate(
            flops=6 * chips * cores * depth * shares * width * hidden,
            bytes_accessed=6 * shares * width * hidden,
            transcendentals=0,
        ),
    )(parts, residual, gain, tail, gate_w, down_w)


def per_device(
    queries,
    keys_values,
    sink_logits,
    residual,
    out_weight,
    norm_gain,
    expert_ids,
    route_weights,
    gate_up,
    down_weight,
):
    tok_rows = queries.shape[0]
    kv_groups = keys_values.shape[1] // (2 * HEAD_DIM)
    local_heads = queries.shape[1] // HEAD_DIM
    repeat = local_heads // kv_groups
    position = lax.axis_index("tok") * tok_rows + jnp.arange(tok_rows, dtype=jnp.int32)
    grouped = queries.reshape(tok_rows, kv_groups, repeat, HEAD_DIM)
    start_max = jnp.broadcast_to(
        sink_logits.reshape(kv_groups, repeat)[:, :, None], (kv_groups, repeat, tok_rows)
    )
    start_totals = jnp.ones((kv_groups, repeat, tok_rows), jnp.float32)
    start_accum = jnp.zeros((kv_groups, repeat, tok_rows, HEAD_DIM), jnp.float32)
    key_piece = lax.all_gather(keys_values, "tok", axis=0, tiled=True)
    hidden = down_weight.shape[1]
    shares = lax.axis_size(("head", "pair"))
    share = out_weight.shape[1] // shares
    gate_w = jnp.transpose(gate_up[0], (1, 0, 2)).reshape(2, shares, share, hidden)
    down_w = jnp.transpose(down_weight[0].reshape(hidden, shares, share), (1, 0, 2))
    key_piece, gate_w, down_w = lax.optimization_barrier((key_piece, gate_w, down_w))
    totals = start_totals
    accum = start_accum
    count = key_piece.shape[0]
    split_piece = key_piece.reshape(count, kv_groups, 2, HEAD_DIM)
    scores = (
        jnp.einsum(
            "tgrd,ngd->grtn", grouped, split_piece[:, :, 0], preferred_element_type=jnp.float32
        )
        * 0.125
    )
    key_position = jnp.arange(count, dtype=jnp.int32)
    allowed = key_position[None, :] <= position[:, None]
    scores = jnp.where(allowed, scores, jnp.float32(-1e30))
    new_max = jnp.maximum(start_max, jnp.max(scores, axis=-1))
    decay = jnp.exp(start_max - new_max)
    weights = jnp.exp(scores - new_max[..., None])
    totals = totals * decay + jnp.sum(weights, axis=-1)
    update = jnp.einsum(
        "grtn,ngd->grtd",
        weights.astype(jnp.bfloat16),
        split_piece[:, :, 1],
        preferred_element_type=jnp.float32,
    )
    accum = accum * decay[..., None] + update
    final_max, totals, accum = (new_max, totals, accum)
    attended = (accum / totals[..., None]).astype(jnp.bfloat16)
    attended = jnp.transpose(attended, (2, 0, 1, 3)).reshape(tok_rows, local_heads * HEAD_DIM)
    width = out_weight.shape[1]
    share = width // lax.axis_size(("head", "pair"))
    column_start = lax.axis_index(("head", "pair")) * share
    partial_value = jnp.dot(attended, out_weight, preferred_element_type=jnp.float32)
    experts = lax.axis_size("tok")
    pairs = lax.axis_size("pair")
    cores = 2 // pairs
    shares = width // share
    wide = -(-(share + 2 * experts) // 128) * 128
    expert = jnp.arange(experts, dtype=jnp.int32)
    routed = expert_ids[:, :, None] == expert
    dense = jnp.sum(jnp.where(routed, route_weights[:, :, None], 0.0), axis=1)
    high = lax.reduce_precision(dense, 8, 7)
    weights = jnp.concatenate([high, dense - high], axis=1).astype(jnp.bfloat16)
    tail = jnp.pad(weights, ((0, 0), (share, wide - share - 2 * experts)))
    spare = (0, wide - share)
    parts = jnp.transpose(
        partial_value.astype(jnp.bfloat16).reshape(tok_rows, shares, share), (1, 0, 2)
    )
    parts = jnp.pad(parts, ((0, 0), (0, 0), spare))
    own_residual = jnp.pad(
        lax.dynamic_slice_in_dim(residual, column_start, share, 1), ((0, 0), spare)
    )
    own_gain = jnp.pad(lax.dynamic_slice_in_dim(norm_gain, column_start, share, 0), spare)
    return moe(
        (experts // cores, cores, shares, pairs, share),
        parts, own_residual, own_gain[None, :], tail, gate_w, down_w,
    )


def layer_kernel(
    dims,
    sink_ref,
    ids_ref,
    route_ref,
    gain_ref,
    query_hbm,
    kv_hbm,
    residual_hbm,
    project_hbm,
    gate_hbm,
    down_hbm,
    out_ref,
    query_v,
    query_t,
    kvs,
    row_max,
    row_total,
    accum,
    attended,
    residual_v,
    project_w,
    gate_w,
    down_v,
    down_t,
    gain_cols,
    stream,
    parts,
    peer_parts,
    rows,
    meta,
    hidden,
    active,
    part,
    kept,
    from_core,
    cross,
    from_peer,
    hop,
    relay,
    inbox,
    wide,
    acc,
    squares,
    peer_squares,
    load_sem,
    kv_recv,
    kv_core_send,
    kv_up_send,
    parts_send,
    parts_recv,
    squares_sem,
    row_recv,
    row_up,
    row_down,
    row_core,
    row_peer,
    meta_recv,
    meta_up,
    meta_down,
    meta_core,
    part_send,
    part_recv,
    peer_send,
    peer_recv,
    hop_send,
    relay_recv,
    inbox_recv,
    wide_send,
    wide_recv,
):
    chips, pairs, chunk, piece, own = dims
    cores = 2
    width, depth = residual_hbm.shape
    kv_groups = kvs.shape[1]
    repeat = query_t.shape[2] // depth
    half = width // 2
    f32, bf16 = jnp.float32, jnp.bfloat16
    far = (width - own * chunk) // 128 * 128
    edges = [(at, min(chunk, far - at)) for at in range(own * chunk, far, chunk)]
    if far + own * chunk < width:
        edges.append((far + own * chunk, width - far - own * chunk))
    spread_over = [(2 * own + n, at, size) for n, (at, size) in enumerate(edges)]
    pieces = half // piece
    joint = next(n for n in range(JOINT, 0, -1) if pieces % n == 0)
    last = chips - 1

    tok = lax.axis_index("tok")
    z = tok // cores
    c = tok % cores
    x = lax.axis_index("head") * pairs + lax.axis_index("pair")
    peer = {"head": (1 - x) // pairs, "pair": (1 - x) % pairs}
    other = {"tok": z * cores + (1 - c)}
    above = {"tok": (z + 1) * cores + c}
    below = {"tok": (z - 1) * cores + c}

    def remote(src, dst, send, recv, target):
        return pltpu.make_async_remote_copy(
            src_ref=src, dst_ref=dst, send_sem=send, recv_sem=recv,
            device_id=target, device_id_type=MESH_ID,
        )

    def landed(slot, sem):
        pltpu.make_async_copy(slot, slot, sem).wait()

    def mult(value, of):
        return pl.multiple_of(value, of)

    loads = [
        pltpu.make_async_copy(
            kv_hbm.at[:, pl.ds(g * 2 * HEAD_DIM, 2 * HEAD_DIM)], kvs.at[tok, g], load_sem.at[g]
        )
        for g in range(kv_groups)
    ]
    bulk = [
        pltpu.make_async_copy(src, dst, load_sem.at[kv_groups + i])
        for i, (src, dst) in enumerate(
            [
                (query_hbm, query_v),
                (residual_hbm, residual_v),
                (project_hbm, project_w),
                (down_hbm, down_v),
                (gate_hbm, gate_w),
            ]
        )
    ]
    for load in loads + bulk:
        load.start()

    barrier = pltpu.get_barrier_semaphore()

    @pl.when(z > 0)
    def _():
        pl.semaphore_signal(barrier, 1, device_id=below, device_id_type=MESH_ID)

    @pl.when(z < last)
    def _():
        pl.semaphore_signal(barrier, 1, device_id=above, device_id_type=MESH_ID)

    pl.semaphore_signal(barrier, 1, device_id=other, device_id_type=MESH_ID)
    pl.semaphore_signal(barrier, 1, device_id=peer, device_id_type=MESH_ID)
    sides = jnp.where(z > 0, 1, 0) + jnp.where(z < last, 1, 0)
    pl.semaphore_wait(barrier, sides + 2)

    def kv_up(chip, g):
        slot = kvs.at[chip * cores + c, g]
        return remote(slot, slot, kv_up_send.at[chip, g], kv_recv.at[chip, c, g], above)

    def kv_core(chip, g):
        slot = kvs.at[chip * cores + c, g]
        return remote(slot, slot, kv_core_send.at[chip, g], kv_recv.at[chip, c, g], other)

    def kv_wait(chip, core, g):
        landed(kvs.at[chip * cores + core, g], kv_recv.at[chip, core, g])

    def kv_pass(chip, g):
        @pl.when(z < last)
        def _():
            kv_up(chip, g).start()

        kv_core(chip, g).start()

    for g, load in enumerate(loads):
        load.wait()
        kv_pass(z, g)

    for b in range(-(-width // 128)):
        size = min(128, width - b * 128)
        gain = gain_ref[b * 128:b * 128 + size]
        gain_cols[b * 128:b * 128 + size, :] = jnp.broadcast_to(gain[None, :], (128, size)).T

    bulk[0].wait()
    for g in range(kv_groups):
        query_t[g, HEAD_DIM:, :] = jnp.zeros((HEAD_DIM, repeat * depth), bf16)
        for m in range(repeat // 2):
            lane = (g * repeat + 2 * m) * HEAD_DIM
            turned = (query_v[:, lane:lane + 2 * HEAD_DIM].astype(f32) * 0.125).T.astype(bf16)
            query_t[g, :HEAD_DIM, 2 * m * depth:(2 * m + 1) * depth] = turned[:HEAD_DIM]
            query_t[g, :HEAD_DIM, (2 * m + 1) * depth:(2 * m + 2) * depth] = turned[HEAD_DIM:]
        for r in range(repeat):
            row_max[g, :, r * depth:(r + 1) * depth] = jnp.full(
                (1, depth), sink_ref[g * repeat + r], f32
            )
    row_total[...] = jnp.ones(row_total.shape, f32)
    accum[...] = jnp.zeros(accum.shape, f32)

    def attend(chip, g, masked):
        keys = kvs[pl.ds(chip * cores, cores), g].reshape(cores * depth, 2 * HEAD_DIM)
        values = keys.astype(f32).T[HEAD_DIM:].astype(bf16)
        olds, totals, sums = row_max[g], row_total[g], accum[g]
        lanes = [slice(2 * m * depth, (2 * m + 2) * depth) for m in range(repeat // 2)]
        scores = [
            jnp.dot(keys, query_t[g, :, lane], preferred_element_type=f32) for lane in lanes
        ]
        if masked:
            row = lax.broadcasted_iota(jnp.int32, scores[0].shape, 0)
            column = lax.broadcasted_iota(jnp.int32, scores[0].shape, 1)
            column = jnp.where(column >= depth, column - depth, column)
            allowed = row <= c * depth + column
            scores = [jnp.where(allowed, score, jnp.float32(-1e30)) for score in scores]
        news = [
            jnp.maximum(olds[:, lane], jnp.max(score, axis=0, keepdims=True))
            for lane, score in zip(lanes, scores)
        ]
        weights = [jnp.exp(score - new) for score, new in zip(scores, news)]
        added = [
            jnp.dot(values, weight.astype(bf16), preferred_element_type=f32) for weight in weights
        ]
        for lane, new, weight, more in zip(lanes, news, weights, added):
            decay = jnp.exp(olds[:, lane] - new)
            row_max[g, :, lane] = new
            row_total[g, :, lane] = totals[:, lane] * decay + jnp.sum(
                weight, axis=0, keepdims=True
            )
            accum[g, :, lane] = sums[:, lane] * decay + more

    def attend_chip(chip, masked):
        def group(g, carry):
            kv_wait(chip, 1 - c, g)
            attend(chip, g, masked)

            @pl.when(chip > 0)
            def _():
                kv_wait(chip - 1, c, g)
                kv_pass(chip - 1, g)

            return carry

        lax.fori_loop(0, kv_groups, group, 0)

    attend_chip(z, True)

    def earlier(i, carry):
        attend_chip(z - i, False)
        return carry

    lax.fori_loop(1, z + 1, earlier, 0)

    for g in range(kv_groups):
        inverse = 1.0 / row_total[g]
        for r in range(repeat):
            lanes = slice(r * depth, (r + 1) * depth)
            head = (g * repeat + r) * HEAD_DIM
            attended[head:head + HEAD_DIM, :] = (accum[g, :, lanes] * inverse[:, lanes]).astype(bf16)

    def own_at(side, t):
        return mult(side * far + t * chunk, 128)

    def own_id(side, t):
        return side * own + t

    def parts_copy(n, start, size):
        return remote(
            parts.at[pl.ds(start, size)], peer_parts.at[pl.ds(start, size)],
            parts_send.at[n], parts_recv.at[n], peer,
        )

    def project(start, size):
        return jnp.dot(
            project_w[pl.ds(start, size), :], attended[...], preferred_element_type=f32
        )

    def give(n, start, size):
        value = project(start, size)
        parts[pl.ds(start, size), :] = value.astype(bf16)
        parts_copy(n, start, size).start()
        return value

    def hold(start, size, value):
        at = pl.ds(start, size)
        stream[at, :] = value + residual_v[at, :].astype(f32)

    def row_copy(chip, k, start, size, send, target):
        slot = rows.at[chip, c, pl.ds(start, size)]
        return remote(slot, slot, send.at[chip, k], row_recv.at[chip, c, k], target)

    def row_wait(chip, core, k, start, size):
        landed(rows.at[chip, core, pl.ds(start, size)], row_recv.at[chip, core, k])

    def pass_along(chip, k, start, size):
        @pl.when((chip <= z) & (z < last))
        def _():
            row_copy(chip, k, start, size, row_up, above).start()

        @pl.when((chip >= z) & (z > 0))
        def _():
            row_copy(chip, k, start, size, row_down, below).start()

    def meta_copy(chip, send, target):
        slot = meta.at[chip, c]
        return remote(slot, slot, send.at[chip], meta_recv.at[chip, c], target)

    def meta_wait(chip, core):
        landed(meta.at[chip, core], meta_recv.at[chip, core])

    def pass_meta(chip):
        @pl.when((chip <= z) & (z < last))
        def _():
            meta_copy(chip, meta_up, above).start()

        @pl.when((chip >= z) & (z > 0))
        def _():
            meta_copy(chip, meta_down, below).start()

        meta_copy(chip, meta_core, other).start()

    def settle(n, k, start, size):
        at = pl.ds(start, size)
        landed(peer_parts.at[at], parts_recv.at[n])
        value = stream[at, :] + peer_parts[at, :].astype(f32)
        stream[at, :] = value
        rows[z, c, at, :] = (value * gain_cols[at, :]).astype(bf16)
        pass_along(z, k, start, size)
        row_copy(z, k, start, size, row_core, other).start()
        return jnp.sum((value * value).reshape(size // 8, 8, depth), axis=0)

    bulk[1].wait()
    bulk[2].wait()

    def give_own(t, carry):
        give(t, own_at(1 - x, t), chunk)
        return carry

    lax.fori_loop(0, own, give_own, 0)
    squares_own = jnp.zeros((8, depth), f32)
    squares_all = jnp.zeros((8, depth), f32)
    for t in range(own):
        hold(own_at(x, t), chunk, project(own_at(x, t), chunk))
        for n, (k, start, size) in enumerate(spread_over):
            if t == 0:
                hold(start, size, give(own + n, start, size))
        squares_own += settle(t, own_id(x, t), own_at(x, t), chunk)
    squares[...] = squares_own
    squares_copy = remote(squares, peer_squares, squares_sem.at[0], squares_sem.at[1], peer)
    squares_copy.start()

    experts = chips * cores
    expert = lax.broadcasted_iota(jnp.int32, (experts, depth), 0)
    dense = jnp.zeros((experts, depth), f32)
    for k in range(ids_ref.shape[0]):
        dense += jnp.where(ids_ref[k:k + 1, :] == expert, route_ref[k:k + 1, :], 0.0)
    meta[z, c, pl.ds(8, experts), :] = dense
    bulk[3].wait()

    def turn(b, carry):
        at = pl.ds(mult(b * 128, 128), 128)
        down_t[at, :] = down_v[:, at].astype(f32).T.astype(bf16)
        return carry

    turns = width // 128
    if width % 128:
        at = pl.ds(turns * 128, width % 128)
        down_t[at, :] = down_v[:, at].astype(f32).T.astype(bf16)
    for n, (k, start, size) in enumerate(spread_over):
        if n < 2:
            lax.fori_loop(n * turns // 2, (n + 1) * turns // 2, turn, 0)
        squares_all += settle(own + n, k, start, size)
    if len(spread_over) < 2:
        lax.fori_loop(len(spread_over) * turns // 2, turns, turn, 0)
    landed(peer_squares, squares_sem.at[1])
    squares_all += squares[...] + peer_squares[...]
    total = jnp.sum(squares_all, axis=0, keepdims=True)
    scale = lax.rsqrt(total / width + 1e-05)
    meta[z, c, 0:8, :] = jnp.broadcast_to(scale, (8, depth))
    pass_meta(z)

    near = jnp.minimum(z, last - z)

    def chip_at(i):
        inner = jnp.where(i % 2 == 1, z - (i + 1) // 2, z + i // 2)
        outer = jnp.where(z < last - z, i, last - i)
        return jnp.where(i <= 2 * near, inner, outer)

    def each_side(i, act):
        @pl.when(z - 1 - i >= 0)
        def _():
            act(z - 1 - i)

        @pl.when(z + 1 + i <= last)
        def _():
            act(z + 1 + i)

    def pump(i, k, start, size, crosses):
        def act(chip):
            row_wait(chip, c, k, start, size)
            pass_along(chip, k, start, size)
            if crosses:
                row_copy(chip, k, start, size, row_peer, peer).start()
            row_copy(chip, k, start, size, row_core, other).start()

        each_side(i, act)

    def pump_own(i):
        def one(t, carry):
            pump(i, own_id(x, t), own_at(x, t), chunk, True)
            return carry

        lax.fori_loop(0, own, one, 0)

    def pump_shared(i):
        for k, start, size in spread_over:
            pump(i, k, start, size, False)

        def act(chip):
            meta_wait(chip, c)
            pass_meta(chip)

        each_side(i, act)

    def cross_in(chip):
        def one(t, carry):
            k, start = own_id(1 - x, t), own_at(1 - x, t)
            row_wait(chip, c, k, start, chunk)
            row_copy(chip, k, start, chunk, row_core, other).start()
            return carry

        lax.fori_loop(0, own, one, 0)

    def multiply(chip, k, start, size):
        row_wait(chip, 1 - c, k, start, size)
        at = pl.ds(start, size)
        pair = jnp.concatenate([rows[chip, c, at, :], rows[chip, 1 - c, at, :]], axis=1)
        units = hidden.shape[0] // 2
        for side in range(2):
            lot = slice(side * units, (side + 1) * units)
            hidden[lot] += jnp.dot(gate_w[lot, at], pair, preferred_element_type=f32)

    def multiply_line(chip):
        hidden[...] = jnp.zeros(hidden.shape, f32)

        def one(t, carry):
            multiply(chip, own_id(x, t), own_at(x, t), chunk)
            return carry

        lax.fori_loop(0, own, one, 0)
        for k, start, size in spread_over:
            multiply(chip, k, start, size)

    def multiply_crossed(chip):
        def one(t, carry):
            multiply(chip, own_id(1 - x, t), own_at(1 - x, t), chunk)
            return carry

        lax.fori_loop(0, own, one, 0)

    def part_copy(chip, r):
        return remote(
            part.at[chip, r], from_core.at[chip, r], part_send.at[chip, r],
            part_recv.at[chip, r], other,
        )

    def cross_copy(chip, r):
        return remote(
            cross.at[chip, r], from_peer.at[chip, r], peer_send.at[chip, r],
            peer_recv.at[chip, r], peer,
        )

    def far_end(chip):
        return chip == jnp.where(chip > z, last, 0)

    def adds(chip):
        return far_end(chip) & (jnp.where(chip > z, z, last - z) % 2 == 1) & (chip != partner)

    def relay_copy(chip, u):
        return remote(
            hop.at[chip, u], relay.at[chip, u], hop_send.at[chip, u],
            relay_recv.at[chip, u], {"tok": tok + jnp.where(chip > z, cores, -cores)},
        )

    def final_copy(chip, u):
        return remote(
            hop.at[chip, u], inbox.at[z, u], hop_send.at[chip, u],
            inbox_recv.at[z, u], {"tok": chip * cores + c},
        )

    partner = z + 1 - 2 * (z % 2)

    def wide_copy(at):
        return remote(
            kept.at[partner, at], wide.at[at], wide_send.at[at], wide_recv.at[at],
            {"tok": partner * cores + c},
        )

    def send_sum(chip, low, high):
        direct = adds(chip) | jnp.logical_not(far_end(chip))

        def one(u, carry):
            landed(from_peer.at[chip, u], peer_recv.at[chip, u])
            acc[...] = kept[chip, x * pieces + u].astype(f32) + from_peer[chip, u].astype(f32)

            @pl.when(adds(chip))
            def _():
                landed(relay.at[chip, u], relay_recv.at[chip, u])
                acc[...] += relay[chip, u].astype(f32)

            hop[chip, u] = acc[...].astype(bf16)

            @pl.when(direct)
            def _():
                final_copy(chip, u).start()

            @pl.when(jnp.logical_not(direct))
            def _():
                relay_copy(chip, u).start()

            return carry

        lax.fori_loop(low, high, one, 0)

    def send_own_sum(chip, low, high):
        @pl.when((chip != partner) & jnp.logical_not(adds(chip)))
        def _():
            send_sum(chip, low, high)

    def activate(chip):
        meta_wait(chip, 1 - c)
        scale = jnp.concatenate([meta[chip, c, 0:1, :], meta[chip, 1 - c, 0:1, :]], axis=1)
        weight = jnp.concatenate(
            [meta[chip, c, pl.ds(8 + tok, 1), :], meta[chip, 1 - c, pl.ds(8 + tok, 1), :]], axis=1
        )
        units = hidden.shape[0] // 2
        gate = hidden[:units] * scale
        up = hidden[units:] * scale
        active[...] = (gate * jax.nn.sigmoid(1.702 * gate) * (up + 1.0) * weight).astype(bf16)

    def spread_out(chip, between=None):
        def spread(n, carry):
            first = joint * n
            first = jnp.where(first < pieces, (1 - x) * pieces + first, x * pieces + first - pieces)
            value = jnp.dot(
                down_t[pl.ds(mult(first * piece, 16), joint * piece), :], active[...],
                preferred_element_type=f32,
            )
            for m in range(joint):
                at = first + m
                block = value[m * piece:(m + 1) * piece]
                part[chip, at] = block[:, depth:].astype(bf16)
                part_copy(chip, at).start()
                kept[chip, at] = block[:, :depth].astype(bf16)
            return carry

        lax.fori_loop(0, 2 * pieces // joint, spread, 0)
        if between is not None:
            between()

        def summed(at):
            landed(from_core.at[chip, at], part_recv.at[chip, at])
            acc[...] = kept[chip, at].astype(f32) + from_core[chip, at].astype(f32)

            @pl.when(chip == z)
            def _():
                landed(wide.at[at], wide_recv.at[at])
                acc[...] += wide[at].astype(f32)

        def keep(at):
            kept[chip, at] = acc[...].astype(bf16)

            @pl.when(chip == partner)
            def _():
                wide_copy(at).start()

        def give_half(r, carry):
            at = (1 - x) * pieces + r
            summed(at)

            @pl.when(chip == partner)
            def _():
                keep(at)

            @pl.when(chip != partner)
            def _():
                cross[chip, r] = acc[...].astype(bf16)
                cross_copy(chip, r).start()

            return carry

        lax.fori_loop(0, pieces, give_half, 0)

        def keep_half(r, carry):
            summed(x * pieces + r)
            keep(x * pieces + r)
            return carry

        lax.fori_loop(0, pieces, keep_half, 0)

    is_end = (z == 0) | (z == last)
    early = z < chips // 2

    def own_across():
        for t in range(own):
            row_copy(z, own_id(x, t), own_at(x, t), chunk, row_peer, peer).start()

    @pl.when(early)
    def _():
        own_across()

    bulk[4].wait()
    pump_own(0)
    pump_shared(0)

    @pl.when(jnp.logical_not(early))
    def _():
        own_across()


    def step(i, carry):
        chip = chip_at(i)
        multiply_line(chip)

        pump_own(i)

        @pl.when(jnp.logical_not(is_end))
        def _():
            pump_shared(i)

        each_side(i - 1, cross_in)
        multiply_crossed(chip)

        @pl.when(i > 1)
        def _():
            send_own_sum(chip_at(i - 1), 0, pieces // 2)

        def between():
            @pl.when(is_end)
            def _():
                pump_shared(i)

        activate(chip)
        spread_out(chip, between)

        @pl.when(i > 1)
        def _():
            send_own_sum(chip_at(i - 1), pieces // 2, pieces)

        return carry

    lax.fori_loop(1, chips, step, 0)
    multiply_line(z)
    cross_in(z)
    multiply_crossed(z)
    activate(z)
    cuts = [pieces * n // 3 for n in range(4)]

    def send_last(n):
        send_own_sum(chip_at(last), cuts[n], cuts[n + 1])

    send_last(0)
    spread_out(z, lambda: send_last(1))
    send_last(2)

    def send_added(i, carry):
        @pl.when(adds(chip_at(i)))
        def _():
            send_sum(chip_at(i), 0, pieces)

        return carry

    lax.fori_loop(1, chips, send_added, 0)

    def finish(r, carry):
        at = pl.ds(mult(x * half + r * piece, 16), piece)
        landed(from_peer.at[z, r], peer_recv.at[z, r])
        acc[...] = kept[z, x * pieces + r].astype(f32) + from_peer[z, r].astype(f32)
        for src in range(chips):
            below_it = (src < z) & ((z < last) | (src % 2 == 1))
            above_it = (src > z) & ((z > 0) | ((last - src) % 2 == 1))

            @pl.when((below_it | above_it) & (src != partner))
            def _():
                landed(inbox.at[src, r], inbox_recv.at[src, r])
                acc[...] += inbox[src, r].astype(f32)

        out_ref[pl.ds(mult(r * piece, piece), piece), :] = (stream[at, :] + acc[...]).astype(bf16)
        return carry

    lax.fori_loop(0, pieces, finish, 0)

    def drain(chip, carry):
        for g in range(kv_groups):
            @pl.when(chip <= z)
            def _():
                kv_core(chip, g).wait_send()

            @pl.when((chip <= z) & (z < last))
            def _():
                kv_up(chip, g).wait_send()

        def sent(k, start, size, on_line, crosses):
            if on_line:
                @pl.when((chip <= z) & (z < last))
                def _():
                    row_copy(chip, k, start, size, row_up, above).wait_send()

                @pl.when((chip >= z) & (z > 0))
                def _():
                    row_copy(chip, k, start, size, row_down, below).wait_send()

            if crosses:
                row_copy(chip, k, start, size, row_peer, peer).wait_send()

            row_copy(chip, k, start, size, row_core, other).wait_send()

        for t in range(own):
            sent(own_id(x, t), own_at(x, t), chunk, True, True)
            sent(own_id(1 - x, t), own_at(1 - x, t), chunk, False, False)
        for k, start, size in spread_over:
            sent(k, start, size, True, False)

        @pl.when((chip <= z) & (z < last))
        def _():
            meta_copy(chip, meta_up, above).wait_send()

        @pl.when((chip >= z) & (z > 0))
        def _():
            meta_copy(chip, meta_down, below).wait_send()

        meta_copy(chip, meta_core, other).wait_send()
        for r in range(2 * pieces):
            part_copy(chip, r).wait_send()
        @pl.when(chip != partner)
        def _():
            for r in range(pieces):
                cross_copy(chip, r).wait_send()

        @pl.when(chip == partner)
        def _():
            for r in range(2 * pieces):
                wide_copy(r).wait_send()

        @pl.when((chip != z) & (chip != partner))
        def _():
            for u in range(pieces):
                final_copy(chip, u).wait_send()

        return carry

    lax.fori_loop(0, chips, drain, 0)
    for t in range(own):
        parts_copy(t, own_at(1 - x, t), chunk).wait_send()
    for n, (k, start, size) in enumerate(spread_over):
        parts_copy(own + n, start, size).wait_send()
    squares_copy.wait_send()


def whole_layer(
    dims, sinks, ids, route, gain, queries, keys_values, residual, project, gate_up, down
):
    chips, pairs, chunk, piece, own = dims
    cores = 2
    width, depth = residual.shape
    kv_groups = keys_values.shape[1] // (2 * HEAD_DIM)
    heads = queries.shape[1] // HEAD_DIM
    repeat = heads // kv_groups
    hidden = down.shape[0]
    half = width // 2
    pieces = half // piece
    count = -(-width // chunk) + 2
    bf16, f32 = jnp.bfloat16, jnp.float32
    dma = pltpu.SemaphoreType.DMA
    vmem = pltpu.VMEM
    experts = chips * cores
    flops = 2 * width * (
        depth * heads * HEAD_DIM + chips * cores * depth * 3 * hidden
    )
    return pl.pallas_call(
        functools.partial(layer_kernel, dims),
        out_shape=jax.ShapeDtypeStruct((half, depth), bf16),
        in_specs=[pl.BlockSpec(memory_space=pltpu.SMEM)]
        + [pl.BlockSpec(memory_space=pltpu.VMEM)] * 3
        + [pl.BlockSpec(memory_space=pl.ANY)] * 6,
        out_specs=pl.BlockSpec(memory_space=pltpu.VMEM),
        scratch_shapes=[
            vmem(queries.shape, bf16),
            vmem((kv_groups, 2 * HEAD_DIM, repeat * depth), bf16),
            vmem((experts, kv_groups, depth, 2 * HEAD_DIM), bf16),
            vmem((kv_groups, 1, repeat * depth), f32),
            vmem((kv_groups, 1, repeat * depth), f32),
            vmem((kv_groups, HEAD_DIM, repeat * depth), f32),
            vmem((heads * HEAD_DIM, depth), bf16),
            vmem(residual.shape, bf16),
            vmem(project.shape, bf16),
            vmem(gate_up.shape, bf16),
            vmem(down.shape, bf16),
            vmem((width, hidden), bf16),
            vmem((width, depth), f32),
            vmem((width, depth), f32),
            vmem((width, depth), bf16),
            vmem((width, depth), bf16),
            vmem((chips, cores, width, depth), bf16),
            vmem((chips, cores, 8 + experts, depth), f32),
            vmem((2 * hidden, cores * depth), f32),
            vmem((hidden, cores * depth), bf16),
            vmem((chips, 2 * pieces, piece, depth), bf16),
            vmem((chips, 2 * pieces, piece, depth), bf16),
            vmem((chips, 2 * pieces, piece, depth), bf16),
            vmem((chips, pieces, piece, depth), bf16),
            vmem((chips, pieces, piece, depth), bf16),
            vmem((chips, pieces, piece, depth), bf16),
            vmem((chips, pieces, piece, depth), bf16),
            vmem((chips, pieces, piece, depth), bf16),
            vmem((2 * pieces, piece, depth), bf16),
            vmem((piece, depth), f32),
            vmem((8, depth), f32),
            vmem((8, depth), f32),
            dma((kv_groups + 5,)),
            dma((chips, cores, kv_groups)),
            dma((chips, kv_groups)),
            dma((chips, kv_groups)),
            dma((count,)),
            dma((count,)),
            dma((2,)),
            dma((chips, cores, count)),
            dma((chips, count)),
            dma((chips, count)),
            dma((chips, count)),
            dma((chips, count)),
            dma((chips, cores)),
            dma((chips,)),
            dma((chips,)),
            dma((chips,)),
            dma((chips, 2 * pieces)),
            dma((chips, 2 * pieces)),
            dma((chips, pieces)),
            dma((chips, pieces)),
            dma((chips, pieces)),
            dma((chips, pieces)),
            dma((chips, pieces)),
            dma((2 * pieces,)),
            dma((2 * pieces,)),
        ],
        compiler_params=pltpu.CompilerParams(
            collective_id=0, has_side_effects=True, vmem_limit_bytes=VMEM_BYTES
        ),
        cost_estimate=pl.CostEstimate(
            flops=flops,
            bytes_accessed=2 * (project.size + gate_up.size + down.size),
            transcendentals=0,
        ),
    )(sinks, ids, route, gain, queries, keys_values, residual, project, gate_up, down)


def per_device_whole(
    queries,
    keys_values,
    sink_logits,
    residual,
    out_weight,
    norm_gain,
    expert_ids,
    route_weights,
    gate_up,
    down_weight,
):
    width = residual.shape[1]
    pairs = lax.axis_size("pair")
    chips = lax.axis_size("tok") // 2
    half = width // 2
    chunk = min(CHUNK, half // 128 * 128)
    piece = next(n for n in (PIECE, 160, 80, 48, 32, 16, half) if half % n == 0)
    own = min(OWN, half // chunk)
    out = whole_layer(
        (chips, pairs, chunk, piece, own),
        sink_logits,
        expert_ids.T,
        route_weights.T,
        norm_gain,
        queries,
        keys_values,
        residual.T,
        out_weight.T,
        jnp.transpose(gate_up[0], (1, 2, 0)).reshape(2 * down_weight.shape[1], width),
        down_weight[0],
    )
    return out.T


def solution(mesh):
    placed = (
        P(("groups", "tok"), ("head", "pair")),
        P(("groups", "tok"), ("head", "pair")),
        P(("head", "pair")),
        P(("groups", "tok"), None),
        P(("head", "pair"), None),
        P(),
        P(("groups", "tok"), None),
        P(("groups", "tok"), None),
        P("tok", None, None, ("head", "pair")),
        P("tok", ("head", "pair"), None),
    )
    sizes = mesh.shape
    chip_pair = sizes["pair"] == 1 and sizes["head"] == 2 and sizes["tok"] % 4 == 0
    return jax.shard_map(
        per_device_whole if chip_pair else per_device,
        mesh=mesh,
        in_specs=placed,
        out_specs=P(("groups", "tok"), ("head", "pair")),
        check_vma=False,
    )
```

```python
import functools

import jax
import jax.numpy as jnp
from jax import lax
from jax.experimental import pallas as pl
from jax.experimental.pallas import tpu as pltpu
from jax.sharding import PartitionSpec as P

HEAD_DIM = 64

MESH_ID = pl.DeviceIdType.MESH

VMEM_BYTES = 67_043_328
CHUNK = 512
PIECE = 480
JOINT = 1
OWN = 2


def moe_kernel(
    dims,
    parts_ref,
    residual_ref,
    gain_ref,
    tail_ref,
    gate_hbm,
    down_hbm,
    out_ref,
    gate_w,
    down_w,
    rows,
    part,
    from_core,
    kept,
    from_peer,
    hop,
    from_right,
    from_left,
    peer_parts,
    stream,
    squares,
    peer_squares,
    acc,
    parts_send,
    parts_recv,
    squares_send,
    squares_recv,
    load_sem,
    row_recv,
    row_right,
    row_left,
    row_peer,
    row_core,
    part_send,
    part_recv,
    peer_send,
    peer_recv,
    hop_send,
    right_recv,
    left_recv,
):
    chips, cores, shares, pairs, width = dims
    tok = lax.axis_index("tok")
    z = tok // cores
    c = tok % cores
    mine = lax.axis_index("head") * pairs + lax.axis_index("pair")
    other = cores - 1 - c

    def tok_id(chip, core):
        return {"tok": chip * cores + core}

    def peer_id(share):
        return {"head": share // pairs, "pair": share % pairs}

    def remote(src, dst, send, recv, target):
        return pltpu.make_async_remote_copy(
            src_ref=src, dst_ref=dst, send_sem=send, recv_sem=recv,
            device_id=target, device_id_type=MESH_ID,
        )

    loads = [
        pltpu.make_async_copy(gate_hbm, gate_w.at[:, :, pl.ds(0, width)], load_sem.at[0]),
        pltpu.make_async_copy(down_hbm, down_w, load_sem.at[1]),
    ]
    for load in loads:
        load.start()

    barrier = pltpu.get_barrier_semaphore()

    @pl.when(z > 0)
    def _():
        pl.semaphore_signal(barrier, 1, device_id=tok_id(z - 1, c), device_id_type=MESH_ID)

    @pl.when(z < chips - 1)
    def _():
        pl.semaphore_signal(barrier, 1, device_id=tok_id(z + 1, c), device_id_type=MESH_ID)

    if cores > 1:
        pl.semaphore_signal(barrier, 1, device_id=tok_id(z, other), device_id_type=MESH_ID)
    for d in range(1, shares):
        pl.semaphore_signal(
            barrier, 1, device_id=peer_id((mine + d) % shares), device_id_type=MESH_ID
        )
    sides = jnp.where(z > 0, 1, 0) + jnp.where(z < chips - 1, 1, 0)
    pl.semaphore_wait(barrier, sides + (cores - 1) + (shares - 1))

    def parts_copy(d):
        share = (mine + d) % shares
        return remote(
            parts_ref.at[share], peer_parts.at[mine], parts_send.at[d - 1],
            parts_recv.at[mine], peer_id(share),
        )

    def squares_copy(d):
        return remote(
            squares, peer_squares.at[mine], squares_send.at[d - 1],
            squares_recv.at[mine], peer_id((mine + d) % shares),
        )

    for d in range(1, shares):
        parts_copy(d).start()
    gate_w[:, :, width:, :] = jnp.zeros(
        gate_w.shape[:2] + (gate_w.shape[2] - width, gate_w.shape[3]), jnp.bfloat16
    )
    stream[...] = residual_ref[...].astype(jnp.float32) + parts_ref[mine].astype(jnp.float32)
    for d in range(1, shares):
        share = (mine + d) % shares
        slot = peer_parts.at[share]
        pltpu.make_async_copy(slot, slot, parts_recv.at[share]).wait()
        stream[...] += peer_parts[share].astype(jnp.float32)
    own = stream[...]
    square = jnp.sum(own * own, axis=1, keepdims=True)
    squares[...] = jnp.broadcast_to(square, squares.shape)
    for d in range(1, shares):
        squares_copy(d).start()
    total_square = squares[...]
    for d in range(1, shares):
        share = (mine + d) % shares
        slot = peer_squares.at[share]
        pltpu.make_async_copy(slot, slot, squares_recv.at[share]).wait()
        total_square += peer_squares[share]
    inverse = lax.rsqrt(total_square[:, :1] / (shares * width) + 1e-05)
    normed = stream[...] * inverse * gain_ref[...] + tail_ref[...].astype(jnp.float32)
    rows[z, mine, c] = normed.astype(jnp.bfloat16)

    near = jnp.minimum(z, chips - 1 - z)

    def chip_at(i):
        inner = jnp.where(i % 2 == 1, z - (i + 1) // 2, z + i // 2)
        outer = jnp.where(z < chips - 1 - z, i, chips - 1 - i)
        return jnp.where(i <= 2 * near, inner, outer)

    def row_copy(chip, share, core, send, target):
        slot = rows.at[chip, share, core]
        return remote(slot, slot, send, row_recv.at[chip, core, share], target)

    def go_right(chip):
        return (chip <= z) & (z < chips - 1)

    def go_left(chip):
        return (chip >= z) & (z > 0)

    def right_copy(chip):
        return row_copy(chip, mine, c, row_right.at[chip], tok_id(z + 1, c))

    def left_copy(chip):
        return row_copy(chip, mine, c, row_left.at[chip], tok_id(z - 1, c))

    def peer_copy(chip, d):
        return row_copy(chip, mine, c, row_peer.at[chip, d - 1], peer_id((mine + d) % shares))

    def core_copy(chip, share):
        return row_copy(chip, share, c, row_core.at[chip, share], tok_id(z, other))

    def row_wait(chip, share, core):
        slot = rows.at[chip, share, core]
        pltpu.make_async_copy(slot, slot, row_recv.at[chip, core, share]).wait()

    def forward(i):
        chip = chip_at(i)

        @pl.when(go_right(chip))
        def _():
            right_copy(chip).start()

        @pl.when(go_left(chip))
        def _():
            left_copy(chip).start()

        for d in range(1, shares):
            peer_copy(chip, d).start()
        if cores > 1:
            core_copy(chip, mine).start()

    forward(0)
    loads[0].wait()
    loads[1].wait()

    tail = (width // 128) * 128
    wide = rows.shape[-1]
    depth = rows.shape[-2]
    experts = chips * cores
    tail_lane = tail + lax.broadcasted_iota(jnp.int32, (cores * depth, wide - tail), 1)
    weight_lane = (tail_lane == width + tok) | (tail_lane == width + experts + tok)

    def kept_at(chip, share):
        return kept.at[chip, share] if cores > 1 else part.at[chip, share, 0]

    def part_copy(chip, share):
        return remote(
            part.at[chip, share, other], from_core.at[chip, share],
            part_send.at[chip, share], part_recv.at[chip, share], tok_id(z, other),
        )

    def sum_copy(chip, d):
        share = (mine + d) % shares
        return remote(
            kept_at(chip, share), from_peer.at[chip, mine],
            peer_send.at[chip, d - 1], peer_recv.at[chip, mine], peer_id(share),
        )

    def compute(i, carry):
        @pl.when(i + 1 < chips)
        def _():
            row_wait(chip_at(i + 1), mine, c)
            forward(i + 1)

        chip = chip_at(i)
        for d in range(1, shares):
            share = (mine + d) % shares
            row_wait(chip, share, c)
            if cores > 1:
                core_copy(chip, share).start()
        if cores > 1:
            for share in range(shares):
                row_wait(chip, share, other)
        gate = jnp.zeros((cores * depth, gate_w.shape[-1]), jnp.float32)
        up = gate
        for share in range(shares):
            block = rows[chip, share].reshape(cores * depth, wide)
            gate += jnp.dot(block, gate_w[0, share], preferred_element_type=jnp.float32)
            up += jnp.dot(block, gate_w[1, share], preferred_element_type=jnp.float32)
        active = (gate * jax.nn.sigmoid(1.702 * gate) * (up + 1.0)).astype(jnp.bfloat16)
        ends = rows[chip, 0, :, :, tail:].reshape(cores * depth, wide - tail).astype(jnp.float32)
        weight = jnp.sum(jnp.where(weight_lane, ends, 0.0), axis=1, keepdims=True)
        for share in range(shares):
            out = jnp.dot(active, down_w[share], preferred_element_type=jnp.float32)
            out = (out * weight).astype(jnp.bfloat16)
            part[chip, share] = out.reshape(cores, depth, width)
            if cores > 1:
                part_copy(chip, share).start()
        for share in range(shares):
            if cores > 1:
                part_copy(chip, share).wait_recv()
                total = part[chip, share, c].astype(jnp.float32)
                total += from_core[chip, share].astype(jnp.float32)
                kept[chip, share] = total.astype(jnp.bfloat16)
        for d in range(1, shares):
            sum_copy(chip, d).start()
        return carry

    lax.fori_loop(0, chips, compute, 0)

    def right_hop(chip):
        return remote(
            hop.at[chip], from_left.at[chip], hop_send.at[chip], left_recv.at[chip],
            tok_id(z + 1, c),
        )

    def left_hop(chip):
        return remote(
            hop.at[chip], from_right.at[chip], hop_send.at[chip], right_recv.at[chip],
            tok_id(z - 1, c),
        )

    def hop_wait(buffer, sem, chip):
        pltpu.make_async_copy(buffer.at[chip], buffer.at[chip], sem.at[chip]).wait()

    def give_back(j, carry):
        chip = chip_at(chips - 1 - j)
        total = kept_at(chip, mine)[...].astype(jnp.float32)
        for d in range(1, shares):
            share = (mine + d) % shares
            slot = from_peer.at[chip, share]
            pltpu.make_async_copy(slot, slot, peer_recv.at[chip, share]).wait()
            total += from_peer[chip, share].astype(jnp.float32)
        acc[...] = total

        @pl.when((chip <= z) & (z < chips - 1))
        def _():
            hop_wait(from_right, right_recv, chip)
            acc[...] += from_right[chip].astype(jnp.float32)

        @pl.when((chip >= z) & (z > 0))
        def _():
            hop_wait(from_left, left_recv, chip)
            acc[...] += from_left[chip].astype(jnp.float32)

        @pl.when(chip == z)
        def _():
            out_ref[...] = (stream[:, :width] + acc[...]).astype(jnp.bfloat16)

        @pl.when(chip != z)
        def _():
            hop[chip] = acc[...].astype(jnp.bfloat16)

        @pl.when(chip < z)
        def _():
            left_hop(chip).start()

        @pl.when(chip > z)
        def _():
            right_hop(chip).start()

        return carry

    lax.fori_loop(0, chips, give_back, 0)

    def drain(chip, carry):
        @pl.when(go_right(chip))
        def _():
            right_copy(chip).wait_send()

        @pl.when(go_left(chip))
        def _():
            left_copy(chip).wait_send()

        for d in range(1, shares):
            peer_copy(chip, d).wait_send()
            sum_copy(chip, d).wait_send()
        if cores > 1:
            for share in range(shares):
                core_copy(chip, share).wait_send()
                part_copy(chip, share).wait_send()

        @pl.when(chip < z)
        def _():
            left_hop(chip).wait_send()

        @pl.when(chip > z)
        def _():
            right_hop(chip).wait_send()

        return carry

    lax.fori_loop(0, chips, drain, 0)
    for d in range(1, shares):
        parts_copy(d).wait_send()
        squares_copy(d).wait_send()


def moe(dims, parts, residual, gain, tail, gate_w, down_w):
    chips, cores, shares, pairs, width = dims
    depth, wide = residual.shape
    hidden = down_w.shape[1]
    bf16 = jnp.bfloat16
    dma = pltpu.SemaphoreType.DMA
    return pl.pallas_call(
        functools.partial(moe_kernel, dims),
        out_shape=jax.ShapeDtypeStruct((depth, width), jnp.bfloat16),
        in_specs=[pl.BlockSpec(memory_space=pltpu.VMEM)] * 4
        + [
            pl.BlockSpec(memory_space=pl.ANY),
            pl.BlockSpec(memory_space=pl.ANY),
        ],
        out_specs=pl.BlockSpec(memory_space=pltpu.VMEM),
        scratch_shapes=[
            pltpu.VMEM((2, shares, wide, hidden), bf16),
            pltpu.VMEM(down_w.shape, bf16),
            pltpu.VMEM((chips, shares, cores, depth, wide), bf16),
            pltpu.VMEM((chips, shares, cores, depth, width), bf16),
            pltpu.VMEM((chips, shares, depth, width) if cores > 1 else (8, 128), bf16),
            pltpu.VMEM((chips, shares, depth, width) if cores > 1 else (8, 128), bf16),
            pltpu.VMEM((chips, shares, depth, width), bf16),
            pltpu.VMEM((chips, depth, width), bf16),
            pltpu.VMEM((chips, depth, width), bf16),
            pltpu.VMEM((chips, depth, width), bf16),
            pltpu.VMEM((shares, depth, wide), bf16),
            pltpu.VMEM((depth, wide), jnp.float32),
            pltpu.VMEM((depth, 128), jnp.float32),
            pltpu.VMEM((shares, depth, 128), jnp.float32),
            pltpu.VMEM((depth, width), jnp.float32),
            dma((max(shares - 1, 1),)),
            dma((shares,)),
            dma((max(shares - 1, 1),)),
            dma((shares,)),
            dma((2,)),
            dma((chips, cores, shares)),
            dma((chips,)),
            dma((chips,)),
            dma((chips, max(shares - 1, 1))),
            dma((chips, shares)),
            dma((chips, shares)),
            dma((chips, shares)),
            dma((chips, max(shares - 1, 1))),
            dma((chips, shares)),
            dma((chips,)),
            dma((chips,)),
            dma((chips,)),
        ],
        compiler_params=pltpu.CompilerParams(
            collective_id=0, has_side_effects=True, vmem_limit_bytes=60 * 1024 * 1024
        ),
        cost_estimate=pl.CostEstimate(
            flops=6 * chips * cores * depth * shares * width * hidden,
            bytes_accessed=6 * shares * width * hidden,
            transcendentals=0,
        ),
    )(parts, residual, gain, tail, gate_w, down_w)


def per_device(
    queries,
    keys_values,
    sink_logits,
    residual,
    out_weight,
    norm_gain,
    expert_ids,
    route_weights,
    gate_up,
    down_weight,
):
    tok_rows = queries.shape[0]
    kv_groups = keys_values.shape[1] // (2 * HEAD_DIM)
    local_heads = queries.shape[1] // HEAD_DIM
    repeat = local_heads // kv_groups
    position = lax.axis_index("tok") * tok_rows + jnp.arange(tok_rows, dtype=jnp.int32)
    grouped = queries.reshape(tok_rows, kv_groups, repeat, HEAD_DIM)
    start_max = jnp.broadcast_to(
        sink_logits.reshape(kv_groups, repeat)[:, :, None], (kv_groups, repeat, tok_rows)
    )
    start_totals = jnp.ones((kv_groups, repeat, tok_rows), jnp.float32)
    start_accum = jnp.zeros((kv_groups, repeat, tok_rows, HEAD_DIM), jnp.float32)
    key_piece = lax.all_gather(keys_values, "tok", axis=0, tiled=True)
    hidden = down_weight.shape[1]
    shares = lax.axis_size(("head", "pair"))
    share = out_weight.shape[1] // shares
    gate_w = jnp.transpose(gate_up[0], (1, 0, 2)).reshape(2, shares, share, hidden)
    down_w = jnp.transpose(down_weight[0].reshape(hidden, shares, share), (1, 0, 2))
    key_piece, gate_w, down_w = lax.optimization_barrier((key_piece, gate_w, down_w))
    totals = start_totals
    accum = start_accum
    count = key_piece.shape[0]
    split_piece = key_piece.reshape(count, kv_groups, 2, HEAD_DIM)
    scores = (
        jnp.einsum(
            "tgrd,ngd->grtn", grouped, split_piece[:, :, 0], preferred_element_type=jnp.float32
        )
        * 0.125
    )
    key_position = jnp.arange(count, dtype=jnp.int32)
    allowed = key_position[None, :] <= position[:, None]
    scores = jnp.where(allowed, scores, jnp.float32(-1e30))
    new_max = jnp.maximum(start_max, jnp.max(scores, axis=-1))
    decay = jnp.exp(start_max - new_max)
    weights = jnp.exp(scores - new_max[..., None])
    totals = totals * decay + jnp.sum(weights, axis=-1)
    update = jnp.einsum(
        "grtn,ngd->grtd",
        weights.astype(jnp.bfloat16),
        split_piece[:, :, 1],
        preferred_element_type=jnp.float32,
    )
    accum = accum * decay[..., None] + update
    final_max, totals, accum = (new_max, totals, accum)
    attended = (accum / totals[..., None]).astype(jnp.bfloat16)
    attended = jnp.transpose(attended, (2, 0, 1, 3)).reshape(tok_rows, local_heads * HEAD_DIM)
    width = out_weight.shape[1]
    share = width // lax.axis_size(("head", "pair"))
    column_start = lax.axis_index(("head", "pair")) * share
    partial_value = jnp.dot(attended, out_weight, preferred_element_type=jnp.float32)
    experts = lax.axis_size("tok")
    pairs = lax.axis_size("pair")
    cores = 2 // pairs
    shares = width // share
    wide = -(-(share + 2 * experts) // 128) * 128
    expert = jnp.arange(experts, dtype=jnp.int32)
    routed = expert_ids[:, :, None] == expert
    dense = jnp.sum(jnp.where(routed, route_weights[:, :, None], 0.0), axis=1)
    high = lax.reduce_precision(dense, 8, 7)
    weights = jnp.concatenate([high, dense - high], axis=1).astype(jnp.bfloat16)
    tail = jnp.pad(weights, ((0, 0), (share, wide - share - 2 * experts)))
    spare = (0, wide - share)
    parts = jnp.transpose(
        partial_value.astype(jnp.bfloat16).reshape(tok_rows, shares, share), (1, 0, 2)
    )
    parts = jnp.pad(parts, ((0, 0), (0, 0), spare))
    own_residual = jnp.pad(
        lax.dynamic_slice_in_dim(residual, column_start, share, 1), ((0, 0), spare)
    )
    own_gain = jnp.pad(lax.dynamic_slice_in_dim(norm_gain, column_start, share, 0), spare)
    return moe(
        (experts // cores, cores, shares, pairs, share),
        parts, own_residual, own_gain[None, :], tail, gate_w, down_w,
    )


def layer_kernel(
    dims,
    sink_ref,
    ids_ref,
    route_ref,
    gain_ref,
    query_hbm,
    kv_hbm,
    residual_hbm,
    project_hbm,
    gate_hbm,
    down_hbm,
    out_ref,
    query_v,
    query_t,
    kvs,
    row_max,
    row_total,
    accum,
    attended,
    residual_v,
    project_w,
    gate_w,
    down_v,
    down_t,
    gain_cols,
    stream,
    parts,
    peer_parts,
    rows,
    meta,
    hidden,
    active,
    part,
    kept,
    from_core,
    cross,
    from_peer,
    hop,
    relay,
    inbox,
    wide,
    acc,
    squares,
    peer_squares,
    load_sem,
    kv_recv,
    kv_core_send,
    kv_up_send,
    parts_send,
    parts_recv,
    squares_sem,
    row_recv,
    row_up,
    row_down,
    row_core,
    row_peer,
    meta_recv,
    meta_up,
    meta_down,
    meta_core,
    part_send,
    part_recv,
    peer_send,
    peer_recv,
    hop_send,
    relay_recv,
    inbox_recv,
    wide_send,
    wide_recv,
):
    chips, pairs, chunk, piece, own = dims
    cores = 2
    width, depth = residual_hbm.shape
    kv_groups = kvs.shape[1]
    repeat = query_t.shape[2] // depth
    half = width // 2
    f32, bf16 = jnp.float32, jnp.bfloat16
    far = (width - own * chunk) // 128 * 128
    edges = [(at, min(chunk, far - at)) for at in range(own * chunk, far, chunk)]
    if far + own * chunk < width:
        edges.append((far + own * chunk, width - far - own * chunk))
    spread_over = [(2 * own + n, at, size) for n, (at, size) in enumerate(edges)]
    pieces = half // piece
    joint = next(n for n in range(JOINT, 0, -1) if pieces % n == 0)
    last = chips - 1

    tok = lax.axis_index("tok")
    z = tok // cores
    c = tok % cores
    x = lax.axis_index("head") * pairs + lax.axis_index("pair")
    peer = {"head": (1 - x) // pairs, "pair": (1 - x) % pairs}
    other = {"tok": z * cores + (1 - c)}
    above = {"tok": (z + 1) * cores + c}
    below = {"tok": (z - 1) * cores + c}

    def remote(src, dst, send, recv, target):
        return pltpu.make_async_remote_copy(
            src_ref=src, dst_ref=dst, send_sem=send, recv_sem=recv,
            device_id=target, device_id_type=MESH_ID,
        )

    def landed(slot, sem):
        pltpu.make_async_copy(slot, slot, sem).wait()

    def mult(value, of):
        return pl.multiple_of(value, of)

    loads = [
        pltpu.make_async_copy(
            kv_hbm.at[:, pl.ds(g * 2 * HEAD_DIM, 2 * HEAD_DIM)], kvs.at[tok, g], load_sem.at[g]
        )
        for g in range(kv_groups)
    ]
    bulk = [
        pltpu.make_async_copy(src, dst, load_sem.at[kv_groups + i])
        for i, (src, dst) in enumerate(
            [
                (query_hbm, query_v),
                (residual_hbm, residual_v),
                (project_hbm, project_w),
                (down_hbm, down_v),
                (gate_hbm, gate_w),
            ]
        )
    ]
    for load in loads + bulk:
        load.start()

    barrier = pltpu.get_barrier_semaphore()

    @pl.when(z > 0)
    def _():
        pl.semaphore_signal(barrier, 1, device_id=below, device_id_type=MESH_ID)

    @pl.when(z < last)
    def _():
        pl.semaphore_signal(barrier, 1, device_id=above, device_id_type=MESH_ID)

    pl.semaphore_signal(barrier, 1, device_id=other, device_id_type=MESH_ID)
    pl.semaphore_signal(barrier, 1, device_id=peer, device_id_type=MESH_ID)
    sides = jnp.where(z > 0, 1, 0) + jnp.where(z < last, 1, 0)
    pl.semaphore_wait(barrier, sides + 2)

    def kv_up(chip, g):
        slot = kvs.at[chip * cores + c, g]
        return remote(slot, slot, kv_up_send.at[chip, g], kv_recv.at[chip, c, g], above)

    def kv_core(chip, g):
        slot = kvs.at[chip * cores + c, g]
        return remote(slot, slot, kv_core_send.at[chip, g], kv_recv.at[chip, c, g], other)

    def kv_wait(chip, core, g):
        landed(kvs.at[chip * cores + core, g], kv_recv.at[chip, core, g])

    def kv_pass(chip, g):
        @pl.when(z < last)
        def _():
            kv_up(chip, g).start()

        kv_core(chip, g).start()

    for g, load in enumerate(loads):
        load.wait()
        kv_pass(z, g)

    bulk[0].wait()
    for g in range(kv_groups):
        query_t[g, HEAD_DIM:, :] = jnp.zeros((HEAD_DIM, repeat * depth), bf16)
        for m in range(repeat // 2):
            lane = (g * repeat + 2 * m) * HEAD_DIM
            turned = (query_v[:, lane:lane + 2 * HEAD_DIM].astype(f32) * 0.125).T.astype(bf16)
            query_t[g, :HEAD_DIM, 2 * m * depth:(2 * m + 1) * depth] = turned[:HEAD_DIM]
            query_t[g, :HEAD_DIM, (2 * m + 1) * depth:(2 * m + 2) * depth] = turned[HEAD_DIM:]
        for r in range(repeat):
            row_max[g, :, r * depth:(r + 1) * depth] = jnp.full(
                (1, depth), sink_ref[g * repeat + r], f32
            )
    row_total[...] = jnp.ones(row_total.shape, f32)
    accum[...] = jnp.zeros(accum.shape, f32)

    def attend(chip, g, masked):
        keys = kvs[pl.ds(chip * cores, cores), g].reshape(cores * depth, 2 * HEAD_DIM)
        values = keys.astype(f32).T[HEAD_DIM:].astype(bf16)
        olds, totals, sums = row_max[g], row_total[g], accum[g]
        lanes = [slice(2 * m * depth, (2 * m + 2) * depth) for m in range(repeat // 2)]
        scores = [
            jnp.dot(keys, query_t[g, :, lane], preferred_element_type=f32) for lane in lanes
        ]
        if masked:
            row = lax.broadcasted_iota(jnp.int32, scores[0].shape, 0)
            column = lax.broadcasted_iota(jnp.int32, scores[0].shape, 1)
            column = jnp.where(column >= depth, column - depth, column)
            allowed = row <= c * depth + column
            scores = [jnp.where(allowed, score, jnp.float32(-1e30)) for score in scores]
        news = [
            jnp.maximum(olds[:, lane], jnp.max(score, axis=0, keepdims=True))
            for lane, score in zip(lanes, scores)
        ]
        weights = [jnp.exp(score - new) for score, new in zip(scores, news)]
        added = [
            jnp.dot(values, weight.astype(bf16), preferred_element_type=f32) for weight in weights
        ]
        for lane, new, weight, more in zip(lanes, news, weights, added):
            decay = jnp.exp(olds[:, lane] - new)
            row_max[g, :, lane] = new
            row_total[g, :, lane] = totals[:, lane] * decay + jnp.sum(
                weight, axis=0, keepdims=True
            )
            accum[g, :, lane] = sums[:, lane] * decay + more

    def attend_chip(chip, masked):
        def group(g, carry):
            kv_wait(chip, 1 - c, g)
            attend(chip, g, masked)

            @pl.when(chip > 0)
            def _():
                kv_wait(chip - 1, c, g)
                kv_pass(chip - 1, g)

            return carry

        lax.fori_loop(0, kv_groups, group, 0)

    attend_chip(z, True)

    def earlier(i, carry):
        attend_chip(z - i, False)
        return carry

    lax.fori_loop(1, z + 1, earlier, 0)

    for g in range(kv_groups):
        inverse = 1.0 / row_total[g]
        for r in range(repeat):
            lanes = slice(r * depth, (r + 1) * depth)
            head = (g * repeat + r) * HEAD_DIM
            attended[head:head + HEAD_DIM, :] = (accum[g, :, lanes] * inverse[:, lanes]).astype(bf16)

    def own_at(side, t):
        return mult(side * far + t * chunk, 128)

    def own_id(side, t):
        return side * own + t

    def parts_copy(n, start, size):
        return remote(
            parts.at[pl.ds(start, size)], peer_parts.at[pl.ds(start, size)],
            parts_send.at[n], parts_recv.at[n], peer,
        )

    def project(start, size):
        return jnp.dot(
            project_w[pl.ds(start, size), :], attended[...], preferred_element_type=f32
        )

    def give(n, start, size):
        value = project(start, size)
        parts[pl.ds(start, size), :] = value.astype(bf16)
        parts_copy(n, start, size).start()
        return value

    def hold(start, size, value):
        at = pl.ds(start, size)
        stream[at, :] = value + residual_v[at, :].astype(f32)

    def row_copy(chip, k, start, size, send, target):
        slot = rows.at[chip, c, pl.ds(start, size)]
        return remote(slot, slot, send.at[chip, k], row_recv.at[chip, c, k], target)

    def row_wait(chip, core, k, start, size):
        landed(rows.at[chip, core, pl.ds(start, size)], row_recv.at[chip, core, k])

    def pass_along(chip, k, start, size):
        @pl.when((chip <= z) & (z < last))
        def _():
            row_copy(chip, k, start, size, row_up, above).start()

        @pl.when((chip >= z) & (z > 0))
        def _():
            row_copy(chip, k, start, size, row_down, below).start()

    def meta_copy(chip, send, target):
        slot = meta.at[chip, c]
        return remote(slot, slot, send.at[chip], meta_recv.at[chip, c], target)

    def meta_wait(chip, core):
        landed(meta.at[chip, core], meta_recv.at[chip, core])

    def pass_meta(chip):
        @pl.when((chip <= z) & (z < last))
        def _():
            meta_copy(chip, meta_up, above).start()

        @pl.when((chip >= z) & (z > 0))
        def _():
            meta_copy(chip, meta_down, below).start()

        meta_copy(chip, meta_core, other).start()

    def settle(n, k, start, size):
        at = pl.ds(start, size)
        landed(peer_parts.at[at], parts_recv.at[n])
        value = stream[at, :] + peer_parts[at, :].astype(f32)
        stream[at, :] = value
        rows[z, c, at, :] = (value * gain_cols[at, :]).astype(bf16)
        pass_along(z, k, start, size)
        row_copy(z, k, start, size, row_core, other).start()
        return jnp.sum((value * value).reshape(size // 8, 8, depth), axis=0)

    bulk[1].wait()
    bulk[2].wait()

    def give_own(t, carry):
        give(t, own_at(1 - x, t), chunk)
        return carry

    lax.fori_loop(0, own, give_own, 0)
    squares_own = jnp.zeros((8, depth), f32)
    squares_all = jnp.zeros((8, depth), f32)
    for t in range(own):
        hold(own_at(x, t), chunk, project(own_at(x, t), chunk))
        for n, (k, start, size) in enumerate(spread_over):
            if t == 0:
                hold(start, size, give(own + n, start, size))
        if t == 0:
            for b in range(-(-width // 128)):
                size = min(128, width - b * 128)
                gain = gain_ref[b * 128:b * 128 + size]
                gain_cols[b * 128:b * 128 + size, :] = jnp.broadcast_to(gain[None, :], (128, size)).T
        squares_own += settle(t, own_id(x, t), own_at(x, t), chunk)
    squares[...] = squares_own
    squares_copy = remote(squares, peer_squares, squares_sem.at[0], squares_sem.at[1], peer)
    squares_copy.start()

    experts = chips * cores
    expert = lax.broadcasted_iota(jnp.int32, (experts, depth), 0)
    dense = jnp.zeros((experts, depth), f32)
    for k in range(ids_ref.shape[0]):
        dense += jnp.where(ids_ref[k:k + 1, :] == expert, route_ref[k:k + 1, :], 0.0)
    meta[z, c, pl.ds(8, experts), :] = dense
    bulk[3].wait()

    def turn(b, carry):
        at = pl.ds(mult(b * 128, 128), 128)
        down_t[at, :] = down_v[:, at].astype(f32).T.astype(bf16)
        return carry

    turns = width // 128
    if width % 128:
        at = pl.ds(turns * 128, width % 128)
        down_t[at, :] = down_v[:, at].astype(f32).T.astype(bf16)
    for n, (k, start, size) in enumerate(spread_over):
        if n < 2:
            lax.fori_loop(n * turns // 2, (n + 1) * turns // 2, turn, 0)
        squares_all += settle(own + n, k, start, size)
    if len(spread_over) < 2:
        lax.fori_loop(len(spread_over) * turns // 2, turns, turn, 0)
    landed(peer_squares, squares_sem.at[1])
    squares_all += squares[...] + peer_squares[...]
    total = jnp.sum(squares_all, axis=0, keepdims=True)
    scale = lax.rsqrt(total / width + 1e-05)
    meta[z, c, 0:8, :] = jnp.broadcast_to(scale, (8, depth))
    pass_meta(z)

    near = jnp.minimum(z, last - z)

    def chip_at(i):
        inner = jnp.where(i % 2 == 1, z - (i + 1) // 2, z + i // 2)
        outer = jnp.where(z < last - z, i, last - i)
        return jnp.where(i <= 2 * near, inner, outer)

    def each_side(i, act):
        @pl.when(z - 1 - i >= 0)
        def _():
            act(z - 1 - i)

        @pl.when(z + 1 + i <= last)
        def _():
            act(z + 1 + i)

    def pump(i, k, start, size, crosses):
        def act(chip):
            row_wait(chip, c, k, start, size)
            pass_along(chip, k, start, size)
            if crosses:
                row_copy(chip, k, start, size, row_peer, peer).start()
            row_copy(chip, k, start, size, row_core, other).start()

        each_side(i, act)

    def pump_own(i):
        def one(t, carry):
            pump(i, own_id(x, t), own_at(x, t), chunk, True)
            return carry

        lax.fori_loop(0, own, one, 0)

    def pump_shared(i):
        for k, start, size in spread_over:
            pump(i, k, start, size, False)

        def act(chip):
            meta_wait(chip, c)
            pass_meta(chip)

        each_side(i, act)

    def cross_in(chip):
        def one(t, carry):
            k, start = own_id(1 - x, t), own_at(1 - x, t)
            row_wait(chip, c, k, start, chunk)
            row_copy(chip, k, start, chunk, row_core, other).start()
            return carry

        lax.fori_loop(0, own, one, 0)

    def multiply(chip, k, start, size):
        row_wait(chip, 1 - c, k, start, size)
        at = pl.ds(start, size)
        pair = jnp.concatenate([rows[chip, c, at, :], rows[chip, 1 - c, at, :]], axis=1)
        units = hidden.shape[0] // 2
        for side in range(2):
            lot = slice(side * units, (side + 1) * units)
            hidden[lot] += jnp.dot(gate_w[lot, at], pair, preferred_element_type=f32)

    def multiply_line(chip):
        hidden[...] = jnp.zeros(hidden.shape, f32)

        def one(t, carry):
            multiply(chip, own_id(x, t), own_at(x, t), chunk)
            return carry

        lax.fori_loop(0, own, one, 0)
        for k, start, size in spread_over:
            multiply(chip, k, start, size)

    def multiply_crossed(chip):
        def one(t, carry):
            multiply(chip, own_id(1 - x, t), own_at(1 - x, t), chunk)
            return carry

        lax.fori_loop(0, own, one, 0)

    def part_copy(chip, r):
        return remote(
            part.at[chip, r], from_core.at[chip, r], part_send.at[chip, r],
            part_recv.at[chip, r], other,
        )

    def cross_copy(chip, r):
        return remote(
            cross.at[chip, r], from_peer.at[chip, r], peer_send.at[chip, r],
            peer_recv.at[chip, r], peer,
        )

    def far_end(chip):
        return chip == jnp.where(chip > z, last, 0)

    def adds(chip):
        return far_end(chip) & (jnp.where(chip > z, z, last - z) % 2 == 1) & (chip != partner)

    def relay_copy(chip, u):
        return remote(
            hop.at[chip, u], relay.at[chip, u], hop_send.at[chip, u],
            relay_recv.at[chip, u], {"tok": tok + jnp.where(chip > z, cores, -cores)},
        )

    def final_copy(chip, u):
        return remote(
            hop.at[chip, u], inbox.at[z, u], hop_send.at[chip, u],
            inbox_recv.at[z, u], {"tok": chip * cores + c},
        )

    partner = z + 1 - 2 * (z % 2)

    def wide_copy(at):
        return remote(
            kept.at[partner, at], wide.at[at], wide_send.at[at], wide_recv.at[at],
            {"tok": partner * cores + c},
        )

    def send_sum(chip, low, high):
        direct = adds(chip) | jnp.logical_not(far_end(chip))

        def one(u, carry):
            landed(from_peer.at[chip, u], peer_recv.at[chip, u])
            acc[...] = kept[chip, x * pieces + u].astype(f32) + from_peer[chip, u].astype(f32)

            @pl.when(adds(chip))
            def _():
                landed(relay.at[chip, u], relay_recv.at[chip, u])
                acc[...] += relay[chip, u].astype(f32)

            hop[chip, u] = acc[...].astype(bf16)

            @pl.when(direct)
            def _():
                final_copy(chip, u).start()

            @pl.when(jnp.logical_not(direct))
            def _():
                relay_copy(chip, u).start()

            return carry

        lax.fori_loop(low, high, one, 0)

    def send_own_sum(chip, low, high):
        @pl.when((chip != partner) & jnp.logical_not(adds(chip)))
        def _():
            send_sum(chip, low, high)

    def activate(chip):
        meta_wait(chip, 1 - c)
        scale = jnp.concatenate([meta[chip, c, 0:1, :], meta[chip, 1 - c, 0:1, :]], axis=1)
        weight = jnp.concatenate(
            [meta[chip, c, pl.ds(8 + tok, 1), :], meta[chip, 1 - c, pl.ds(8 + tok, 1), :]], axis=1
        )
        units = hidden.shape[0] // 2
        gate = hidden[:units] * scale
        up = hidden[units:] * scale
        active[...] = (gate * jax.nn.sigmoid(1.702 * gate) * (up + 1.0) * weight).astype(bf16)

    def spread_out(chip, between=None):
        def spread(n, carry):
            first = joint * n
            first = jnp.where(first < pieces, (1 - x) * pieces + first, x * pieces + first - pieces)
            value = jnp.dot(
                down_t[pl.ds(mult(first * piece, 16), joint * piece), :], active[...],
                preferred_element_type=f32,
            )
            for m in range(joint):
                at = first + m
                block = value[m * piece:(m + 1) * piece]
                part[chip, at] = block[:, depth:].astype(bf16)
                part_copy(chip, at).start()
                kept[chip, at] = block[:, :depth].astype(bf16)
            return carry

        lax.fori_loop(0, 2 * pieces // joint, spread, 0)
        if between is not None:
            between()

        def summed(at):
            landed(from_core.at[chip, at], part_recv.at[chip, at])
            acc[...] = kept[chip, at].astype(f32) + from_core[chip, at].astype(f32)

            @pl.when(chip == z)
            def _():
                landed(wide.at[at], wide_recv.at[at])
                acc[...] += wide[at].astype(f32)

        def keep(at):
            kept[chip, at] = acc[...].astype(bf16)

            @pl.when(chip == partner)
            def _():
                wide_copy(at).start()

        def give_half(r, carry):
            at = (1 - x) * pieces + r
            summed(at)

            @pl.when(chip == partner)
            def _():
                keep(at)

            @pl.when(chip != partner)
            def _():
                cross[chip, r] = acc[...].astype(bf16)
                cross_copy(chip, r).start()

            return carry

        lax.fori_loop(0, pieces, give_half, 0)

        def keep_half(r, carry):
            summed(x * pieces + r)
            keep(x * pieces + r)
            return carry

        lax.fori_loop(0, pieces, keep_half, 0)

    is_end = (z == 0) | (z == last)
    early = z < chips // 2

    def own_across():
        for t in range(own):
            row_copy(z, own_id(x, t), own_at(x, t), chunk, row_peer, peer).start()

    @pl.when(early)
    def _():
        own_across()

    bulk[4].wait()
    pump_own(0)
    pump_shared(0)

    @pl.when(jnp.logical_not(early))
    def _():
        own_across()


    def step(i, carry):
        chip = chip_at(i)
        multiply_line(chip)

        pump_own(i)

        @pl.when(jnp.logical_not(is_end))
        def _():
            pump_shared(i)

        each_side(i - 1, cross_in)
        multiply_crossed(chip)

        @pl.when(i > 1)
        def _():
            send_own_sum(chip_at(i - 1), 0, pieces // 2)

        def between():
            @pl.when(is_end)
            def _():
                pump_shared(i)

        activate(chip)
        spread_out(chip, between)

        @pl.when(i > 1)
        def _():
            send_own_sum(chip_at(i - 1), pieces // 2, pieces)

        return carry

    lax.fori_loop(1, chips, step, 0)
    cuts = [pieces * n // 3 for n in range(4)]

    def send_last(n):
        send_own_sum(chip_at(last), cuts[n], cuts[n + 1])

    multiply_line(z)
    send_last(0)
    cross_in(z)
    multiply_crossed(z)
    activate(z)
    send_last(1)
    spread_out(z, lambda: send_last(2))

    def send_added(i, carry):
        @pl.when(adds(chip_at(i)))
        def _():
            send_sum(chip_at(i), 0, pieces)

        return carry

    lax.fori_loop(1, chips, send_added, 0)

    def finish(r, carry):
        at = pl.ds(mult(x * half + r * piece, 16), piece)
        landed(from_peer.at[z, r], peer_recv.at[z, r])
        acc[...] = kept[z, x * pieces + r].astype(f32) + from_peer[z, r].astype(f32)
        for src in range(chips):
            below_it = (src < z) & ((z < last) | (src % 2 == 1))
            above_it = (src > z) & ((z > 0) | ((last - src) % 2 == 1))

            @pl.when((below_it | above_it) & (src != partner))
            def _():
                landed(inbox.at[src, r], inbox_recv.at[src, r])
                acc[...] += inbox[src, r].astype(f32)

        out_ref[pl.ds(mult(r * piece, piece), piece), :] = (stream[at, :] + acc[...]).astype(bf16)
        return carry

    lax.fori_loop(0, pieces, finish, 0)

    def drain(chip, carry):
        for g in range(kv_groups):
            @pl.when(chip <= z)
            def _():
                kv_core(chip, g).wait_send()

            @pl.when((chip <= z) & (z < last))
            def _():
                kv_up(chip, g).wait_send()

        def sent(k, start, size, on_line, crosses):
            if on_line:
                @pl.when((chip <= z) & (z < last))
                def _():
                    row_copy(chip, k, start, size, row_up, above).wait_send()

                @pl.when((chip >= z) & (z > 0))
                def _():
                    row_copy(chip, k, start, size, row_down, below).wait_send()

            if crosses:
                row_copy(chip, k, start, size, row_peer, peer).wait_send()

            row_copy(chip, k, start, size, row_core, other).wait_send()

        for t in range(own):
            sent(own_id(x, t), own_at(x, t), chunk, True, True)
            sent(own_id(1 - x, t), own_at(1 - x, t), chunk, False, False)
        for k, start, size in spread_over:
            sent(k, start, size, True, False)

        @pl.when((chip <= z) & (z < last))
        def _():
            meta_copy(chip, meta_up, above).wait_send()

        @pl.when((chip >= z) & (z > 0))
        def _():
            meta_copy(chip, meta_down, below).wait_send()

        meta_copy(chip, meta_core, other).wait_send()
        for r in range(2 * pieces):
            part_copy(chip, r).wait_send()
        @pl.when(chip != partner)
        def _():
            for r in range(pieces):
                cross_copy(chip, r).wait_send()

        @pl.when(chip == partner)
        def _():
            for r in range(2 * pieces):
                wide_copy(r).wait_send()

        @pl.when((chip != z) & (chip != partner))
        def _():
            for u in range(pieces):
                final_copy(chip, u).wait_send()

        return carry

    lax.fori_loop(0, chips, drain, 0)
    for t in range(own):
        parts_copy(t, own_at(1 - x, t), chunk).wait_send()
    for n, (k, start, size) in enumerate(spread_over):
        parts_copy(own + n, start, size).wait_send()
    squares_copy.wait_send()


def whole_layer(
    dims, sinks, ids, route, gain, queries, keys_values, residual, project, gate_up, down
):
    chips, pairs, chunk, piece, own = dims
    cores = 2
    width, depth = residual.shape
    kv_groups = keys_values.shape[1] // (2 * HEAD_DIM)
    heads = queries.shape[1] // HEAD_DIM
    repeat = heads // kv_groups
    hidden = down.shape[0]
    half = width // 2
    pieces = half // piece
    count = -(-width // chunk) + 2
    bf16, f32 = jnp.bfloat16, jnp.float32
    dma = pltpu.SemaphoreType.DMA
    vmem = pltpu.VMEM
    experts = chips * cores
    flops = 2 * width * (
        depth * heads * HEAD_DIM + chips * cores * depth * 3 * hidden
    )
    return pl.pallas_call(
        functools.partial(layer_kernel, dims),
        out_shape=jax.ShapeDtypeStruct((half, depth), bf16),
        in_specs=[pl.BlockSpec(memory_space=pltpu.SMEM)]
        + [pl.BlockSpec(memory_space=pltpu.VMEM)] * 3
        + [pl.BlockSpec(memory_space=pl.ANY)] * 6,
        out_specs=pl.BlockSpec(memory_space=pltpu.VMEM),
        scratch_shapes=[
            vmem(queries.shape, bf16),
            vmem((kv_groups, 2 * HEAD_DIM, repeat * depth), bf16),
            vmem((experts, kv_groups, depth, 2 * HEAD_DIM), bf16),
            vmem((kv_groups, 1, repeat * depth), f32),
            vmem((kv_groups, 1, repeat * depth), f32),
            vmem((kv_groups, HEAD_DIM, repeat * depth), f32),
            vmem((heads * HEAD_DIM, depth), bf16),
            vmem(residual.shape, bf16),
            vmem(project.shape, bf16),
            vmem(gate_up.shape, bf16),
            vmem(down.shape, bf16),
            vmem((width, hidden), bf16),
            vmem((width, depth), f32),
            vmem((width, depth), f32),
            vmem((width, depth), bf16),
            vmem((width, depth), bf16),
            vmem((chips, cores, width, depth), bf16),
            vmem((chips, cores, 8 + experts, depth), f32),
            vmem((2 * hidden, cores * depth), f32),
            vmem((hidden, cores * depth), bf16),
            vmem((chips, 2 * pieces, piece, depth), bf16),
            vmem((chips, 2 * pieces, piece, depth), bf16),
            vmem((chips, 2 * pieces, piece, depth), bf16),
            vmem((chips, pieces, piece, depth), bf16),
            vmem((chips, pieces, piece, depth), bf16),
            vmem((chips, pieces, piece, depth), bf16),
            vmem((chips, pieces, piece, depth), bf16),
            vmem((chips, pieces, piece, depth), bf16),
            vmem((2 * pieces, piece, depth), bf16),
            vmem((piece, depth), f32),
            vmem((8, depth), f32),
            vmem((8, depth), f32),
            dma((kv_groups + 5,)),
            dma((chips, cores, kv_groups)),
            dma((chips, kv_groups)),
            dma((chips, kv_groups)),
            dma((count,)),
            dma((count,)),
            dma((2,)),
            dma((chips, cores, count)),
            dma((chips, count)),
            dma((chips, count)),
            dma((chips, count)),
            dma((chips, count)),
            dma((chips, cores)),
            dma((chips,)),
            dma((chips,)),
            dma((chips,)),
            dma((chips, 2 * pieces)),
            dma((chips, 2 * pieces)),
            dma((chips, pieces)),
            dma((chips, pieces)),
            dma((chips, pieces)),
            dma((chips, pieces)),
            dma((chips, pieces)),
            dma((2 * pieces,)),
            dma((2 * pieces,)),
        ],
        compiler_params=pltpu.CompilerParams(
            collective_id=0, has_side_effects=True, vmem_limit_bytes=VMEM_BYTES
        ),
        cost_estimate=pl.CostEstimate(
            flops=flops,
            bytes_accessed=2 * (project.size + gate_up.size + down.size),
            transcendentals=0,
        ),
    )(sinks, ids, route, gain, queries, keys_values, residual, project, gate_up, down)


def per_device_whole(
    queries,
    keys_values,
    sink_logits,
    residual,
    out_weight,
    norm_gain,
    expert_ids,
    route_weights,
    gate_up,
    down_weight,
):
    width = residual.shape[1]
    pairs = lax.axis_size("pair")
    chips = lax.axis_size("tok") // 2
    half = width // 2
    chunk = min(CHUNK, half // 128 * 128)
    piece = next(n for n in (PIECE, 160, 80, 48, 32, 16, half) if half % n == 0)
    own = min(OWN, half // chunk)
    out = whole_layer(
        (chips, pairs, chunk, piece, own),
        sink_logits,
        expert_ids.T,
        route_weights.T,
        norm_gain,
        queries,
        keys_values,
        residual.T,
        out_weight.T,
        jnp.transpose(gate_up[0], (1, 2, 0)).reshape(2 * down_weight.shape[1], width),
        down_weight[0],
    )
    return out.T


def solution(mesh):
    placed = (
        P(("groups", "tok"), ("head", "pair")),
        P(("groups", "tok"), ("head", "pair")),
        P(("head", "pair")),
        P(("groups", "tok"), None),
        P(("head", "pair"), None),
        P(),
        P(("groups", "tok"), None),
        P(("groups", "tok"), None),
        P("tok", None, None, ("head", "pair")),
        P("tok", ("head", "pair"), None),
    )
    sizes = mesh.shape
    chip_pair = sizes["pair"] == 1 and sizes["head"] == 2 and sizes["tok"] % 4 == 0
    return jax.shard_map(
        per_device_whole if chip_pair else per_device,
        mesh=mesh,
        in_specs=placed,
        out_specs=P(("groups", "tok"), ("head", "pair")),
        check_vma=False,
    )
```
